32 devices in a mesh: data: 4 (over y, z), seq: 8 (over x, core).
Axes of the slice: x: 4, y: 2, z: 2, core: 2. Of those that a mesh axis runs over, the one named last changes fastest.
The devices are a block of a 4x4x8 slice.
Arguments:
- patches: bfloat16 [256, 1024, 256], P('data', 'seq'), parts along dimension 0
- ln1_gain: float32 [256], replicated
- ln1_bias: float32 [256], replicated
- w_in: bfloat16 [256, 1536], replicated
- b_in: float32 [1536], replicated
- ln2_gain: float32 [768], replicated
- ln2_bias: float32 [768], replicated
- w_spatial: bfloat16 [1024, 1024], replicated
- b_spatial: float32 [1024], replicated
- w_out: bfloat16 [768, 256], replicated
- b_out: float32 [256], replicated
Outputs:
- output: bfloat16 [256, 1024, 256], P('data', 'seq'), parts along dimension 0
There are 4 independent parts. The reference program is written for one: setup_inputs(seed, part) draws one part's arguments, and reference() takes and returns one part's arrays. A program takes and returns all parts, laid end to end along the dimension named above; an argument that names none is the same for every part.
All inputs are finite; a program needn't handle non-finite values.
Results may differ from the reference program's by a relative error of at most 0.00919827.
Values are sent between devices in bfloat16 or wider.
A program may use at most 768 MiB of HBM per device.

```python
import jax
import jax.numpy as jnp
from jax import lax

BATCH_SIZE = 64
NUM_PATCHES = 1024
MODEL_DIM = 256
GATE_DIM = 768
LN_EPS = 1e-6


def layer_norm(values, gain_vec, offset):
    values_f = values.astype(jnp.float32)
    mean_val = jnp.mean(values_f, axis=-1, keepdims=True)
    centered = values_f - mean_val
    var_val = jnp.mean(centered * centered, axis=-1, keepdims=True)
    return (centered * lax.rsqrt(var_val + LN_EPS) * gain_vec + offset).astype(jnp.bfloat16)


def setup_inputs(seed: int = 0, part: int = 0) -> dict:
    key_list = jax.random.split(jax.random.key(seed), 11)
    part_key = jax.random.fold_in(key_list[0], part)
    two_gate = 2 * GATE_DIM
    patches = jax.random.normal(part_key, (BATCH_SIZE, NUM_PATCHES, MODEL_DIM), jnp.float32)
    ln1_gain = 1.0 + 0.3 * jax.random.normal(key_list[1], (MODEL_DIM,), jnp.float32)
    ln1_bias = 0.3 * jax.random.normal(key_list[2], (MODEL_DIM,), jnp.float32)
    w_in = jax.random.normal(key_list[3], (MODEL_DIM, two_gate), jnp.float32) * MODEL_DIM ** -0.5
    b_in = 0.3 * jax.random.normal(key_list[4], (two_gate,), jnp.float32)
    ln2_gain = 1.0 + 0.3 * jax.random.normal(key_list[5], (GATE_DIM,), jnp.float32)
    ln2_bias = 0.3 * jax.random.normal(key_list[6], (GATE_DIM,), jnp.float32)
    w_spatial = jax.random.normal(key_list[7], (NUM_PATCHES, NUM_PATCHES), jnp.float32) * NUM_PATCHES ** -0.5
    b_spatial = 1.0 + 0.5 * jax.random.normal(key_list[8], (NUM_PATCHES,), jnp.float32)
    w_out = jax.random.normal(key_list[9], (GATE_DIM, MODEL_DIM), jnp.float32) * GATE_DIM ** -0.5
    b_out = 0.3 * jax.random.normal(key_list[10], (MODEL_DIM,), jnp.float32)
    return {
        "patches": patches.astype(jnp.bfloat16),
        "ln1_gain": ln1_gain,
        "ln1_bias": ln1_bias,
        "w_in": w_in.astype(jnp.bfloat16),
        "b_in": b_in,
        "ln2_gain": ln2_gain,
        "ln2_bias": ln2_bias,
        "w_spatial": w_spatial.astype(jnp.bfloat16),
        "b_spatial": b_spatial,
        "w_out": w_out.astype(jnp.bfloat16),
        "b_out": b_out,
    }


def reference(patches, ln1_gain, ln1_bias, w_in, b_in, ln2_gain, ln2_bias, w_spatial, b_spatial, w_out, b_out):
    half_dim = w_out.shape[0]

    def one_image(image):
        normed = layer_norm(image, ln1_gain, ln1_bias)
        hidden = jnp.dot(normed, w_in, preferred_element_type=jnp.float32) + b_in
        hidden = jax.nn.gelu(hidden, approximate=False).astype(jnp.bfloat16)
        gate_a = hidden[:, :half_dim]
        gate_n = layer_norm(hidden[:, half_dim:], ln2_gain, ln2_bias)
        spatial = jnp.dot(w_spatial.T, gate_n, preferred_element_type=jnp.float32).astype(jnp.bfloat16)
        gated = (gate_a.astype(jnp.float32) * (spatial.astype(jnp.float32) + b_spatial[:, None])).astype(jnp.bfloat16)
        mixed = jnp.dot(gated, w_out, preferred_element_type=jnp.float32) + b_out
        return (image.astype(jnp.float32) + mixed).astype(jnp.bfloat16)

    return lax.map(one_image, patches)
```

```python
import functools

import jax
import jax.numpy as jnp
from jax import lax
from jax.experimental import pallas as pl
from jax.experimental.pallas import tpu as pltpu
from jax.sharding import PartitionSpec as P

LN_EPS = 1e-6
MESH = pl.DeviceIdType.MESH
F32 = jnp.float32
BF16 = jnp.bfloat16
TILE = 256


def layer_norm(values, gain_vec, offset):
    values_f = values.astype(F32)
    mean_val = jnp.mean(values_f, axis=-1, keepdims=True)
    centered = values_f - mean_val
    var_val = jnp.mean(centered * centered, axis=-1, keepdims=True)
    return (centered * lax.rsqrt(var_val + LN_EPS) * gain_vec + offset).astype(BF16)


def gelu(hidden):
    half = 0.5 * hidden
    return (half + half * lax.erf(hidden * (0.5 ** 0.5))).astype(BF16)


def block_kernel(n_seq, axis, x_hbm, ln1_gain, ln1_bias, w_in_hbm, b_in, ln2_gain, ln2_bias, w_spatial_hbm, b_spatial, w_out_hbm,
                 b_out, out_hbm, x_buf, o_buf, n_buf, a_buf, w_in, w_out, w_spatial, w_mix, bias_col, in_send, in_recv,
                 out_send, out_recv, w_sem):
    me = lax.axis_index(axis)
    images, rows, _ = x_hbm.shape
    own = images // n_seq
    patches = rows * n_seq
    half_dim = w_out.shape[0]
    per_tile = TILE // rows
    tiles = patches // TILE
    home = me // per_tile

    barrier = pltpu.get_barrier_semaphore()
    for off in range(1, n_seq):
        pl.semaphore_signal(barrier, inc=1, device_id={axis: lax.rem(me + off, n_seq)}, device_id_type=MESH)
    pl.semaphore_wait(barrier, n_seq - 1)

    def block_rows(dev):
        return pl.ds(pl.multiple_of(dev * rows, rows), rows)

    @pl.loop(0, own)
    def _(slot):
        for off in range(1, n_seq):
            dev = lax.rem(me + off, n_seq)
            pltpu.make_async_remote_copy(
                src_ref=x_hbm.at[dev * own + slot],
                dst_ref=x_buf.at[slot, block_rows(me)],
                send_sem=in_send.at[off],
                recv_sem=in_recv.at[slot],
                device_id={axis: dev},
                device_id_type=MESH,
            ).start()
        pltpu.make_async_copy(x_hbm.at[me * own + slot], x_buf.at[slot, block_rows(me)], in_recv.at[slot]).start()

    weights = [
        pltpu.make_async_copy(w_spatial_hbm, w_spatial, w_sem.at[0]),
        pltpu.make_async_copy(w_in_hbm, w_in, w_sem.at[1]),
        pltpu.make_async_copy(w_out_hbm, w_out, w_sem.at[2]),
    ]
    for copy in weights:
        copy.start()
    for first in range(0, patches, 128):
        lane_bias = jnp.broadcast_to(b_spatial[:, first:first + 128], (128, 128))
        bias_col[first:first + 128, :] = lane_bias.T
    weights[0].wait()

    @pl.loop(0, patches // TILE)
    def _(step):
        out_rows = pl.ds(pl.multiple_of(step * TILE, TILE), TILE)
        for first in range(0, patches, TILE):
            w_mix[out_rows, first:first + TILE] = w_spatial[first:first + TILE, out_rows].T

    weights[1].wait()
    weights[2].wait()

    def send_tile(slot, tile):
        for part in range(per_tile):
            dev = tile * per_tile + part
            pltpu.make_async_remote_copy(
                src_ref=o_buf.at[slot, block_rows(dev)],
                dst_ref=out_hbm.at[me * own + slot],
                send_sem=out_send.at[0],
                recv_sem=out_recv.at[me],
                device_id={axis: dev},
                device_id_type=MESH,
            ).start()

    def send_home(slot):
        pltpu.make_async_copy(o_buf.at[slot, block_rows(me)], out_hbm.at[me * own + slot], out_recv.at[me]).start()
        for step in range(1, per_tile):
            dev = home * per_tile + lax.rem(me + step, per_tile)
            pltpu.make_async_remote_copy(
                src_ref=o_buf.at[slot, block_rows(dev)],
                dst_ref=out_hbm.at[me * own + slot],
                send_sem=out_send.at[0],
                recv_sem=out_recv.at[me],
                device_id={axis: dev},
                device_id_type=MESH,
            ).start()

    @pl.loop(0, own)
    def _(slot):
        pltpu.make_async_copy(x_buf.at[slot], x_buf.at[slot], in_recv.at[slot]).wait()

        @pl.loop(0, tiles)
        def _(tile):
            here = pl.ds(pl.multiple_of(tile * TILE, TILE), TILE)
            normed = layer_norm(x_buf[slot, here, :], ln1_gain[...], ln1_bias[...])
            gate = []
            for first in range(0, 2 * half_dim, 256):
                cols = slice(first, first + 256)
                hidden = jnp.dot(normed, w_in[:, cols], preferred_element_type=F32) + b_in[:, cols]
                act = gelu(hidden)
                if first < half_dim:
                    a_buf[here, cols] = act
                else:
                    gate.append(act)
            gate = jnp.concatenate(gate, axis=1)
            n_buf[here, :] = layer_norm(gate, ln2_gain[...], ln2_bias[...])

        @pl.when(slot > 0)
        def _():
            send_home(slot - 1)

        @pl.loop(0, tiles)
        def _(step):
            tile = lax.rem(home + 1 + step, tiles)
            here = pl.ds(pl.multiple_of(tile * TILE, TILE), TILE)
            spatial = jnp.dot(w_mix[here, :], n_buf[...], preferred_element_type=F32).astype(BF16)
            bias = jnp.tile(bias_col[here, :], (1, half_dim // 128))
            gated = (a_buf[here, :].astype(F32) * (spatial.astype(F32) + bias)).astype(BF16)
            mixed = jnp.dot(gated, w_out[...], preferred_element_type=F32) + b_out[...]
            o_buf[slot, here, :] = (x_buf[slot, here, :].astype(F32) + mixed).astype(BF16)

            @pl.when(step > 0)
            def _():
                send_tile(slot, lax.rem(home + step, tiles))

    send_home(own - 1)

    for off in range(1, n_seq):
        dev = lax.rem(me + off, n_seq)
        pltpu.make_async_copy(x_hbm.at[pl.ds(0, own)], x_hbm.at[pl.ds(0, own)], in_send.at[off]).wait()
    sent = o_buf.at[:, pl.ds(0, rows * (n_seq - 1))]
    pltpu.make_async_copy(sent, sent, out_send.at[0]).wait()
    for dev in range(n_seq):
        part = out_hbm.at[pl.ds(dev * own, own)]
        pltpu.make_async_copy(part, part, out_recv.at[dev]).wait()


def solution(mesh):
    row_spec = P("data", "seq", None)
    vec_spec = P(None)
    mat_spec = P(None, None)
    in_specs = (row_spec, vec_spec, vec_spec, mat_spec, vec_spec, vec_spec, vec_spec, mat_spec, vec_spec, mat_spec, vec_spec)
    n_seq = mesh.shape["seq"]

    def per_device(patches, ln1_gain, ln1_bias, w_in, b_in, ln2_gain, ln2_bias, w_spatial, b_spatial, w_out, b_out):
        images, rows, dim = patches.shape
        own = images // n_seq
        total = rows * n_seq
        half_dim = w_out.shape[0]
        hbm = pl.BlockSpec(memory_space=pl.ANY)
        vmem = pl.BlockSpec(memory_space=pltpu.VMEM)
        row = lambda vec: vec.reshape(1, vec.shape[0])
        return pl.pallas_call(
            functools.partial(block_kernel, n_seq, "seq"),
            out_shape=jax.ShapeDtypeStruct(patches.shape, BF16),
            in_specs=[hbm, vmem, vmem, hbm, vmem, vmem, vmem, hbm, vmem, hbm, vmem],
            out_specs=hbm,
            scratch_shapes=[
                pltpu.VMEM((own, total, dim), BF16),
                pltpu.VMEM((own, total, dim), BF16),
                pltpu.VMEM((total, half_dim), BF16),
                pltpu.VMEM((total, half_dim), BF16),
                pltpu.VMEM(w_in.shape, BF16),
                pltpu.VMEM(w_out.shape, BF16),
                pltpu.VMEM(w_spatial.shape, BF16),
                pltpu.VMEM(w_spatial.shape, BF16),
                pltpu.VMEM((total, 128), F32),
                pltpu.SemaphoreType.DMA((n_seq,)),
                pltpu.SemaphoreType.DMA((own,)),
                pltpu.SemaphoreType.DMA((1,)),
                pltpu.SemaphoreType.DMA((n_seq,)),
                pltpu.SemaphoreType.DMA((3,)),
            ],
            compiler_params=pltpu.CompilerParams(
                collective_id=0, has_side_effects=True, vmem_limit_bytes=48 * 1024 * 1024
            ),
            name="gmlp_block",
        )(patches, row(ln1_gain), row(ln1_bias), w_in, row(b_in), row(ln2_gain), row(ln2_bias), w_spatial, row(b_spatial),
          w_out, row(b_out))

    return jax.shard_map(per_device, mesh=mesh, in_specs=in_specs, out_specs=row_spec, check_vma=False)
```

```python
import functools

import jax
import jax.numpy as jnp
from jax import lax
from jax.experimental import pallas as pl
from jax.experimental.pallas import tpu as pltpu
from jax.sharding import PartitionSpec as P

LN_EPS = 1e-6
MESH = pl.DeviceIdType.MESH
F32 = jnp.float32
BF16 = jnp.bfloat16
TILE = 256


def layer_norm(values, gain_vec, offset):
    values_f = values.astype(F32)
    mean_val = jnp.mean(values_f, axis=-1, keepdims=True)
    centered = values_f - mean_val
    var_val = jnp.mean(centered * centered, axis=-1, keepdims=True)
    return (centered * lax.rsqrt(var_val + LN_EPS) * gain_vec + offset).astype(BF16)


def as_row(ref):
    return ref[...].reshape(1, ref.shape[0])


def gelu(hidden):
    half = 0.5 * hidden
    return (half + half * lax.erf(hidden * (0.5 ** 0.5))).astype(BF16)


def block_kernel(n_seq, axis, x_hbm, ln1_gain_hbm, ln1_bias_hbm, w_in_hbm, b_in_hbm, ln2_gain_hbm, ln2_bias_hbm, w_spatial_hbm,
                 b_spatial_hbm, w_out_hbm, b_out_hbm, out_ref, x_buf, o_buf, n_buf, a_buf, ln1_gain, ln1_bias, w_in, b_in, ln2_gain,
                 ln2_bias, w_spatial, b_spatial, w_out, b_out, w_mix, bias_col, in_send, in_recv, out_send, out_recv, w_sem):
    me = lax.axis_index(axis)
    images, rows, _ = x_hbm.shape
    own = images // n_seq
    patches = rows * n_seq
    half_dim = w_out.shape[0]
    per_tile = TILE // rows
    tiles = patches // TILE
    home = me // per_tile

    barrier = pltpu.get_barrier_semaphore()
    for off in range(1, n_seq):
        pl.semaphore_signal(barrier, inc=1, device_id={axis: lax.rem(me + off, n_seq)}, device_id_type=MESH)
    pl.semaphore_wait(barrier, n_seq - 1)

    def block_rows(dev):
        return pl.ds(pl.multiple_of(dev * rows, rows), rows)

    @pl.loop(0, own)
    def _(slot):
        for off in range(1, n_seq):
            dev = lax.rem(me + off, n_seq)
            pltpu.make_async_remote_copy(
                src_ref=x_hbm.at[dev * own + slot],
                dst_ref=x_buf.at[slot, block_rows(me)],
                send_sem=in_send.at[off],
                recv_sem=in_recv.at[slot],
                device_id={axis: dev},
                device_id_type=MESH,
            ).start()
        pltpu.make_async_copy(x_hbm.at[me * own + slot], x_buf.at[slot, block_rows(me)], in_recv.at[slot]).start()

    operands = [
        (b_spatial_hbm, b_spatial), (w_spatial_hbm, w_spatial), (ln1_gain_hbm, ln1_gain), (ln1_bias_hbm, ln1_bias), (w_in_hbm, w_in),
        (b_in_hbm, b_in), (ln2_gain_hbm, ln2_gain), (ln2_bias_hbm, ln2_bias), (w_out_hbm, w_out), (b_out_hbm, b_out),
    ]
    loads = [pltpu.make_async_copy(src, dst, w_sem.at[k]) for k, (src, dst) in enumerate(operands)]
    for load in loads:
        load.start()
    loads[0].wait()
    for first in range(0, patches, 128):
        lane_bias = jnp.broadcast_to(b_spatial[first:first + 128].reshape(1, 128), (128, 128))
        bias_col[first:first + 128, :] = lane_bias.T
    loads[1].wait()

    @pl.loop(0, patches // TILE)
    def _(step):
        out_rows = pl.ds(pl.multiple_of(step * TILE, TILE), TILE)
        for first in range(0, patches, TILE):
            w_mix[out_rows, first:first + TILE] = w_spatial[first:first + TILE, out_rows].T

    for load in loads[2:]:
        load.wait()

    def send_tile(slot, tile):
        for part in range(per_tile):
            dev = tile * per_tile + part
            pltpu.make_async_remote_copy(
                src_ref=o_buf.at[slot, block_rows(dev)],
                dst_ref=out_ref.at[me * own + slot],
                send_sem=out_send.at[0],
                recv_sem=out_recv.at[me],
                device_id={axis: dev},
                device_id_type=MESH,
            ).start()

    def send_home(slot):
        pltpu.make_async_copy(o_buf.at[slot, block_rows(me)], out_ref.at[me * own + slot], out_recv.at[me]).start()
        for step in range(1, per_tile):
            dev = home * per_tile + lax.rem(me + step, per_tile)
            pltpu.make_async_remote_copy(
                src_ref=o_buf.at[slot, block_rows(dev)],
                dst_ref=out_ref.at[me * own + slot],
                send_sem=out_send.at[0],
                recv_sem=out_recv.at[me],
                device_id={axis: dev},
                device_id_type=MESH,
            ).start()

    @pl.loop(0, own)
    def _(slot):
        pltpu.make_async_copy(x_buf.at[slot], x_buf.at[slot], in_recv.at[slot]).wait()

        @pl.loop(0, tiles)
        def _(tile):
            here = pl.ds(pl.multiple_of(tile * TILE, TILE), TILE)
            normed = layer_norm(x_buf[slot, here, :], as_row(ln1_gain), as_row(ln1_bias))
            gate = []
            for first in range(0, 2 * half_dim, 256):
                cols = slice(first, first + 256)
                hidden = jnp.dot(normed, w_in[:, cols], preferred_element_type=F32) + b_in[cols].reshape(1, 256)
                act = gelu(hidden)
                if first < half_dim:
                    a_buf[here, cols] = act
                else:
                    gate.append(act)
            gate = jnp.concatenate(gate, axis=1)
            n_buf[here, :] = layer_norm(gate, as_row(ln2_gain), as_row(ln2_bias))

        @pl.when(slot > 0)
        def _():
            send_home(slot - 1)

        @pl.loop(0, tiles)
        def _(step):
            tile = lax.rem(home + 1 + step, tiles)
            here = pl.ds(pl.multiple_of(tile * TILE, TILE), TILE)
            spatial = jnp.dot(w_mix[here, :], n_buf[...], preferred_element_type=F32).astype(BF16)
            bias = jnp.tile(bias_col[here, :], (1, half_dim // 128))
            gated = (a_buf[here, :].astype(F32) * (spatial.astype(F32) + bias)).astype(BF16)
            mixed = jnp.dot(gated, w_out[...], preferred_element_type=F32) + as_row(b_out)
            o_buf[slot, here, :] = (x_buf[slot, here, :].astype(F32) + mixed).astype(BF16)

            @pl.when(step > 0)
            def _():
                send_tile(slot, lax.rem(home + step, tiles))

    send_home(own - 1)

    for off in range(1, n_seq):
        dev = lax.rem(me + off, n_seq)
        pltpu.make_async_copy(x_hbm.at[pl.ds(0, own)], x_hbm.at[pl.ds(0, own)], in_send.at[off]).wait()
    sent = o_buf.at[:, pl.ds(0, rows * (n_seq - 1))]
    pltpu.make_async_copy(sent, sent, out_send.at[0]).wait()
    for dev in range(n_seq):
        part = out_ref.at[pl.ds(dev * own, own)]
        pltpu.make_async_copy(part, part, out_recv.at[dev]).wait()


def solution(mesh):
    row_spec = P("data", "seq", None)
    vec_spec = P(None)
    mat_spec = P(None, None)
    in_specs = (row_spec, vec_spec, vec_spec, mat_spec, vec_spec, vec_spec, vec_spec, mat_spec, vec_spec, mat_spec, vec_spec)
    n_seq = mesh.shape["seq"]

    def per_device(patches, ln1_gain, ln1_bias, w_in, b_in, ln2_gain, ln2_bias, w_spatial, b_spatial, w_out, b_out):
        operands = (patches, ln1_gain, ln1_bias, w_in, b_in, ln2_gain, ln2_bias, w_spatial, b_spatial, w_out, b_out)
        images, rows, dim = patches.shape
        own = images // n_seq
        total = rows * n_seq
        half_dim = w_out.shape[0]
        hbm = pl.BlockSpec(memory_space=pltpu.HBM)
        vec = lambda ref: pltpu.VMEM(ref.shape, ref.dtype)
        return pl.pallas_call(
            functools.partial(block_kernel, n_seq, "seq"),
            out_shape=pltpu.VMEM(patches.shape, BF16),
            in_specs=[hbm] * 11,
            out_specs=pl.BlockSpec(memory_space=pltpu.VMEM),
            scratch_shapes=[
                pltpu.VMEM((own, total, dim), BF16),
                pltpu.VMEM((own, total, dim), BF16),
                pltpu.VMEM((total, half_dim), BF16),
                pltpu.VMEM((total, half_dim), BF16),
                *[vec(v) for v in operands[1:]],
                pltpu.VMEM(w_spatial.shape, BF16),
                pltpu.VMEM((total, 128), F32),
                pltpu.SemaphoreType.DMA((n_seq,)),
                pltpu.SemaphoreType.DMA((own,)),
                pltpu.SemaphoreType.DMA((1,)),
                pltpu.SemaphoreType.DMA((n_seq,)),
                pltpu.SemaphoreType.DMA((10,)),
            ],
            compiler_params=pltpu.CompilerParams(
                collective_id=0, has_side_effects=True, vmem_limit_bytes=48 * 1024 * 1024
            ),
            name="gmlp_block",
        )(*[pltpu.with_memory_space_constraint(v, pltpu.HBM) for v in operands])

    return jax.shard_map(per_device, mesh=mesh, in_specs=in_specs, out_specs=row_spec, check_vma=False)
```

```python
import functools

import jax
import jax.numpy as jnp
from jax import lax
from jax.experimental import pallas as pl
from jax.experimental.pallas import tpu as pltpu
from jax.sharding import PartitionSpec as P

LN_EPS = 1e-6
MESH = pl.DeviceIdType.MESH
F32 = jnp.float32
BF16 = jnp.bfloat16
TILE = 256
NEAR = (1, 3)
FAR = (2,)


def layer_norm(values, gain_vec, offset):
    values_f = values.astype(F32)
    mean_val = jnp.mean(values_f, axis=-1, keepdims=True)
    centered = values_f - mean_val
    var_val = jnp.mean(centered * centered, axis=-1, keepdims=True)
    return (centered * lax.rsqrt(var_val + LN_EPS) * gain_vec + offset).astype(BF16)


def as_row(ref):
    return ref[...].reshape(1, ref.shape[0])


def gelu(hidden):
    half = 0.5 * hidden
    return (half + half * lax.erf(hidden * (0.5 ** 0.5))).astype(BF16)


def block_kernel(n_seq, axis, x_hbm, ln1_gain_hbm, ln1_bias_hbm, w_in_hbm, b_in_hbm, ln2_gain_hbm, ln2_bias_hbm, w_spatial_hbm,
                 b_spatial_hbm, w_out_hbm, b_out_hbm, out_ref, x_buf, o_buf, n_buf, a_buf, ln1_gain, ln1_bias, w_in, b_in, ln2_gain,
                 ln2_bias, w_spatial, b_spatial, w_out, b_out, w_mix, bias_col, x_stage, far_sem, in_send, in_recv, out_send, out_recv, w_sem):
    me = lax.axis_index(axis)
    images, rows, _ = x_hbm.shape
    own = images // n_seq
    patches = rows * n_seq
    half_dim = w_out.shape[0]
    per_tile = TILE // rows
    tiles = patches // TILE
    groups = tiles
    home = me // per_tile

    def block_rows(dev):
        return pl.ds(pl.multiple_of(dev * rows, rows), rows)

    def across(group, part):
        return lax.rem(home + group, groups) * per_tile + part

    def send_block(src, dev, slot, sem):
        pltpu.make_async_remote_copy(
            src_ref=src,
            dst_ref=x_buf.at[slot, block_rows(me)],
            send_sem=sem,
            recv_sem=in_recv.at[slot],
            device_id={axis: dev},
            device_id_type=MESH,
        ).start()

    stage = [pltpu.make_async_copy(x_hbm.at[dev * own], x_stage.at[dev], w_sem.at[dev]) for dev in range(n_seq)]
    for load in stage:
        load.start()

    barrier = pltpu.get_barrier_semaphore()
    near = [across(0, lax.rem(me + step, per_tile)) for step in range(1, per_tile)]
    near += [across(group, part) for group in NEAR for part in range(per_tile)]
    far = [across(group, part) for group in FAR for part in range(per_tile)]
    for dev in near:
        pl.semaphore_signal(barrier, inc=1, device_id={axis: dev}, device_id_type=MESH)
    pl.semaphore_wait(barrier, len(near))

    pl.semaphore_signal(far_sem, inc=1, device_id={axis: across(1, lax.rem(me, per_tile))}, device_id_type=MESH)
    for load in stage:
        load.wait()
    for dev in near:
        send_block(x_stage.at[dev], dev, 0, in_send.at[0])
    pltpu.make_async_copy(x_hbm.at[me * own], x_buf.at[0, block_rows(me)], in_recv.at[0]).start()
    pl.semaphore_wait(far_sem, 1)
    for dev in far:
        send_block(x_stage.at[dev], dev, 0, in_send.at[0])

    @pl.loop(1, own)
    def _(slot):
        for dev in near + far:
            send_block(x_hbm.at[dev * own + slot], dev, slot, in_send.at[1])
        pltpu.make_async_copy(x_hbm.at[me * own + slot], x_buf.at[slot, block_rows(me)], in_recv.at[slot]).start()

    operands = [
        (b_spatial_hbm, b_spatial), (w_spatial_hbm, w_spatial), (ln1_gain_hbm, ln1_gain), (ln1_bias_hbm, ln1_bias), (w_in_hbm, w_in),
        (b_in_hbm, b_in), (ln2_gain_hbm, ln2_gain), (ln2_bias_hbm, ln2_bias), (w_out_hbm, w_out), (b_out_hbm, b_out),
    ]
    loads = [pltpu.make_async_copy(src, dst, w_sem.at[n_seq + k]) for k, (src, dst) in enumerate(operands)]
    for load in loads:
        load.start()
    loads[0].wait()
    for first in range(0, patches, 128):
        lane_bias = jnp.broadcast_to(b_spatial[first:first + 128].reshape(1, 128), (128, 128))
        bias_col[first:first + 128, :] = lane_bias.T
    loads[1].wait()

    @pl.loop(0, patches // TILE)
    def _(step):
        out_rows = pl.ds(pl.multiple_of(step * TILE, TILE), TILE)
        for first in range(0, patches, TILE):
            w_mix[out_rows, first:first + TILE] = w_spatial[first:first + TILE, out_rows].T

    for load in loads[2:]:
        load.wait()

    def send_tile(slot, tile):
        for part in range(per_tile):
            dev = tile * per_tile + part
            pltpu.make_async_remote_copy(
                src_ref=o_buf.at[slot, block_rows(dev)],
                dst_ref=out_ref.at[me * own + slot],
                send_sem=out_send.at[0],
                recv_sem=out_recv.at[me],
                device_id={axis: dev},
                device_id_type=MESH,
            ).start()

    def send_home(slot):
        pltpu.make_async_copy(o_buf.at[slot, block_rows(me)], out_ref.at[me * own + slot], out_recv.at[me]).start()
        for step in range(1, per_tile):
            dev = home * per_tile + lax.rem(me + step, per_tile)
            pltpu.make_async_remote_copy(
                src_ref=o_buf.at[slot, block_rows(dev)],
                dst_ref=out_ref.at[me * own + slot],
                send_sem=out_send.at[0],
                recv_sem=out_recv.at[me],
                device_id={axis: dev},
                device_id_type=MESH,
            ).start()

    @pl.loop(0, own)
    def _(slot):
        pltpu.make_async_copy(x_buf.at[slot], x_buf.at[slot], in_recv.at[slot]).wait()

        @pl.loop(0, tiles)
        def _(tile):
            here = pl.ds(pl.multiple_of(tile * TILE, TILE), TILE)
            normed = layer_norm(x_buf[slot, here, :], as_row(ln1_gain), as_row(ln1_bias))
            gate = []
            for first in range(0, 2 * half_dim, 256):
                cols = slice(first, first + 256)
                hidden = jnp.dot(normed, w_in[:, cols], preferred_element_type=F32) + b_in[cols].reshape(1, 256)
                act = gelu(hidden)
                if first < half_dim:
                    a_buf[here, cols] = act
                else:
                    gate.append(act)
            gate = jnp.concatenate(gate, axis=1)
            n_buf[here, :] = layer_norm(gate, as_row(ln2_gain), as_row(ln2_bias))

        @pl.when(slot > 0)
        def _():
            send_home(slot - 1)

        previous = None
        for group in FAR + NEAR + (0,):
            tile = lax.rem(home + group, groups)
            here = pl.ds(pl.multiple_of(tile * TILE, TILE), TILE)
            spatial = jnp.dot(w_mix[here, :], n_buf[...], preferred_element_type=F32).astype(BF16)
            bias = jnp.tile(bias_col[here, :], (1, half_dim // 128))
            gated = (a_buf[here, :].astype(F32) * (spatial.astype(F32) + bias)).astype(BF16)
            mixed = jnp.dot(gated, w_out[...], preferred_element_type=F32) + as_row(b_out)
            o_buf[slot, here, :] = (x_buf[slot, here, :].astype(F32) + mixed).astype(BF16)
            if previous is not None:
                send_tile(slot, previous)
            previous = tile

    send_home(own - 1)

    first_sent = x_stage.at[pl.ds(0, n_seq - 1)]
    pltpu.make_async_copy(first_sent, first_sent, in_send.at[0]).wait()
    rest_sent = x_buf.at[pl.ds(0, own - 1), pl.ds(0, rows * (n_seq - 1))]
    pltpu.make_async_copy(rest_sent, rest_sent, in_send.at[1]).wait()
    sent = o_buf.at[:, pl.ds(0, rows * (n_seq - 1))]
    pltpu.make_async_copy(sent, sent, out_send.at[0]).wait()
    for dev in range(n_seq):
        part = out_ref.at[pl.ds(dev * own, own)]
        pltpu.make_async_copy(part, part, out_recv.at[dev]).wait()


def solution(mesh):
    row_spec = P("data", "seq", None)
    vec_spec = P(None)
    mat_spec = P(None, None)
    in_specs = (row_spec, vec_spec, vec_spec, mat_spec, vec_spec, vec_spec, vec_spec, mat_spec, vec_spec, mat_spec, vec_spec)
    n_seq = mesh.shape["seq"]

    def per_device(patches, ln1_gain, ln1_bias, w_in, b_in, ln2_gain, ln2_bias, w_spatial, b_spatial, w_out, b_out):
        operands = (patches, ln1_gain, ln1_bias, w_in, b_in, ln2_gain, ln2_bias, w_spatial, b_spatial, w_out, b_out)
        images, rows, dim = patches.shape
        own = images // n_seq
        total = rows * n_seq
        half_dim = w_out.shape[0]
        hbm = pl.BlockSpec(memory_space=pltpu.HBM)
        vec = lambda ref: pltpu.VMEM(ref.shape, ref.dtype)
        return pl.pallas_call(
            functools.partial(block_kernel, n_seq, "seq"),
            out_shape=pltpu.VMEM(patches.shape, BF16),
            in_specs=[hbm] * 11,
            out_specs=pl.BlockSpec(memory_space=pltpu.VMEM),
            scratch_shapes=[
                pltpu.VMEM((own, total, dim), BF16),
                pltpu.VMEM((own, total, dim), BF16),
                pltpu.VMEM((total, half_dim), BF16),
                pltpu.VMEM((total, half_dim), BF16),
                *[vec(v) for v in operands[1:]],
                pltpu.VMEM(w_spatial.shape, BF16),
                pltpu.VMEM((total, 128), F32),
                pltpu.VMEM((n_seq, rows, dim), BF16),
                pltpu.SemaphoreType.REGULAR,
                pltpu.SemaphoreType.DMA((2,)),
                pltpu.SemaphoreType.DMA((own,)),
                pltpu.SemaphoreType.DMA((1,)),
                pltpu.SemaphoreType.DMA((n_seq,)),
                pltpu.SemaphoreType.DMA((n_seq + 10,)),
            ],
            compiler_params=pltpu.CompilerParams(
                collective_id=0, has_side_effects=True, vmem_limit_bytes=48 * 1024 * 1024
            ),
            name="gmlp_block",
        )(*[pltpu.with_memory_space_constraint(v, pltpu.HBM) for v in operands])

    return jax.shard_map(per_device, mesh=mesh, in_specs=in_specs, out_specs=row_spec, check_vma=False)
```

```python
import functools

import jax
import jax.numpy as jnp
from jax import lax
from jax.experimental import pallas as pl
from jax.experimental.pallas import tpu as pltpu
from jax.sharding import PartitionSpec as P

LN_EPS = 1e-6
MESH = pl.DeviceIdType.MESH
F32 = jnp.float32
BF16 = jnp.bfloat16
TILE = 256
NEAR = (1, 3)
FAR = (2,)


def layer_norm(values, gain_vec, offset):
    values_f = values.astype(F32)
    mean_val = jnp.mean(values_f, axis=-1, keepdims=True)
    centered = values_f - mean_val
    var_val = jnp.mean(centered * centered, axis=-1, keepdims=True)
    return (centered * lax.rsqrt(var_val + LN_EPS) * gain_vec + offset).astype(BF16)


def as_row(ref):
    return ref[...].reshape(1, ref.shape[0])


def gelu(hidden):
    half = 0.5 * hidden
    return (half + half * lax.erf(hidden * (0.5 ** 0.5))).astype(BF16)


def block_kernel(n_seq, axis, x_hbm, ln1_gain_hbm, ln1_bias_hbm, w_in_hbm, b_in_hbm, ln2_gain_hbm, ln2_bias_hbm, w_spatial_hbm,
                 b_spatial_hbm, w_out_hbm, b_out_hbm, out_ref, x_buf, o_buf, n_buf, a_buf, ln1_gain, ln1_bias, w_in, b_in, ln2_gain,
                 ln2_bias, w_spatial, b_spatial, w_out, b_out, w_mix, bias_col, x_stage, far_sem, in_send, in_recv, out_send, out_recv, w_sem):
    me = lax.axis_index(axis)
    images, rows, _ = x_hbm.shape
    own = images // n_seq
    patches = rows * n_seq
    half_dim = w_out.shape[0]
    per_tile = TILE // rows
    tiles = patches // TILE
    groups = tiles
    home = me // per_tile

    def block_rows(dev):
        return pl.ds(pl.multiple_of(dev * rows, rows), rows)

    def across(group, part):
        return lax.rem(home + group, groups) * per_tile + part

    def turn(step, shift):
        return 1 + lax.rem(groups // 2 - 1 + step + lax.rem(shift, per_tile), groups - 1)

    def send_block(src, dev, slot, sem):
        pltpu.make_async_remote_copy(
            src_ref=src,
            dst_ref=x_buf.at[slot, block_rows(me)],
            send_sem=sem,
            recv_sem=in_recv.at[slot],
            device_id={axis: dev},
            device_id_type=MESH,
        ).start()

    stage = [pltpu.make_async_copy(x_hbm.at[dev * own], x_stage.at[dev], w_sem.at[dev]) for dev in range(n_seq)]
    for load in stage:
        load.start()

    barrier = pltpu.get_barrier_semaphore()
    near = [across(0, lax.rem(me + step, per_tile)) for step in range(1, per_tile)]
    near += [across(group, part) for group in NEAR for part in range(per_tile)]
    far = [across(group, part) for group in FAR for part in range(per_tile)]
    for dev in near:
        pl.semaphore_signal(barrier, inc=1, device_id={axis: dev}, device_id_type=MESH)
    pl.semaphore_wait(barrier, len(near))

    pl.semaphore_signal(far_sem, inc=1, device_id={axis: across(1, lax.rem(me, per_tile))}, device_id_type=MESH)
    for load in stage:
        load.wait()
    for dev in near:
        send_block(x_stage.at[dev], dev, 0, in_send.at[0])
    pltpu.make_async_copy(x_hbm.at[me * own], x_buf.at[0, block_rows(me)], in_recv.at[0]).start()
    pl.semaphore_wait(far_sem, 1)
    for dev in far:
        send_block(x_stage.at[dev], dev, 0, in_send.at[0])

    @pl.loop(1, own)
    def _(slot):
        for dev in near[:per_tile - 1] + [across(turn(step, me), part) for step in range(groups - 1) for part in range(per_tile)]:
            send_block(x_hbm.at[dev * own + slot], dev, slot, in_send.at[1])
        pltpu.make_async_copy(x_hbm.at[me * own + slot], x_buf.at[slot, block_rows(me)], in_recv.at[slot]).start()

    operands = [
        (b_spatial_hbm, b_spatial), (w_spatial_hbm, w_spatial), (ln1_gain_hbm, ln1_gain), (ln1_bias_hbm, ln1_bias), (w_in_hbm, w_in),
        (b_in_hbm, b_in), (ln2_gain_hbm, ln2_gain), (ln2_bias_hbm, ln2_bias), (w_out_hbm, w_out), (b_out_hbm, b_out),
    ]
    loads = [pltpu.make_async_copy(src, dst, w_sem.at[n_seq + k]) for k, (src, dst) in enumerate(operands)]
    for load in loads:
        load.start()
    loads[0].wait()
    for first in range(0, patches, 128):
        lane_bias = jnp.broadcast_to(b_spatial[first:first + 128].reshape(1, 128), (128, 128))
        bias_col[first:first + 128, :] = lane_bias.T
    loads[1].wait()

    @pl.loop(0, patches // TILE)
    def _(step):
        out_rows = pl.ds(pl.multiple_of(step * TILE, TILE), TILE)
        for first in range(0, patches, TILE):
            w_mix[out_rows, first:first + TILE] = w_spatial[first:first + TILE, out_rows].T

    for load in loads[2:]:
        load.wait()

    def send_tile(slot, tile):
        for part in range(per_tile):
            dev = tile * per_tile + part
            pltpu.make_async_remote_copy(
                src_ref=o_buf.at[slot, block_rows(dev)],
                dst_ref=out_ref.at[me * own + slot],
                send_sem=out_send.at[0],
                recv_sem=out_recv.at[me],
                device_id={axis: dev},
                device_id_type=MESH,
            ).start()

    def send_home(slot):
        pltpu.make_async_copy(o_buf.at[slot, block_rows(me)], out_ref.at[me * own + slot], out_recv.at[me]).start()
        for step in range(1, per_tile):
            dev = home * per_tile + lax.rem(me + step, per_tile)
            pltpu.make_async_remote_copy(
                src_ref=o_buf.at[slot, block_rows(dev)],
                dst_ref=out_ref.at[me * own + slot],
                send_sem=out_send.at[0],
                recv_sem=out_recv.at[me],
                device_id={axis: dev},
                device_id_type=MESH,
            ).start()

    @pl.loop(0, own)
    def _(slot):
        pltpu.make_async_copy(x_buf.at[slot], x_buf.at[slot], in_recv.at[slot]).wait()

        @pl.loop(0, tiles)
        def _(tile):
            here = pl.ds(pl.multiple_of(tile * TILE, TILE), TILE)
            normed = layer_norm(x_buf[slot, here, :], as_row(ln1_gain), as_row(ln1_bias))
            gate = []
            for first in range(0, 2 * half_dim, 256):
                cols = slice(first, first + 256)
                hidden = jnp.dot(normed, w_in[:, cols], preferred_element_type=F32) + b_in[cols].reshape(1, 256)
                act = gelu(hidden)
                if first < half_dim:
                    a_buf[here, cols] = act
                else:
                    gate.append(act)
            gate = jnp.concatenate(gate, axis=1)
            n_buf[here, :] = layer_norm(gate, as_row(ln2_gain), as_row(ln2_bias))

        @pl.when(slot > 0)
        def _():
            send_home(slot - 1)

        previous = None
        for step in range(groups):
            group = turn(step, jnp.where(slot < own - 1, me, 0)) if step < groups - 1 else 0
            tile = lax.rem(home + group, groups)
            here = pl.ds(pl.multiple_of(tile * TILE, TILE), TILE)
            spatial = jnp.dot(w_mix[here, :], n_buf[...], preferred_element_type=F32).astype(BF16)
            bias = jnp.tile(bias_col[here, :], (1, half_dim // 128))
            gated = (a_buf[here, :].astype(F32) * (spatial.astype(F32) + bias)).astype(BF16)
            mixed = jnp.dot(gated, w_out[...], preferred_element_type=F32) + as_row(b_out)
            o_buf[slot, here, :] = (x_buf[slot, here, :].astype(F32) + mixed).astype(BF16)
            if previous is not None:
                send_tile(slot, previous)
            previous = tile

    send_home(own - 1)

    first_sent = x_stage.at[pl.ds(0, n_seq - 1)]
    pltpu.make_async_copy(first_sent, first_sent, in_send.at[0]).wait()
    rest_sent = x_buf.at[pl.ds(0, own - 1), pl.ds(0, rows * (n_seq - 1))]
    pltpu.make_async_copy(rest_sent, rest_sent, in_send.at[1]).wait()
    sent = o_buf.at[:, pl.ds(0, rows * (n_seq - 1))]
    pltpu.make_async_copy(sent, sent, out_send.at[0]).wait()
    for dev in range(n_seq):
        part = out_ref.at[pl.ds(dev * own, own)]
        pltpu.make_async_copy(part, part, out_recv.at[dev]).wait()


def solution(mesh):
    row_spec = P("data", "seq", None)
    vec_spec = P(None)
    mat_spec = P(None, None)
    in_specs = (row_spec, vec_spec, vec_spec, mat_spec, vec_spec, vec_spec, vec_spec, mat_spec, vec_spec, mat_spec, vec_spec)
    n_seq = mesh.shape["seq"]

    def per_device(patches, ln1_gain, ln1_bias, w_in, b_in, ln2_gain, ln2_bias, w_spatial, b_spatial, w_out, b_out):
        operands = (patches, ln1_gain, ln1_bias, w_in, b_in, ln2_gain, ln2_bias, w_spatial, b_spatial, w_out, b_out)
        images, rows, dim = patches.shape
        own = images // n_seq
        total = rows * n_seq
        half_dim = w_out.shape[0]
        hbm = pl.BlockSpec(memory_space=pltpu.HBM)
        vec = lambda ref: pltpu.VMEM(ref.shape, ref.dtype)
        return pl.pallas_call(
            functools.partial(block_kernel, n_seq, "seq"),
            out_shape=pltpu.VMEM(patches.shape, BF16),
            in_specs=[hbm] * 11,
            out_specs=pl.BlockSpec(memory_space=pltpu.VMEM),
            scratch_shapes=[
                pltpu.VMEM((own, total, dim), BF16),
                pltpu.VMEM((own, total, dim), BF16),
                pltpu.VMEM((total, half_dim), BF16),
                pltpu.VMEM((total, half_dim), BF16),
                *[vec(v) for v in operands[1:]],
                pltpu.VMEM(w_spatial.shape, BF16),
                pltpu.VMEM((total, 128), F32),
                pltpu.VMEM((n_seq, rows, dim), BF16),
                pltpu.SemaphoreType.REGULAR,
                pltpu.SemaphoreType.DMA((2,)),
                pltpu.SemaphoreType.DMA((own,)),
                pltpu.SemaphoreType.DMA((1,)),
                pltpu.SemaphoreType.DMA((n_seq,)),
                pltpu.SemaphoreType.DMA((n_seq + 10,)),
            ],
            compiler_params=pltpu.CompilerParams(
                collective_id=0, has_side_effects=True, vmem_limit_bytes=48 * 1024 * 1024
            ),
            name="gmlp_block",
        )(*[pltpu.with_memory_space_constraint(v, pltpu.HBM) for v in operands])

    return jax.shard_map(per_device, mesh=mesh, in_specs=in_specs, out_specs=row_spec, check_vma=False)
```

```python
import functools

import jax
import jax.numpy as jnp
from jax import lax
from jax.experimental import pallas as pl
from jax.experimental.pallas import tpu as pltpu
from jax.sharding import PartitionSpec as P

LN_EPS = 1e-6
MESH = pl.DeviceIdType.MESH
F32 = jnp.float32
BF16 = jnp.bfloat16
TILE = 256
NEAR = (1, 3)
FAR = (2,)


def layer_norm(values, gain_vec, offset):
    values_f = values.astype(F32)
    mean_val = jnp.mean(values_f, axis=-1, keepdims=True)
    centered = values_f - mean_val
    var_val = jnp.mean(centered * centered, axis=-1, keepdims=True)
    return (centered * lax.rsqrt(var_val + LN_EPS) * gain_vec + offset).astype(BF16)


def as_row(ref):
    return ref[...].reshape(1, ref.shape[0])


def gelu(hidden):
    half = 0.5 * hidden
    return (half + half * lax.erf(hidden * (0.5 ** 0.5))).astype(BF16)


def block_kernel(n_seq, axis, x_hbm, ln1_gain_hbm, ln1_bias_hbm, w_in_hbm, b_in_hbm, ln2_gain_hbm, ln2_bias_hbm, w_spatial_hbm,
                 b_spatial_hbm, w_out_hbm, b_out_hbm, out_ref, x_buf, o_buf, n_buf, a_buf, ln1_gain, ln1_bias, w_in, b_in, ln2_gain,
                 ln2_bias, w_spatial, b_spatial, w_out, b_out, w_mix, bias_col, x_stage, far_sem, in_send, in_recv, out_send, out_recv, w_sem):
    me = lax.axis_index(axis)
    images, rows, _ = x_hbm.shape
    own = images // n_seq
    patches = rows * n_seq
    half_dim = w_out.shape[0]
    per_tile = TILE // rows
    tiles = patches // TILE
    groups = tiles
    home = me // per_tile

    def block_rows(dev):
        return pl.ds(pl.multiple_of(dev * rows, rows), rows)

    def across(group, part):
        return lax.rem(home + group, groups) * per_tile + part

    def send_block(src, dev, slot, sem):
        pltpu.make_async_remote_copy(
            src_ref=src,
            dst_ref=x_buf.at[slot, block_rows(me)],
            send_sem=sem,
            recv_sem=in_recv.at[slot],
            device_id={axis: dev},
            device_id_type=MESH,
        ).start()

    barrier = pltpu.get_barrier_semaphore()
    near = [across(0, lax.rem(me + step, per_tile)) for step in range(1, per_tile)]
    near += [across(group, part) for group in NEAR for part in range(per_tile)]
    far = [across(group, part) for group in FAR for part in range(per_tile)]
    for dev in near:
        pl.semaphore_signal(barrier, inc=1, device_id={axis: dev}, device_id_type=MESH)
    stage = [pltpu.make_async_copy(x_hbm.at[dev * own], x_stage.at[dev], w_sem.at[dev]) for dev in range(n_seq)]
    for load in stage:
        load.start()

    pl.semaphore_wait(barrier, len(near))

    pl.semaphore_signal(far_sem, inc=1, device_id={axis: across(1, lax.rem(me, per_tile))}, device_id_type=MESH)
    for load in stage:
        load.wait()
    for dev in near:
        send_block(x_stage.at[dev], dev, 0, in_send.at[0])
    pltpu.make_async_copy(x_hbm.at[me * own], x_buf.at[0, block_rows(me)], in_recv.at[0]).start()
    pl.semaphore_wait(far_sem, 1)
    for dev in far:
        send_block(x_stage.at[dev], dev, 0, in_send.at[0])

    @pl.loop(1, own)
    def _(slot):
        for dev in near + far:
            send_block(x_hbm.at[dev * own + slot], dev, slot, in_send.at[1])
        pltpu.make_async_copy(x_hbm.at[me * own + slot], x_buf.at[slot, block_rows(me)], in_recv.at[slot]).start()

    operands = [
        (b_spatial_hbm, b_spatial), (w_spatial_hbm, w_spatial), (ln1_gain_hbm, ln1_gain), (ln1_bias_hbm, ln1_bias), (w_in_hbm, w_in),
        (b_in_hbm, b_in), (ln2_gain_hbm, ln2_gain), (ln2_bias_hbm, ln2_bias), (w_out_hbm, w_out), (b_out_hbm, b_out),
    ]
    loads = [pltpu.make_async_copy(src, dst, w_sem.at[n_seq + k]) for k, (src, dst) in enumerate(operands)]
    for load in loads:
        load.start()
    loads[0].wait()
    for first in range(0, patches, 128):
        lane_bias = jnp.broadcast_to(b_spatial[first:first + 128].reshape(1, 128), (128, 128))
        bias_col[first:first + 128, :] = lane_bias.T
    loads[1].wait()

    @pl.loop(0, patches // TILE)
    def _(step):
        out_rows = pl.ds(pl.multiple_of(step * TILE, TILE), TILE)
        for first in range(0, patches, TILE):
            w_mix[out_rows, first:first + TILE] = w_spatial[first:first + TILE, out_rows].T

    for load in loads[2:]:
        load.wait()

    def send_tile(slot, tile):
        for part in reversed(range(per_tile)):
            dev = tile * per_tile + part
            pltpu.make_async_remote_copy(
                src_ref=o_buf.at[slot, block_rows(dev)],
                dst_ref=out_ref.at[me * own + slot],
                send_sem=out_send.at[0],
                recv_sem=out_recv.at[me],
                device_id={axis: dev},
                device_id_type=MESH,
            ).start()

    def send_home(slot):
        pltpu.make_async_copy(o_buf.at[slot, block_rows(me)], out_ref.at[me * own + slot], out_recv.at[me]).start()
        for step in range(1, per_tile):
            dev = home * per_tile + lax.rem(me + step, per_tile)
            pltpu.make_async_remote_copy(
                src_ref=o_buf.at[slot, block_rows(dev)],
                dst_ref=out_ref.at[me * own + slot],
                send_sem=out_send.at[0],
                recv_sem=out_recv.at[me],
                device_id={axis: dev},
                device_id_type=MESH,
            ).start()

    @pl.loop(0, own)
    def _(slot):
        pltpu.make_async_copy(x_buf.at[slot], x_buf.at[slot], in_recv.at[slot]).wait()

        @pl.loop(0, tiles)
        def _(tile):
            here = pl.ds(pl.multiple_of(tile * TILE, TILE), TILE)
            normed = layer_norm(x_buf[slot, here, :], as_row(ln1_gain), as_row(ln1_bias))
            gate = []
            for first in range(0, 2 * half_dim, 256):
                cols = slice(first, first + 256)
                hidden = jnp.dot(normed, w_in[:, cols], preferred_element_type=F32) + b_in[cols].reshape(1, 256)
                act = gelu(hidden)
                if first < half_dim:
                    a_buf[here, cols] = act
                else:
                    gate.append(act)
            gate = jnp.concatenate(gate, axis=1)
            n_buf[here, :] = layer_norm(gate, as_row(ln2_gain), as_row(ln2_bias))

        @pl.when(slot > 0)
        def _():
            send_home(slot - 1)

        previous = None
        for group in FAR + NEAR + (0,):
            tile = lax.rem(home + group, groups)
            here = pl.ds(pl.multiple_of(tile * TILE, TILE), TILE)
            spatial = jnp.dot(w_mix[here, :], n_buf[...], preferred_element_type=F32).astype(BF16)
            bias = jnp.tile(bias_col[here, :], (1, half_dim // 128))
            gated = (a_buf[here, :].astype(F32) * (spatial.astype(F32) + bias)).astype(BF16)
            mixed = jnp.dot(gated, w_out[...], preferred_element_type=F32) + as_row(b_out)
            o_buf[slot, here, :] = (x_buf[slot, here, :].astype(F32) + mixed).astype(BF16)
            if previous is not None:
                send_tile(slot, previous)
            previous = tile

    send_home(own - 1)

    first_sent = x_stage.at[pl.ds(0, n_seq - 1)]
    pltpu.make_async_copy(first_sent, first_sent, in_send.at[0]).wait()
    rest_sent = x_buf.at[pl.ds(0, own - 1), pl.ds(0, rows * (n_seq - 1))]
    pltpu.make_async_copy(rest_sent, rest_sent, in_send.at[1]).wait()
    sent = o_buf.at[:, pl.ds(0, rows * (n_seq - 1))]
    pltpu.make_async_copy(sent, sent, out_send.at[0]).wait()
    for dev in range(n_seq):
        part = out_ref.at[pl.ds(dev * own, own)]
        pltpu.make_async_copy(part, part, out_recv.at[dev]).wait()


def solution(mesh):
    row_spec = P("data", "seq", None)
    vec_spec = P(None)
    mat_spec = P(None, None)
    in_specs = (row_spec, vec_spec, vec_spec, mat_spec, vec_spec, vec_spec, vec_spec, mat_spec, vec_spec, mat_spec, vec_spec)
    n_seq = mesh.shape["seq"]

    def per_device(patches, ln1_gain, ln1_bias, w_in, b_in, ln2_gain, ln2_bias, w_spatial, b_spatial, w_out, b_out):
        operands = (patches, ln1_gain, ln1_bias, w_in, b_in, ln2_gain, ln2_bias, w_spatial, b_spatial, w_out, b_out)
        images, rows, dim = patches.shape
        own = images // n_seq
        total = rows * n_seq
        half_dim = w_out.shape[0]
        hbm = pl.BlockSpec(memory_space=pltpu.HBM)
        vec = lambda ref: pltpu.VMEM(ref.shape, ref.dtype)
        return pl.pallas_call(
            functools.partial(block_kernel, n_seq, "seq"),
            out_shape=pltpu.VMEM(patches.shape, BF16),
            in_specs=[hbm] * 11,
            out_specs=pl.BlockSpec(memory_space=pltpu.VMEM),
            scratch_shapes=[
                pltpu.VMEM((own, total, dim), BF16),
                pltpu.VMEM((own, total, dim), BF16),
                pltpu.VMEM((total, half_dim), BF16),
                pltpu.VMEM((total, half_dim), BF16),
                *[vec(v) for v in operands[1:]],
                pltpu.VMEM(w_spatial.shape, BF16),
                pltpu.VMEM((total, 128), F32),
                pltpu.VMEM((n_seq, rows, dim), BF16),
                pltpu.SemaphoreType.REGULAR,
                pltpu.SemaphoreType.DMA((2,)),
                pltpu.SemaphoreType.DMA((own,)),
                pltpu.SemaphoreType.DMA((1,)),
                pltpu.SemaphoreType.DMA((n_seq,)),
                pltpu.SemaphoreType.DMA((n_seq + 10,)),
            ],
            compiler_params=pltpu.CompilerParams(
                collective_id=0, has_side_effects=True, vmem_limit_bytes=48 * 1024 * 1024
            ),
            name="gmlp_block",
        )(*[pltpu.with_memory_space_constraint(v, pltpu.HBM) for v in operands])

    return jax.shard_map(per_device, mesh=mesh, in_specs=in_specs, out_specs=row_spec, check_vma=False)
```

```python
import functools

import jax
import jax.numpy as jnp
from jax import lax
from jax.experimental import pallas as pl
from jax.experimental.pallas import tpu as pltpu
from jax.sharding import PartitionSpec as P

LN_EPS = 1e-6
MESH = pl.DeviceIdType.MESH
F32 = jnp.float32
BF16 = jnp.bfloat16
TILE = 256
NEAR = (1, 3)
FAR = (2,)
EARLY = 2


def layer_norm(values, gain_vec, offset):
    values_f = values.astype(F32)
    mean_val = jnp.mean(values_f, axis=-1, keepdims=True)
    centered = values_f - mean_val
    var_val = jnp.mean(centered * centered, axis=-1, keepdims=True)
    return (centered * lax.rsqrt(var_val + LN_EPS) * gain_vec + offset).astype(BF16)


def as_row(ref):
    return ref[...].reshape(1, ref.shape[0])


def gelu(hidden):
    half = 0.5 * hidden
    return (half + half * lax.erf(hidden * (0.5 ** 0.5))).astype(BF16)


def block_kernel(n_seq, axis, x_hbm, ln1_gain_hbm, ln1_bias_hbm, w_in_hbm, b_in_hbm, ln2_gain_hbm, ln2_bias_hbm, w_spatial_hbm,
                 b_spatial_hbm, w_out_hbm, b_out_hbm, out_ref, x_buf, o_buf, n_buf, a_buf, ln1_gain, ln1_bias, w_in, b_in, ln2_gain,
                 ln2_bias, w_spatial, b_spatial, w_out, b_out, w_mix, bias_col, x_stage, near_sem, far_sem, in_send, in_recv, out_send, out_recv, w_sem):
    me = lax.axis_index(axis)
    images, rows, _ = x_hbm.shape
    own = images // n_seq
    patches = rows * n_seq
    half_dim = w_out.shape[0]
    per_tile = TILE // rows
    tiles = patches // TILE
    groups = tiles
    home = me // per_tile

    def block_rows(dev):
        return pl.ds(pl.multiple_of(dev * rows, rows), rows)

    def across(group, part):
        return lax.rem(home + group, groups) * per_tile + part

    def send_block(src, dev, slot, sem):
        pltpu.make_async_remote_copy(
            src_ref=src,
            dst_ref=x_buf.at[slot, block_rows(me)],
            send_sem=sem,
            recv_sem=in_recv.at[slot],
            device_id={axis: dev},
            device_id_type=MESH,
        ).start()

    core = lax.rem(me, per_tile)
    mate = across(0, per_tile - 1 - core)
    side = [across(group, core) for group in NEAR]
    cross = [across(group, per_tile - 1 - core) for group in NEAR]
    far = [across(group, part) for group in FAR for part in range(per_tile)]

    barrier = pltpu.get_barrier_semaphore()
    for dev in side + [mate]:
        pl.semaphore_signal(barrier, inc=1, device_id={axis: dev}, device_id_type=MESH)
    stage = [pltpu.make_async_copy(x_hbm.at[dev * own], x_stage.at[k], w_sem.at[k]) for k, dev in enumerate(side)]
    for load in stage:
        load.start()
    pl.semaphore_wait(barrier, len(side) + 1)

    for dev in side:
        pl.semaphore_signal(near_sem, inc=1, device_id={axis: dev}, device_id_type=MESH)
    for k, dev in enumerate(side):
        stage[k].wait()
        send_block(x_stage.at[k], dev, 0, in_send.at[0])
    for slot in range(1, EARLY):
        for dev in side:
            send_block(x_hbm.at[dev * own + slot], dev, slot, in_send.at[1])
    pl.semaphore_wait(near_sem, len(side))

    pl.semaphore_signal(far_sem, inc=1, device_id={axis: mate}, device_id_type=MESH)
    for slot in range(EARLY):
        for dev in cross:
            send_block(x_hbm.at[dev * own + slot], dev, slot, in_send.at[1])
    pl.semaphore_wait(far_sem, 1)
    for slot in range(EARLY):
        for dev in far + [mate]:
            send_block(x_hbm.at[dev * own + slot], dev, slot, in_send.at[1])

    @pl.loop(EARLY, own)
    def _(slot):
        for dev in side + cross + far + [mate]:
            send_block(x_hbm.at[dev * own + slot], dev, slot, in_send.at[1])

    @pl.loop(0, own)
    def _(slot):
        pltpu.make_async_copy(x_hbm.at[me * own + slot], x_buf.at[slot, block_rows(me)], in_recv.at[slot]).start()

    operands = [
        (b_spatial_hbm, b_spatial), (w_spatial_hbm, w_spatial), (ln1_gain_hbm, ln1_gain), (ln1_bias_hbm, ln1_bias), (w_in_hbm, w_in),
        (b_in_hbm, b_in), (ln2_gain_hbm, ln2_gain), (ln2_bias_hbm, ln2_bias), (w_out_hbm, w_out), (b_out_hbm, b_out),
    ]
    loads = [pltpu.make_async_copy(src, dst, w_sem.at[len(NEAR) + k]) for k, (src, dst) in enumerate(operands)]
    for load in loads:
        load.start()
    loads[0].wait()
    for first in range(0, patches, 128):
        lane_bias = jnp.broadcast_to(b_spatial[first:first + 128].reshape(1, 128), (128, 128))
        bias_col[first:first + 128, :] = lane_bias.T
    loads[1].wait()

    @pl.loop(0, patches // TILE)
    def _(step):
        out_rows = pl.ds(pl.multiple_of(step * TILE, TILE), TILE)
        for first in range(0, patches, TILE):
            w_mix[out_rows, first:first + TILE] = w_spatial[first:first + TILE, out_rows].T

    for load in loads[2:]:
        load.wait()

    def send_tile(slot, tile):
        for part in reversed(range(per_tile)):
            dev = tile * per_tile + part
            pltpu.make_async_remote_copy(
                src_ref=o_buf.at[slot, block_rows(dev)],
                dst_ref=out_ref.at[me * own + slot],
                send_sem=out_send.at[0],
                recv_sem=out_recv.at[me],
                device_id={axis: dev},
                device_id_type=MESH,
            ).start()

    def send_home(slot):
        pltpu.make_async_copy(o_buf.at[slot, block_rows(me)], out_ref.at[me * own + slot], out_recv.at[me]).start()
        for step in range(1, per_tile):
            dev = home * per_tile + lax.rem(me + step, per_tile)
            pltpu.make_async_remote_copy(
                src_ref=o_buf.at[slot, block_rows(dev)],
                dst_ref=out_ref.at[me * own + slot],
                send_sem=out_send.at[0],
                recv_sem=out_recv.at[me],
                device_id={axis: dev},
                device_id_type=MESH,
            ).start()

    @pl.loop(0, own)
    def _(slot):
        pltpu.make_async_copy(x_buf.at[slot], x_buf.at[slot], in_recv.at[slot]).wait()

        @pl.loop(0, tiles)
        def _(tile):
            here = pl.ds(pl.multiple_of(tile * TILE, TILE), TILE)
            normed = layer_norm(x_buf[slot, here, :], as_row(ln1_gain), as_row(ln1_bias))
            gate = []
            for first in range(0, 2 * half_dim, 256):
                cols = slice(first, first + 256)
                hidden = jnp.dot(normed, w_in[:, cols], preferred_element_type=F32) + b_in[cols].reshape(1, 256)
                act = gelu(hidden)
                if first < half_dim:
                    a_buf[here, cols] = act
                else:
                    gate.append(act)
            gate = jnp.concatenate(gate, axis=1)
            n_buf[here, :] = layer_norm(gate, as_row(ln2_gain), as_row(ln2_bias))

        @pl.when(slot > 0)
        def _():
            send_home(slot - 1)

        previous = None
        for group in FAR + NEAR + (0,):
            tile = lax.rem(home + group, groups)
            here = pl.ds(pl.multiple_of(tile * TILE, TILE), TILE)
            spatial = jnp.dot(w_mix[here, :], n_buf[...], preferred_element_type=F32).astype(BF16)
            bias = jnp.tile(bias_col[here, :], (1, half_dim // 128))
            gated = (a_buf[here, :].astype(F32) * (spatial.astype(F32) + bias)).astype(BF16)
            mixed = jnp.dot(gated, w_out[...], preferred_element_type=F32) + as_row(b_out)
            o_buf[slot, here, :] = (x_buf[slot, here, :].astype(F32) + mixed).astype(BF16)
            if previous is not None:
                send_tile(slot, previous)
            previous = tile

    send_home(own - 1)

    pltpu.make_async_copy(x_stage, x_stage, in_send.at[0]).wait()
    rest_sent = [x_buf.at[pl.ds(1, own - 1), pl.ds(0, rows * (n_seq - 1))], x_buf.at[0, pl.ds(0, rows * (n_seq - 1 - len(NEAR)))]]
    for part in rest_sent:
        pltpu.make_async_copy(part, part, in_send.at[1]).wait()
    sent = o_buf.at[:, pl.ds(0, rows * (n_seq - 1))]
    pltpu.make_async_copy(sent, sent, out_send.at[0]).wait()
    for dev in range(n_seq):
        part = out_ref.at[pl.ds(dev * own, own)]
        pltpu.make_async_copy(part, part, out_recv.at[dev]).wait()


def solution(mesh):
    row_spec = P("data", "seq", None)
    vec_spec = P(None)
    mat_spec = P(None, None)
    in_specs = (row_spec, vec_spec, vec_spec, mat_spec, vec_spec, vec_spec, vec_spec, mat_spec, vec_spec, mat_spec, vec_spec)
    n_seq = mesh.shape["seq"]

    def per_device(patches, ln1_gain, ln1_bias, w_in, b_in, ln2_gain, ln2_bias, w_spatial, b_spatial, w_out, b_out):
        operands = (patches, ln1_gain, ln1_bias, w_in, b_in, ln2_gain, ln2_bias, w_spatial, b_spatial, w_out, b_out)
        images, rows, dim = patches.shape
        own = images // n_seq
        total = rows * n_seq
        half_dim = w_out.shape[0]
        hbm = pl.BlockSpec(memory_space=pltpu.HBM)
        vec = lambda ref: pltpu.VMEM(ref.shape, ref.dtype)
        return pl.pallas_call(
            functools.partial(block_kernel, n_seq, "seq"),
            out_shape=pltpu.VMEM(patches.shape, BF16),
            in_specs=[hbm] * 11,
            out_specs=pl.BlockSpec(memory_space=pltpu.VMEM),
            scratch_shapes=[
                pltpu.VMEM((own, total, dim), BF16),
                pltpu.VMEM((own, total, dim), BF16),
                pltpu.VMEM((total, half_dim), BF16),
                pltpu.VMEM((total, half_dim), BF16),
                *[vec(v) for v in operands[1:]],
                pltpu.VMEM(w_spatial.shape, BF16),
                pltpu.VMEM((total, 128), F32),
                pltpu.VMEM((len(NEAR), rows, dim), BF16),
                pltpu.SemaphoreType.REGULAR,
                pltpu.SemaphoreType.REGULAR,
                pltpu.SemaphoreType.DMA((2,)),
                pltpu.SemaphoreType.DMA((own,)),
                pltpu.SemaphoreType.DMA((1,)),
                pltpu.SemaphoreType.DMA((n_seq,)),
                pltpu.SemaphoreType.DMA((len(NEAR) + 10,)),
            ],
            compiler_params=pltpu.CompilerParams(
                collective_id=0, has_side_effects=True, vmem_limit_bytes=48 * 1024 * 1024
            ),
            name="gmlp_block",
        )(*[pltpu.with_memory_space_constraint(v, pltpu.HBM) for v in operands])

    return jax.shard_map(per_device, mesh=mesh, in_specs=in_specs, out_specs=row_spec, check_vma=False)
```

```python
import functools

import jax
import jax.numpy as jnp
from jax import lax
from jax.experimental import pallas as pl
from jax.experimental.pallas import tpu as pltpu
from jax.sharding import PartitionSpec as P

LN_EPS = 1e-6
MESH = pl.DeviceIdType.MESH
F32 = jnp.float32
BF16 = jnp.bfloat16
TILE = 256
NEAR = (1, 3)
FAR = (2,)
EARLY = 4


def layer_norm(values, gain_vec, offset):
    values_f = values.astype(F32)
    mean_val = jnp.mean(values_f, axis=-1, keepdims=True)
    centered = values_f - mean_val
    var_val = jnp.mean(centered * centered, axis=-1, keepdims=True)
    return (centered * lax.rsqrt(var_val + LN_EPS) * gain_vec + offset).astype(BF16)


def as_row(ref):
    return ref[...].reshape(1, ref.shape[0])


def gelu(hidden):
    half = 0.5 * hidden
    return (half + half * lax.erf(hidden * (0.5 ** 0.5))).astype(BF16)


def block_kernel(n_seq, axis, x_hbm, ln1_gain_hbm, ln1_bias_hbm, w_in_hbm, b_in_hbm, ln2_gain_hbm, ln2_bias_hbm, w_spatial_hbm,
                 b_spatial_hbm, w_out_hbm, b_out_hbm, out_ref, x_buf, o_buf, n_buf, a_buf, ln1_gain, ln1_bias, w_in, b_in, ln2_gain,
                 ln2_bias, w_spatial, b_spatial, w_out, b_out, w_mix, bias_col, x_stage, near_sem, far_sem,
                 in_send, in_recv, out_send, out_recv, w_sem):
    me = lax.axis_index(axis)
    images, rows, _ = x_hbm.shape
    own = images // n_seq
    patches = rows * n_seq
    half_dim = w_out.shape[0]
    per_tile = TILE // rows
    tiles = patches // TILE
    groups = tiles
    home = me // per_tile

    def block_rows(dev):
        return pl.ds(pl.multiple_of(dev * rows, rows), rows)

    def across(group, part):
        return lax.rem(home + group, groups) * per_tile + part

    def send_block(src, dev, slot, sem):
        pltpu.make_async_remote_copy(
            src_ref=src,
            dst_ref=x_buf.at[slot, block_rows(me)],
            send_sem=sem,
            recv_sem=in_recv.at[slot],
            device_id={axis: dev},
            device_id_type=MESH,
        ).start()

    core = lax.rem(me, per_tile)
    mate = across(0, per_tile - 1 - core)
    side = [across(group, core) for group in NEAR]
    cross = [across(group, per_tile - 1 - core) for group in NEAR]
    far = [across(group, part) for group in FAR for part in range(per_tile)]

    barrier = pltpu.get_barrier_semaphore()
    for dev in side + [mate]:
        pl.semaphore_signal(barrier, inc=1, device_id={axis: dev}, device_id_type=MESH)
    stage = [pltpu.make_async_copy(x_hbm.at[dev * own], x_stage.at[k], w_sem.at[k]) for k, dev in enumerate(side)]
    for load in stage:
        load.start()
    pl.semaphore_wait(barrier, len(side) + 1)

    for dev in side:
        pl.semaphore_signal(near_sem, inc=1, device_id={axis: dev}, device_id_type=MESH)
    for k, dev in enumerate(side):
        stage[k].wait()
        send_block(x_stage.at[k], dev, 0, in_send.at[0])
    for slot in range(1, EARLY):
        for dev in side:
            send_block(x_hbm.at[dev * own + slot], dev, slot, in_send.at[1])
    pl.semaphore_wait(near_sem, len(side))

    pl.semaphore_signal(far_sem, inc=1, device_id={axis: mate}, device_id_type=MESH)
    for slot in range(EARLY):
        for dev in cross:
            send_block(x_hbm.at[dev * own + slot], dev, slot, in_send.at[1])
    pl.semaphore_wait(far_sem, 1)
    for slot in range(EARLY):
        for dev in far + [mate]:
            send_block(x_hbm.at[dev * own + slot], dev, slot, in_send.at[1])

    @pl.loop(EARLY, own)
    def _(slot):
        for dev in side + cross + far + [mate]:
            send_block(x_hbm.at[dev * own + slot], dev, slot, in_send.at[1])

    @pl.loop(0, own)
    def _(slot):
        pltpu.make_async_copy(x_hbm.at[me * own + slot], x_buf.at[slot, block_rows(me)], in_recv.at[slot]).start()

    operands = [
        (b_spatial_hbm, b_spatial), (w_spatial_hbm, w_spatial), (ln1_gain_hbm, ln1_gain), (ln1_bias_hbm, ln1_bias), (w_in_hbm, w_in),
        (b_in_hbm, b_in), (ln2_gain_hbm, ln2_gain), (ln2_bias_hbm, ln2_bias), (w_out_hbm, w_out), (b_out_hbm, b_out),
    ]
    loads = [pltpu.make_async_copy(src, dst, w_sem.at[len(NEAR) + k]) for k, (src, dst) in enumerate(operands)]
    for load in loads:
        load.start()
    loads[0].wait()
    for first in range(0, patches, 128):
        lane_bias = jnp.broadcast_to(b_spatial[first:first + 128].reshape(1, 128), (128, 128))
        bias_col[first:first + 128, :] = lane_bias.T
    loads[1].wait()

    @pl.loop(0, patches // TILE)
    def _(step):
        out_rows = pl.ds(pl.multiple_of(step * TILE, TILE), TILE)
        for first in range(0, patches, TILE):
            w_mix[out_rows, first:first + TILE] = w_spatial[first:first + TILE, out_rows].T

    for load in loads[2:]:
        load.wait()

    def send_tile(slot, tile):
        for part in reversed(range(per_tile)):
            dev = tile * per_tile + part
            pltpu.make_async_remote_copy(
                src_ref=o_buf.at[slot, block_rows(dev)],
                dst_ref=out_ref.at[me * own + slot],
                send_sem=out_send.at[0],
                recv_sem=out_recv.at[me],
                device_id={axis: dev},
                device_id_type=MESH,
            ).start()

    def send_home(slot):
        pltpu.make_async_copy(o_buf.at[slot, block_rows(me)], out_ref.at[me * own + slot], out_recv.at[me]).start()
        for step in range(1, per_tile):
            dev = home * per_tile + lax.rem(me + step, per_tile)
            pltpu.make_async_remote_copy(
                src_ref=o_buf.at[slot, block_rows(dev)],
                dst_ref=out_ref.at[me * own + slot],
                send_sem=out_send.at[0],
                recv_sem=out_recv.at[me],
                device_id={axis: dev},
                device_id_type=MESH,
            ).start()

    @pl.loop(0, own)
    def _(slot):
        pltpu.make_async_copy(x_buf.at[slot], x_buf.at[slot], in_recv.at[slot]).wait()

        @pl.loop(0, tiles)
        def _(tile):
            here = pl.ds(pl.multiple_of(tile * TILE, TILE), TILE)
            normed = layer_norm(x_buf[slot, here, :], as_row(ln1_gain), as_row(ln1_bias))
            gate = []
            for first in range(0, 2 * half_dim, 256):
                cols = slice(first, first + 256)
                hidden = jnp.dot(normed, w_in[:, cols], preferred_element_type=F32) + b_in[cols].reshape(1, 256)
                act = gelu(hidden)
                if first < half_dim:
                    a_buf[here, cols] = act
                else:
                    gate.append(act)
            gate = jnp.concatenate(gate, axis=1)
            n_buf[here, :] = layer_norm(gate, as_row(ln2_gain), as_row(ln2_bias))

        @pl.when(slot > 0)
        def _():
            send_home(slot - 1)

        previous = None
        for group in FAR + NEAR + (0,):
            tile = lax.rem(home + group, groups)
            here = pl.ds(pl.multiple_of(tile * TILE, TILE), TILE)
            spatial = jnp.dot(w_mix[here, :], n_buf[...], preferred_element_type=F32).astype(BF16)
            bias = jnp.tile(bias_col[here, :], (1, half_dim // 128))
            gated = (a_buf[here, :].astype(F32) * (spatial.astype(F32) + bias)).astype(BF16)
            mixed = jnp.dot(gated, w_out[...], preferred_element_type=F32) + as_row(b_out)
            o_buf[slot, here, :] = (x_buf[slot, here, :].astype(F32) + mixed).astype(BF16)
            if previous is not None:
                send_tile(slot, previous)
            previous = tile

    send_home(own - 1)

    pltpu.make_async_copy(x_stage, x_stage, in_send.at[0]).wait()
    rest_sent = [x_buf.at[pl.ds(1, own - 1), pl.ds(0, rows * (n_seq - 1))], x_buf.at[0, pl.ds(0, rows * (n_seq - 1 - len(NEAR)))]]
    for part in rest_sent:
        pltpu.make_async_copy(part, part, in_send.at[1]).wait()
    sent = o_buf.at[:, pl.ds(0, rows * (n_seq - 1))]
    pltpu.make_async_copy(sent, sent, out_send.at[0]).wait()
    for dev in range(n_seq):
        part = out_ref.at[pl.ds(dev * own, own)]
        pltpu.make_async_copy(part, part, out_recv.at[dev]).wait()


def solution(mesh):
    row_spec = P("data", "seq", None)
    vec_spec = P(None)
    mat_spec = P(None, None)
    in_specs = (row_spec, vec_spec, vec_spec, mat_spec, vec_spec, vec_spec, vec_spec, mat_spec, vec_spec, mat_spec, vec_spec)
    n_seq = mesh.shape["seq"]

    def per_device(patches, ln1_gain, ln1_bias, w_in, b_in, ln2_gain, ln2_bias, w_spatial, b_spatial, w_out, b_out):
        operands = (patches, ln1_gain, ln1_bias, w_in, b_in, ln2_gain, ln2_bias, w_spatial, b_spatial, w_out, b_out)
        images, rows, dim = patches.shape
        own = images // n_seq
        total = rows * n_seq
        half_dim = w_out.shape[0]
        hbm = pl.BlockSpec(memory_space=pltpu.HBM)
        vec = lambda ref: pltpu.VMEM(ref.shape, ref.dtype)
        return pl.pallas_call(
            functools.partial(block_kernel, n_seq, "seq"),
            out_shape=pltpu.VMEM(patches.shape, BF16),
            in_specs=[hbm] * 11,
            out_specs=pl.BlockSpec(memory_space=pltpu.VMEM),
            scratch_shapes=[
                pltpu.VMEM((own, total, dim), BF16),
                pltpu.VMEM((own, total, dim), BF16),
                pltpu.VMEM((total, half_dim), BF16),
                pltpu.VMEM((total, half_dim), BF16),
                *[vec(v) for v in operands[1:]],
                pltpu.VMEM(w_spatial.shape, BF16),
                pltpu.VMEM((total, 128), F32),
                pltpu.VMEM((len(NEAR), rows, dim), BF16),
                pltpu.SemaphoreType.REGULAR,
                pltpu.SemaphoreType.REGULAR,
                pltpu.SemaphoreType.DMA((2,)),
                pltpu.SemaphoreType.DMA((own,)),
                pltpu.SemaphoreType.DMA((1,)),
                pltpu.SemaphoreType.DMA((n_seq,)),
                pltpu.SemaphoreType.DMA((len(NEAR) + 10,)),
            ],
            compiler_params=pltpu.CompilerParams(
                collective_id=0, has_side_effects=True, vmem_limit_bytes=48 * 1024 * 1024
            ),
            name="gmlp_block",
        )(*[pltpu.with_memory_space_constraint(v, pltpu.HBM) for v in operands])

    return jax.shard_map(per_device, mesh=mesh, in_specs=in_specs, out_specs=row_spec, check_vma=False)
```

```python
import functools

import jax
import jax.numpy as jnp
from jax import lax
from jax.experimental import pallas as pl
from jax.experimental.pallas import tpu as pltpu
from jax.sharding import PartitionSpec as P

LN_EPS = 1e-6
MESH = pl.DeviceIdType.MESH
F32 = jnp.float32
BF16 = jnp.bfloat16
TILE = 256
NEAR = (1, 3)
FAR = (2,)
EARLY = 4


def layer_norm(values, gain_vec, offset):
    values_f = values.astype(F32)
    mean_val = jnp.mean(values_f, axis=-1, keepdims=True)
    centered = values_f - mean_val
    var_val = jnp.mean(centered * centered, axis=-1, keepdims=True)
    return (centered * lax.rsqrt(var_val + LN_EPS) * gain_vec + offset).astype(BF16)


def as_row(ref):
    return ref[...].reshape(1, ref.shape[0])


def gelu(hidden):
    half = 0.5 * hidden
    return (half + half * lax.erf(hidden * (0.5 ** 0.5))).astype(BF16)


def block_kernel(n_seq, axis, x_hbm, ln1_gain_hbm, ln1_bias_hbm, w_in_hbm, b_in_hbm, ln2_gain_hbm, ln2_bias_hbm, w_spatial_hbm,
                 b_spatial_hbm, w_out_hbm, b_out_hbm, out_ref, x_buf, o_buf, n_buf, a_buf, ln1_gain, ln1_bias, w_in, b_in, ln2_gain,
                 ln2_bias, w_spatial, b_spatial, w_out, b_out, w_mix, bias_col, x_stage, near_sem, far_sem,
                 relay, in_send, in_recv, out_send, out_recv, relay_sem, w_sem):
    me = lax.axis_index(axis)
    images, rows, _ = x_hbm.shape
    own = images // n_seq
    patches = rows * n_seq
    half_dim = w_out.shape[0]
    per_tile = TILE // rows
    tiles = patches // TILE
    groups = tiles
    home = me // per_tile

    def block_rows(dev):
        return pl.ds(pl.multiple_of(dev * rows, rows), rows)

    def across(group, part):
        return lax.rem(home + group, groups) * per_tile + part

    def send_block(src, dev, slot, sem):
        pltpu.make_async_remote_copy(
            src_ref=src,
            dst_ref=x_buf.at[slot, block_rows(me)],
            send_sem=sem,
            recv_sem=in_recv.at[slot],
            device_id={axis: dev},
            device_id_type=MESH,
        ).start()

    core = lax.rem(me, per_tile)
    mate = across(0, per_tile - 1 - core)
    side = [across(group, core) for group in NEAR]
    cross = [across(group, per_tile - 1 - core) for group in NEAR]
    far = [across(group, part) for group in FAR for part in range(per_tile)]

    barrier = pltpu.get_barrier_semaphore()
    for dev in side + [mate]:
        pl.semaphore_signal(barrier, inc=1, device_id={axis: dev}, device_id_type=MESH)
    stage = [pltpu.make_async_copy(x_hbm.at[dev * own], x_stage.at[k], w_sem.at[k]) for k, dev in enumerate(side)]
    for load in stage:
        load.start()
    pl.semaphore_wait(barrier, len(side) + 1)

    for dev in side:
        pl.semaphore_signal(near_sem, inc=1, device_id={axis: dev}, device_id_type=MESH)
    for k, dev in enumerate(side):
        stage[k].wait()
        send_block(x_stage.at[k], dev, 0, in_send.at[0])
    for slot in range(1, EARLY):
        for dev in side:
            send_block(x_hbm.at[dev * own + slot], dev, slot, in_send.at[1])
    pl.semaphore_wait(near_sem, len(side))

    pl.semaphore_signal(far_sem, inc=1, device_id={axis: mate}, device_id_type=MESH)
    for slot in range(EARLY):
        for dev in cross:
            send_block(x_hbm.at[dev * own + slot], dev, slot, in_send.at[1])
    pl.semaphore_wait(far_sem, 1)
    for slot in range(EARLY):
        for dev in far + [mate]:
            send_block(x_hbm.at[dev * own + slot], dev, slot, in_send.at[1])

    @pl.loop(EARLY, own)
    def _(slot):
        for dev in side + cross + far + [mate]:
            send_block(x_hbm.at[dev * own + slot], dev, slot, in_send.at[1])

    @pl.loop(0, own)
    def _(slot):
        pltpu.make_async_copy(x_hbm.at[me * own + slot], x_buf.at[slot, block_rows(me)], in_recv.at[slot]).start()

    operands = [
        (b_spatial_hbm, b_spatial), (w_spatial_hbm, w_spatial), (ln1_gain_hbm, ln1_gain), (ln1_bias_hbm, ln1_bias), (w_in_hbm, w_in),
        (b_in_hbm, b_in), (ln2_gain_hbm, ln2_gain), (ln2_bias_hbm, ln2_bias), (w_out_hbm, w_out), (b_out_hbm, b_out),
    ]
    loads = [pltpu.make_async_copy(src, dst, w_sem.at[len(NEAR) + k]) for k, (src, dst) in enumerate(operands)]
    for load in loads:
        load.start()
    loads[0].wait()
    for first in range(0, patches, 128):
        lane_bias = jnp.broadcast_to(b_spatial[first:first + 128].reshape(1, 128), (128, 128))
        bias_col[first:first + 128, :] = lane_bias.T
    loads[1].wait()

    @pl.loop(0, patches // TILE)
    def _(step):
        out_rows = pl.ds(pl.multiple_of(step * TILE, TILE), TILE)
        for first in range(0, patches, TILE):
            w_mix[out_rows, first:first + TILE] = w_spatial[first:first + TILE, out_rows].T

    for load in loads[2:]:
        load.wait()

    def send_result(src, owner, slot, dev, sem):
        pltpu.make_async_remote_copy(
            src_ref=src,
            dst_ref=out_ref.at[owner * own + slot],
            send_sem=sem,
            recv_sem=out_recv.at[owner],
            device_id={axis: dev},
            device_id_type=MESH,
        ).start()

    def send_tile(slot, tile, group):
        for part in reversed(range(per_tile)):
            dev = tile * per_tile + part
            src = o_buf.at[slot, block_rows(dev)]
            if part > 0 or group not in NEAR:
                send_result(src, me, slot, dev, out_send.at[0])
                continue
            handed = (slot == own - 1) & (core == 0)

            @pl.when(jnp.logical_not(handed))
            def _():
                send_result(src, me, slot, dev, out_send.at[0])

            @pl.when(handed)
            def _():
                pltpu.make_async_remote_copy(
                    src_ref=src,
                    dst_ref=relay.at[NEAR.index(group)],
                    send_sem=out_send.at[0],
                    recv_sem=relay_sem.at[0],
                    device_id={axis: mate},
                    device_id_type=MESH,
                ).start()

    def send_home(slot):
        pltpu.make_async_copy(o_buf.at[slot, block_rows(me)], out_ref.at[me * own + slot], out_recv.at[me]).start()
        send_result(o_buf.at[slot, block_rows(mate)], me, slot, mate, out_send.at[0])

    @pl.loop(0, own)
    def _(slot):
        pltpu.make_async_copy(x_buf.at[slot], x_buf.at[slot], in_recv.at[slot]).wait()

        @pl.loop(0, tiles)
        def _(tile):
            here = pl.ds(pl.multiple_of(tile * TILE, TILE), TILE)
            normed = layer_norm(x_buf[slot, here, :], as_row(ln1_gain), as_row(ln1_bias))
            gate = []
            for first in range(0, 2 * half_dim, 256):
                cols = slice(first, first + 256)
                hidden = jnp.dot(normed, w_in[:, cols], preferred_element_type=F32) + b_in[cols].reshape(1, 256)
                act = gelu(hidden)
                if first < half_dim:
                    a_buf[here, cols] = act
                else:
                    gate.append(act)
            gate = jnp.concatenate(gate, axis=1)
            n_buf[here, :] = layer_norm(gate, as_row(ln2_gain), as_row(ln2_bias))

        @pl.when(slot > 0)
        def _():
            send_home(slot - 1)

        previous = None
        for group in FAR + NEAR + (0,):
            tile = lax.rem(home + group, groups)
            here = pl.ds(pl.multiple_of(tile * TILE, TILE), TILE)
            spatial = jnp.dot(w_mix[here, :], n_buf[...], preferred_element_type=F32).astype(BF16)
            bias = jnp.tile(bias_col[here, :], (1, half_dim // 128))
            gated = (a_buf[here, :].astype(F32) * (spatial.astype(F32) + bias)).astype(BF16)
            mixed = jnp.dot(gated, w_out[...], preferred_element_type=F32) + as_row(b_out)
            o_buf[slot, here, :] = (x_buf[slot, here, :].astype(F32) + mixed).astype(BF16)
            if previous is not None:
                send_tile(slot, *previous)
            previous = tile, group

    @pl.when(core == per_tile - 1)
    def _():
        pltpu.make_async_copy(relay, relay, relay_sem.at[0]).wait()
        for k, group in enumerate(NEAR):
            send_result(relay.at[k], mate, own - 1, across(group, 0), relay_sem.at[1])

    send_home(own - 1)

    pltpu.make_async_copy(x_stage, x_stage, in_send.at[0]).wait()
    rest_sent = [x_buf.at[pl.ds(1, own - 1), pl.ds(0, rows * (n_seq - 1))], x_buf.at[0, pl.ds(0, rows * (n_seq - 1 - len(NEAR)))]]
    for part in rest_sent:
        pltpu.make_async_copy(part, part, in_send.at[1]).wait()
    sent = o_buf.at[:, pl.ds(0, rows * (n_seq - 1))]
    pltpu.make_async_copy(sent, sent, out_send.at[0]).wait()

    @pl.when(core == per_tile - 1)
    def _():
        pltpu.make_async_copy(relay, relay, relay_sem.at[1]).wait()

    for dev in range(n_seq):
        part = out_ref.at[pl.ds(dev * own, own)]
        pltpu.make_async_copy(part, part, out_recv.at[dev]).wait()


def solution(mesh):
    row_spec = P("data", "seq", None)
    vec_spec = P(None)
    mat_spec = P(None, None)
    in_specs = (row_spec, vec_spec, vec_spec, mat_spec, vec_spec, vec_spec, vec_spec, mat_spec, vec_spec, mat_spec, vec_spec)
    n_seq = mesh.shape["seq"]

    def per_device(patches, ln1_gain, ln1_bias, w_in, b_in, ln2_gain, ln2_bias, w_spatial, b_spatial, w_out, b_out):
        operands = (patches, ln1_gain, ln1_bias, w_in, b_in, ln2_gain, ln2_bias, w_spatial, b_spatial, w_out, b_out)
        images, rows, dim = patches.shape
        own = images // n_seq
        total = rows * n_seq
        half_dim = w_out.shape[0]
        hbm = pl.BlockSpec(memory_space=pltpu.HBM)
        vec = lambda ref: pltpu.VMEM(ref.shape, ref.dtype)
        return pl.pallas_call(
            functools.partial(block_kernel, n_seq, "seq"),
            out_shape=pltpu.VMEM(patches.shape, BF16),
            in_specs=[hbm] * 11,
            out_specs=pl.BlockSpec(memory_space=pltpu.VMEM),
            scratch_shapes=[
                pltpu.VMEM((own, total, dim), BF16),
                pltpu.VMEM((own, total, dim), BF16),
                pltpu.VMEM((total, half_dim), BF16),
                pltpu.VMEM((total, half_dim), BF16),
                *[vec(v) for v in operands[1:]],
                pltpu.VMEM(w_spatial.shape, BF16),
                pltpu.VMEM((total, 128), F32),
                pltpu.VMEM((len(NEAR), rows, dim), BF16),
                pltpu.SemaphoreType.REGULAR,
                pltpu.SemaphoreType.REGULAR,
                pltpu.VMEM((len(NEAR), rows, dim), BF16),
                pltpu.SemaphoreType.DMA((2,)),
                pltpu.SemaphoreType.DMA((own,)),
                pltpu.SemaphoreType.DMA((1,)),
                pltpu.SemaphoreType.DMA((n_seq,)),
                pltpu.SemaphoreType.DMA((2,)),
                pltpu.SemaphoreType.DMA((len(NEAR) + 10,)),
            ],
            compiler_params=pltpu.CompilerParams(
                collective_id=0, has_side_effects=True, vmem_limit_bytes=48 * 1024 * 1024
            ),
            name="gmlp_block",
        )(*[pltpu.with_memory_space_constraint(v, pltpu.HBM) for v in operands])

    return jax.shard_map(per_device, mesh=mesh, in_specs=in_specs, out_specs=row_spec, check_vma=False)
```

```python
import functools

import jax
import jax.numpy as jnp
from jax import lax
from jax.experimental import pallas as pl
from jax.experimental.pallas import tpu as pltpu
from jax.sharding import PartitionSpec as P

LN_EPS = 1e-6
MESH = pl.DeviceIdType.MESH
F32 = jnp.float32
BF16 = jnp.bfloat16
TILE = 256
NEAR = (1, 3)
FAR = (2,)
EARLY = 4


def layer_norm(values, gain_vec, offset):
    values_f = values.astype(F32)
    mean_val = jnp.mean(values_f, axis=-1, keepdims=True)
    centered = values_f - mean_val
    var_val = jnp.mean(centered * centered, axis=-1, keepdims=True)
    return (centered * lax.rsqrt(var_val + LN_EPS) * gain_vec + offset).astype(BF16)


def as_row(ref):
    return ref[...].reshape(1, ref.shape[0])


def gelu(hidden):
    half = 0.5 * hidden
    return (half + half * lax.erf(hidden * (0.5 ** 0.5))).astype(BF16)


def block_kernel(n_seq, axis, x_hbm, ln1_gain_hbm, ln1_bias_hbm, w_in_hbm, b_in_hbm, ln2_gain_hbm, ln2_bias_hbm, w_spatial_hbm,
                 b_spatial_hbm, w_out_hbm, b_out_hbm, out_ref, x_buf, o_buf, n_buf, a_buf, ln1_gain, ln1_bias, w_in, b_in, ln2_gain,
                 ln2_bias, w_spatial, b_spatial, w_out, b_out, w_mix, bias_col, x_stage, near_sem, far_sem,
                 in_send, in_recv, out_send, out_recv, w_sem):
    me = lax.axis_index(axis)
    images, rows, _ = x_hbm.shape
    own = images // n_seq
    patches = rows * n_seq
    half_dim = w_out.shape[0]
    per_tile = TILE // rows
    tiles = patches // TILE
    groups = tiles
    home = me // per_tile

    def block_rows(dev):
        return pl.ds(pl.multiple_of(dev * rows, rows), rows)

    def across(group, part):
        return lax.rem(home + group, groups) * per_tile + part

    def send_block(src, dev, slot, sem):
        pltpu.make_async_remote_copy(
            src_ref=src,
            dst_ref=x_buf.at[slot, block_rows(me)],
            send_sem=sem,
            recv_sem=in_recv.at[slot],
            device_id={axis: dev},
            device_id_type=MESH,
        ).start()

    core = lax.rem(me, per_tile)
    mate = across(0, per_tile - 1 - core)
    side = [across(group, core) for group in NEAR]
    cross = [across(group, per_tile - 1 - core) for group in NEAR]
    far = [across(group, part) for group in FAR for part in range(per_tile)]

    stage = [pltpu.make_async_copy(x_hbm.at[dev * own], x_stage.at[k], w_sem.at[k]) for k, dev in enumerate(side)]
    for load in stage:
        load.start()

    barrier = pltpu.get_barrier_semaphore()
    for dev in side + [mate]:
        pl.semaphore_signal(barrier, inc=1, device_id={axis: dev}, device_id_type=MESH)
    pl.semaphore_wait(barrier, len(side) + 1)

    for dev in side:
        pl.semaphore_signal(near_sem, inc=1, device_id={axis: dev}, device_id_type=MESH)
    for k, dev in enumerate(side):
        stage[k].wait()
        send_block(x_stage.at[k], dev, 0, in_send.at[0])
    for slot in range(1, EARLY):
        for dev in side:
            send_block(x_hbm.at[dev * own + slot], dev, slot, in_send.at[1])
    pl.semaphore_wait(near_sem, len(side))

    pl.semaphore_signal(far_sem, inc=1, device_id={axis: mate}, device_id_type=MESH)
    for slot in range(EARLY):
        for dev in cross:
            send_block(x_hbm.at[dev * own + slot], dev, slot, in_send.at[1])
    pl.semaphore_wait(far_sem, 1)
    for slot in range(EARLY):
        for dev in far + [mate]:
            send_block(x_hbm.at[dev * own + slot], dev, slot, in_send.at[1])

    @pl.loop(EARLY, own)
    def _(slot):
        for dev in side + cross + far + [mate]:
            send_block(x_hbm.at[dev * own + slot], dev, slot, in_send.at[1])

    @pl.loop(0, own)
    def _(slot):
        pltpu.make_async_copy(x_hbm.at[me * own + slot], x_buf.at[slot, block_rows(me)], in_recv.at[slot]).start()

    operands = [
        (b_spatial_hbm, b_spatial), (w_spatial_hbm, w_spatial), (ln1_gain_hbm, ln1_gain), (ln1_bias_hbm, ln1_bias), (w_in_hbm, w_in),
        (b_in_hbm, b_in), (ln2_gain_hbm, ln2_gain), (ln2_bias_hbm, ln2_bias), (w_out_hbm, w_out), (b_out_hbm, b_out),
    ]
    loads = [pltpu.make_async_copy(src, dst, w_sem.at[len(NEAR) + k]) for k, (src, dst) in enumerate(operands)]
    for load in loads:
        load.start()
    loads[0].wait()
    for first in range(0, patches, 128):
        lane_bias = jnp.broadcast_to(b_spatial[first:first + 128].reshape(1, 128), (128, 128))
        bias_col[first:first + 128, :] = lane_bias.T
    loads[1].wait()

    @pl.loop(0, patches // TILE)
    def _(step):
        out_rows = pl.ds(pl.multiple_of(step * TILE, TILE), TILE)
        for first in range(0, patches, TILE):
            w_mix[out_rows, first:first + TILE] = w_spatial[first:first + TILE, out_rows].T

    for load in loads[2:]:
        load.wait()

    def send_tile(slot, tile, group):
        for part in range(per_tile) if group in FAR else reversed(range(per_tile)):
            dev = tile * per_tile + part
            pltpu.make_async_remote_copy(
                src_ref=o_buf.at[slot, block_rows(dev)],
                dst_ref=out_ref.at[me * own + slot],
                send_sem=out_send.at[0],
                recv_sem=out_recv.at[me],
                device_id={axis: dev},
                device_id_type=MESH,
            ).start()

    def send_home(slot):
        pltpu.make_async_copy(o_buf.at[slot, block_rows(me)], out_ref.at[me * own + slot], out_recv.at[me]).start()
        for step in range(1, per_tile):
            dev = home * per_tile + lax.rem(me + step, per_tile)
            pltpu.make_async_remote_copy(
                src_ref=o_buf.at[slot, block_rows(dev)],
                dst_ref=out_ref.at[me * own + slot],
                send_sem=out_send.at[0],
                recv_sem=out_recv.at[me],
                device_id={axis: dev},
                device_id_type=MESH,
            ).start()

    @pl.loop(0, own)
    def _(slot):
        pltpu.make_async_copy(x_buf.at[slot], x_buf.at[slot], in_recv.at[slot]).wait()

        @pl.loop(0, tiles)
        def _(tile):
            here = pl.ds(pl.multiple_of(tile * TILE, TILE), TILE)
            normed = layer_norm(x_buf[slot, here, :], as_row(ln1_gain), as_row(ln1_bias))
            gate = []
            for first in range(0, 2 * half_dim, 256):
                cols = slice(first, first + 256)
                hidden = jnp.dot(normed, w_in[:, cols], preferred_element_type=F32) + b_in[cols].reshape(1, 256)
                act = gelu(hidden)
                if first < half_dim:
                    a_buf[here, cols] = act
                else:
                    gate.append(act)
            gate = jnp.concatenate(gate, axis=1)
            n_buf[here, :] = layer_norm(gate, as_row(ln2_gain), as_row(ln2_bias))

        @pl.when(slot > 0)
        def _():
            send_home(slot - 1)

        previous = None
        for group in FAR + NEAR + (0,):
            tile = lax.rem(home + group, groups)
            here = pl.ds(pl.multiple_of(tile * TILE, TILE), TILE)
            spatial = jnp.dot(w_mix[here, :], n_buf[...], preferred_element_type=F32).astype(BF16)
            bias = jnp.tile(bias_col[here, :], (1, half_dim // 128))
            gated = (a_buf[here, :].astype(F32) * (spatial.astype(F32) + bias)).astype(BF16)
            mixed = jnp.dot(gated, w_out[...], preferred_element_type=F32) + as_row(b_out)
            o_buf[slot, here, :] = (x_buf[slot, here, :].astype(F32) + mixed).astype(BF16)
            if previous is not None:
                send_tile(slot, *previous)
            previous = tile, group

    send_home(own - 1)

    pltpu.make_async_copy(x_stage, x_stage, in_send.at[0]).wait()
    rest_sent = [x_buf.at[pl.ds(1, own - 1), pl.ds(0, rows * (n_seq - 1))], x_buf.at[0, pl.ds(0, rows * (n_seq - 1 - len(NEAR)))]]
    for part in rest_sent:
        pltpu.make_async_copy(part, part, in_send.at[1]).wait()
    sent = o_buf.at[:, pl.ds(0, rows * (n_seq - 1))]
    pltpu.make_async_copy(sent, sent, out_send.at[0]).wait()
    for dev in range(n_seq):
        part = out_ref.at[pl.ds(dev * own, own)]
        pltpu.make_async_copy(part, part, out_recv.at[dev]).wait()


def solution(mesh):
    row_spec = P("data", "seq", None)
    vec_spec = P(None)
    mat_spec = P(None, None)
    in_specs = (row_spec, vec_spec, vec_spec, mat_spec, vec_spec, vec_spec, vec_spec, mat_spec, vec_spec, mat_spec, vec_spec)
    n_seq = mesh.shape["seq"]

    def per_device(patches, ln1_gain, ln1_bias, w_in, b_in, ln2_gain, ln2_bias, w_spatial, b_spatial, w_out, b_out):
        operands = (patches, ln1_gain, ln1_bias, w_in, b_in, ln2_gain, ln2_bias, w_spatial, b_spatial, w_out, b_out)
        images, rows, dim = patches.shape
        own = images // n_seq
        total = rows * n_seq
        half_dim = w_out.shape[0]
        hbm = pl.BlockSpec(memory_space=pltpu.HBM)
        vec = lambda ref: pltpu.VMEM(ref.shape, ref.dtype)
        return pl.pallas_call(
            functools.partial(block_kernel, n_seq, "seq"),
            out_shape=pltpu.VMEM(patches.shape, BF16),
            in_specs=[hbm] * 11,
            out_specs=pl.BlockSpec(memory_space=pltpu.VMEM),
            scratch_shapes=[
                pltpu.VMEM((own, total, dim), BF16),
                pltpu.VMEM((own, total, dim), BF16),
                pltpu.VMEM((total, half_dim), BF16),
                pltpu.VMEM((total, half_dim), BF16),
                *[vec(v) for v in operands[1:]],
                pltpu.VMEM(w_spatial.shape, BF16),
                pltpu.VMEM((total, 128), F32),
                pltpu.VMEM((len(NEAR), rows, dim), BF16),
                pltpu.SemaphoreType.REGULAR,
                pltpu.SemaphoreType.REGULAR,
                pltpu.SemaphoreType.DMA((2,)),
                pltpu.SemaphoreType.DMA((own,)),
                pltpu.SemaphoreType.DMA((1,)),
                pltpu.SemaphoreType.DMA((n_seq,)),
                pltpu.SemaphoreType.DMA((len(NEAR) + 10,)),
            ],
            compiler_params=pltpu.CompilerParams(
                collective_id=0, has_side_effects=True, vmem_limit_bytes=48 * 1024 * 1024
            ),
            name="gmlp_block",
        )(*[pltpu.with_memory_space_constraint(v, pltpu.HBM) for v in operands])

    return jax.shard_map(per_device, mesh=mesh, in_specs=in_specs, out_specs=row_spec, check_vma=False)
```

```python
import functools

import jax
import jax.numpy as jnp
from jax import lax
from jax.experimental import pallas as pl
from jax.experimental.pallas import tpu as pltpu
from jax.sharding import PartitionSpec as P

LN_EPS = 1e-6
MESH = pl.DeviceIdType.MESH
F32 = jnp.float32
BF16 = jnp.bfloat16
TILE = 256
NEAR = (1, 3)
FAR = (2,)
EARLY = 4


def layer_norm(values, gain_vec, offset):
    values_f = values.astype(F32)
    mean_val = jnp.mean(values_f, axis=-1, keepdims=True)
    centered = values_f - mean_val
    var_val = jnp.mean(centered * centered, axis=-1, keepdims=True)
    return (centered * lax.rsqrt(var_val + LN_EPS) * gain_vec + offset).astype(BF16)


def as_row(ref):
    return ref[...].reshape(1, ref.shape[0])


def gelu(hidden):
    half = 0.5 * hidden
    return (half + half * lax.erf(hidden * (0.5 ** 0.5))).astype(BF16)


def block_kernel(n_seq, axis, x_hbm, ln1_gain_hbm, ln1_bias_hbm, w_in_hbm, b_in_hbm, ln2_gain_hbm, ln2_bias_hbm, w_spatial_hbm,
                 b_spatial_hbm, w_out_hbm, b_out_hbm, out_ref, x_buf, o_buf, n_buf, a_buf, ln1_gain, ln1_bias, w_in, b_in, ln2_gain,
                 ln2_bias, w_spatial, b_spatial, w_out, b_out, w_mix, bias_col, x_stage, near_sem, far_sem,
                 relay, in_send, in_recv, out_send, out_recv, relay_sem, w_sem):
    me = lax.axis_index(axis)
    images, rows, _ = x_hbm.shape
    own = images // n_seq
    patches = rows * n_seq
    half_dim = w_out.shape[0]
    per_tile = TILE // rows
    tiles = patches // TILE
    groups = tiles
    home = me // per_tile

    def block_rows(dev):
        return pl.ds(pl.multiple_of(dev * rows, rows), rows)

    def across(group, part):
        return lax.rem(home + group, groups) * per_tile + part

    def send_block(src, dev, slot, sem):
        pltpu.make_async_remote_copy(
            src_ref=src,
            dst_ref=x_buf.at[slot, block_rows(me)],
            send_sem=sem,
            recv_sem=in_recv.at[slot],
            device_id={axis: dev},
            device_id_type=MESH,
        ).start()

    core = lax.rem(me, per_tile)
    mate = across(0, per_tile - 1 - core)
    side = [across(group, core) for group in NEAR]
    cross = [across(group, per_tile - 1 - core) for group in NEAR]
    far = [across(group, part) for group in FAR for part in range(per_tile)]

    stage = [pltpu.make_async_copy(x_hbm.at[dev * own], x_stage.at[k], w_sem.at[k]) for k, dev in enumerate(side)]
    for load in stage:
        load.start()

    barrier = pltpu.get_barrier_semaphore()
    for dev in side + [mate]:
        pl.semaphore_signal(barrier, inc=1, device_id={axis: dev}, device_id_type=MESH)
    pl.semaphore_wait(barrier, len(side) + 1)

    for dev in side:
        pl.semaphore_signal(near_sem, inc=1, device_id={axis: dev}, device_id_type=MESH)
    for k, dev in enumerate(side):
        stage[k].wait()
        send_block(x_stage.at[k], dev, 0, in_send.at[0])
    for slot in range(1, EARLY):
        for dev in side:
            send_block(x_hbm.at[dev * own + slot], dev, slot, in_send.at[1])
    pl.semaphore_wait(near_sem, len(side))

    pl.semaphore_signal(far_sem, inc=1, device_id={axis: mate}, device_id_type=MESH)
    for slot in range(EARLY):
        for dev in cross:
            send_block(x_hbm.at[dev * own + slot], dev, slot, in_send.at[1])
    pl.semaphore_wait(far_sem, 1)
    for slot in range(EARLY):
        for dev in far + [mate]:
            send_block(x_hbm.at[dev * own + slot], dev, slot, in_send.at[1])

    @pl.loop(EARLY, own)
    def _(slot):
        for dev in side + cross + far + [mate]:
            send_block(x_hbm.at[dev * own + slot], dev, slot, in_send.at[1])

    @pl.loop(0, own)
    def _(slot):
        pltpu.make_async_copy(x_hbm.at[me * own + slot], x_buf.at[slot, block_rows(me)], in_recv.at[slot]).start()

    operands = [
        (b_spatial_hbm, b_spatial), (w_spatial_hbm, w_spatial), (ln1_gain_hbm, ln1_gain), (ln1_bias_hbm, ln1_bias), (w_in_hbm, w_in),
        (b_in_hbm, b_in), (ln2_gain_hbm, ln2_gain), (ln2_bias_hbm, ln2_bias), (w_out_hbm, w_out), (b_out_hbm, b_out),
    ]
    loads = [pltpu.make_async_copy(src, dst, w_sem.at[len(NEAR) + k]) for k, (src, dst) in enumerate(operands)]
    for load in loads:
        load.start()
    loads[0].wait()
    for first in range(0, patches, 128):
        lane_bias = jnp.broadcast_to(b_spatial[first:first + 128].reshape(1, 128), (128, 128))
        bias_col[first:first + 128, :] = lane_bias.T
    loads[1].wait()

    @pl.loop(0, patches // TILE)
    def _(step):
        out_rows = pl.ds(pl.multiple_of(step * TILE, TILE), TILE)
        for first in range(0, patches, TILE):
            w_mix[out_rows, first:first + TILE] = w_spatial[first:first + TILE, out_rows].T

    for load in loads[2:]:
        load.wait()

    def send_result(src, owner, slot, dev, sem):
        pltpu.make_async_remote_copy(
            src_ref=src,
            dst_ref=out_ref.at[owner * own + slot],
            send_sem=sem,
            recv_sem=out_recv.at[owner],
            device_id={axis: dev},
            device_id_type=MESH,
        ).start()

    def send_tile(slot, tile, group):
        for part in reversed(range(per_tile)):
            dev = tile * per_tile + part
            src = o_buf.at[slot, block_rows(dev)]
            if part > 0 or group not in NEAR:
                send_result(src, me, slot, dev, out_send.at[0])
                continue
            handed = (slot == own - 1) & (core > 0)

            @pl.when(jnp.logical_not(handed))
            def _():
                send_result(src, me, slot, dev, out_send.at[0])

            @pl.when(handed)
            def _():
                pltpu.make_async_remote_copy(
                    src_ref=src,
                    dst_ref=relay.at[NEAR.index(group)],
                    send_sem=out_send.at[0],
                    recv_sem=relay_sem.at[0],
                    device_id={axis: mate},
                    device_id_type=MESH,
                ).start()

    def send_home(slot):
        pltpu.make_async_copy(o_buf.at[slot, block_rows(me)], out_ref.at[me * own + slot], out_recv.at[me]).start()
        send_result(o_buf.at[slot, block_rows(mate)], me, slot, mate, out_send.at[0])

    @pl.loop(0, own)
    def _(slot):
        pltpu.make_async_copy(x_buf.at[slot], x_buf.at[slot], in_recv.at[slot]).wait()

        @pl.loop(0, tiles)
        def _(tile):
            here = pl.ds(pl.multiple_of(tile * TILE, TILE), TILE)
            normed = layer_norm(x_buf[slot, here, :], as_row(ln1_gain), as_row(ln1_bias))
            gate = []
            for first in range(0, 2 * half_dim, 256):
                cols = slice(first, first + 256)
                hidden = jnp.dot(normed, w_in[:, cols], preferred_element_type=F32) + b_in[cols].reshape(1, 256)
                act = gelu(hidden)
                if first < half_dim:
                    a_buf[here, cols] = act
                else:
                    gate.append(act)
            gate = jnp.concatenate(gate, axis=1)
            n_buf[here, :] = layer_norm(gate, as_row(ln2_gain), as_row(ln2_bias))

        @pl.when(slot > 0)
        def _():
            send_home(slot - 1)

        previous = None
        for group in FAR + NEAR + (0,):
            tile = lax.rem(home + group, groups)
            here = pl.ds(pl.multiple_of(tile * TILE, TILE), TILE)
            spatial = jnp.dot(w_mix[here, :], n_buf[...], preferred_element_type=F32).astype(BF16)
            bias = jnp.tile(bias_col[here, :], (1, half_dim // 128))
            gated = (a_buf[here, :].astype(F32) * (spatial.astype(F32) + bias)).astype(BF16)
            mixed = jnp.dot(gated, w_out[...], preferred_element_type=F32) + as_row(b_out)
            o_buf[slot, here, :] = (x_buf[slot, here, :].astype(F32) + mixed).astype(BF16)
            if previous is not None:
                send_tile(slot, *previous)
            previous = tile, group

    @pl.when(core == 0)
    def _():
        pltpu.make_async_copy(relay, relay, relay_sem.at[0]).wait()
        for k, group in enumerate(NEAR):
            send_result(relay.at[k], mate, own - 1, across(group, 0), relay_sem.at[1])

    send_home(own - 1)

    pltpu.make_async_copy(x_stage, x_stage, in_send.at[0]).wait()
    rest_sent = [x_buf.at[pl.ds(1, own - 1), pl.ds(0, rows * (n_seq - 1))], x_buf.at[0, pl.ds(0, rows * (n_seq - 1 - len(NEAR)))]]
    for part in rest_sent:
        pltpu.make_async_copy(part, part, in_send.at[1]).wait()
    sent = o_buf.at[:, pl.ds(0, rows * (n_seq - 1))]
    pltpu.make_async_copy(sent, sent, out_send.at[0]).wait()

    @pl.when(core == 0)
    def _():
        pltpu.make_async_copy(relay, relay, relay_sem.at[1]).wait()

    for dev in range(n_seq):
        part = out_ref.at[pl.ds(dev * own, own)]
        pltpu.make_async_copy(part, part, out_recv.at[dev]).wait()


def solution(mesh):
    row_spec = P("data", "seq", None)
    vec_spec = P(None)
    mat_spec = P(None, None)
    in_specs = (row_spec, vec_spec, vec_spec, mat_spec, vec_spec, vec_spec, vec_spec, mat_spec, vec_spec, mat_spec, vec_spec)
    n_seq = mesh.shape["seq"]

    def per_device(patches, ln1_gain, ln1_bias, w_in, b_in, ln2_gain, ln2_bias, w_spatial, b_spatial, w_out, b_out):
        operands = (patches, ln1_gain, ln1_bias, w_in, b_in, ln2_gain, ln2_bias, w_spatial, b_spatial, w_out, b_out)
        images, rows, dim = patches.shape
        own = images // n_seq
        total = rows * n_seq
        half_dim = w_out.shape[0]
        hbm = pl.BlockSpec(memory_space=pltpu.HBM)
        vec = lambda ref: pltpu.VMEM(ref.shape, ref.dtype)
        return pl.pallas_call(
            functools.partial(block_kernel, n_seq, "seq"),
            out_shape=pltpu.VMEM(patches.shape, BF16),
            in_specs=[hbm] * 11,
            out_specs=pl.BlockSpec(memory_space=pltpu.VMEM),
            scratch_shapes=[
                pltpu.VMEM((own, total, dim), BF16),
                pltpu.VMEM((own, total, dim), BF16),
                pltpu.VMEM((total, half_dim), BF16),
                pltpu.VMEM((total, half_dim), BF16),
                *[vec(v) for v in operands[1:]],
                pltpu.VMEM(w_spatial.shape, BF16),
                pltpu.VMEM((total, 128), F32),
                pltpu.VMEM((len(NEAR), rows, dim), BF16),
                pltpu.SemaphoreType.REGULAR,
                pltpu.SemaphoreType.REGULAR,
                pltpu.VMEM((len(NEAR), rows, dim), BF16),
                pltpu.SemaphoreType.DMA((2,)),
                pltpu.SemaphoreType.DMA((own,)),
                pltpu.SemaphoreType.DMA((1,)),
                pltpu.SemaphoreType.DMA((n_seq,)),
                pltpu.SemaphoreType.DMA((2,)),
                pltpu.SemaphoreType.DMA((len(NEAR) + 10,)),
            ],
            compiler_params=pltpu.CompilerParams(
                collective_id=0, has_side_effects=True, vmem_limit_bytes=48 * 1024 * 1024
            ),
            name="gmlp_block",
        )(*[pltpu.with_memory_space_constraint(v, pltpu.HBM) for v in operands])

    return jax.shard_map(per_device, mesh=mesh, in_specs=in_specs, out_specs=row_spec, check_vma=False)
```

```python
import functools

import jax
import jax.numpy as jnp
from jax import lax
from jax.experimental import pallas as pl
from jax.experimental.pallas import tpu as pltpu
from jax.sharding import PartitionSpec as P

LN_EPS = 1e-6
MESH = pl.DeviceIdType.MESH
F32 = jnp.float32
BF16 = jnp.bfloat16
TILE = 256
NEAR = (1, 3)
FAR = (2,)
EARLY = 4


def layer_norm(values, gain_vec, offset):
    values_f = values.astype(F32)
    mean_val = jnp.mean(values_f, axis=-1, keepdims=True)
    centered = values_f - mean_val
    var_val = jnp.mean(centered * centered, axis=-1, keepdims=True)
    return (centered * lax.rsqrt(var_val + LN_EPS) * gain_vec + offset).astype(BF16)


def as_row(ref):
    return ref[...].reshape(1, ref.shape[0])


def gelu(hidden):
    half = 0.5 * hidden
    return (half + half * lax.erf(hidden * (0.5 ** 0.5))).astype(BF16)


def block_kernel(n_seq, axis, x_hbm, ln1_gain_hbm, ln1_bias_hbm, w_in_hbm, b_in_hbm, ln2_gain_hbm, ln2_bias_hbm, w_spatial_hbm,
                 b_spatial_hbm, w_out_hbm, b_out_hbm, out_ref, x_buf, o_buf, n_buf, a_buf, ln1_gain, ln1_bias, w_in, b_in, ln2_gain,
                 ln2_bias, w_spatial, b_spatial, w_out, b_out, w_mix, bias_col, x_stage, near_sem, far_sem,
                 relay, x_relay, in_send, in_recv, out_send, out_recv, relay_sem, bypass_sem, w_sem):
    me = lax.axis_index(axis)
    images, rows, _ = x_hbm.shape
    own = images // n_seq
    patches = rows * n_seq
    half_dim = w_out.shape[0]
    per_tile = TILE // rows
    tiles = patches // TILE
    groups = tiles
    home = me // per_tile

    def block_rows(dev):
        return pl.ds(pl.multiple_of(dev * rows, rows), rows)

    def across(group, part):
        return lax.rem(home + group, groups) * per_tile + part

    def send_block(src, dev, slot, sem):
        pltpu.make_async_remote_copy(
            src_ref=src,
            dst_ref=x_buf.at[slot, block_rows(me)],
            send_sem=sem,
            recv_sem=in_recv.at[slot],
            device_id={axis: dev},
            device_id_type=MESH,
        ).start()

    core = lax.rem(me, per_tile)
    mate = across(0, per_tile - 1 - core)
    side = [across(group, core) for group in NEAR]
    cross = [across(group, per_tile - 1 - core) for group in NEAR]
    far = [across(group, part) for group in FAR for part in range(per_tile)]

    stage = [pltpu.make_async_copy(x_hbm.at[dev * own], x_stage.at[k], w_sem.at[k]) for k, dev in enumerate(side)]
    for load in stage:
        load.start()

    barrier = pltpu.get_barrier_semaphore()
    for dev in side + [mate]:
        pl.semaphore_signal(barrier, inc=1, device_id={axis: dev}, device_id_type=MESH)
    pl.semaphore_wait(barrier, len(side) + 1)

    for dev in side:
        pl.semaphore_signal(near_sem, inc=1, device_id={axis: dev}, device_id_type=MESH)
    for k, dev in enumerate(side):
        stage[k].wait()
        send_block(x_stage.at[k], dev, 0, in_send.at[0])
    for slot in range(1, EARLY):
        for dev in side:
            send_block(x_hbm.at[dev * own + slot], dev, slot, in_send.at[1])
    pl.semaphore_wait(near_sem, len(side))

    pl.semaphore_signal(far_sem, inc=1, device_id={axis: mate}, device_id_type=MESH)
    for slot in range(EARLY):
        for dev in cross:
            send_block(x_hbm.at[dev * own + slot], dev, slot, in_send.at[1])
    pl.semaphore_wait(far_sem, 1)
    for slot in range(EARLY):
        for dev in far + [mate]:
            send_block(x_hbm.at[dev * own + slot], dev, slot, in_send.at[1])

    inner = (core > 0) & (home > 0) & (home < groups - 1)
    opposite = (groups - 1 - home) * per_tile + core

    @pl.when(inner)
    def _():
        pltpu.make_async_remote_copy(
            src_ref=x_hbm.at[far[-1] * own + own - 1],
            dst_ref=x_relay,
            send_sem=in_send.at[1],
            recv_sem=bypass_sem.at[0],
            device_id={axis: opposite},
            device_id_type=MESH,
        ).start()

    @pl.loop(EARLY, own)
    def _(slot):
        for dev in side + cross + far[:-1] + [mate]:
            send_block(x_hbm.at[dev * own + slot], dev, slot, in_send.at[1])

        @pl.when(jnp.logical_not(inner & (slot == own - 1)))
        def _():
            send_block(x_hbm.at[far[-1] * own + slot], far[-1], slot, in_send.at[1])

    @pl.loop(0, own)
    def _(slot):
        pltpu.make_async_copy(x_hbm.at[me * own + slot], x_buf.at[slot, block_rows(me)], in_recv.at[slot]).start()

    operands = [
        (b_spatial_hbm, b_spatial), (w_spatial_hbm, w_spatial), (ln1_gain_hbm, ln1_gain), (ln1_bias_hbm, ln1_bias), (w_in_hbm, w_in),
        (b_in_hbm, b_in), (ln2_gain_hbm, ln2_gain), (ln2_bias_hbm, ln2_bias), (w_out_hbm, w_out), (b_out_hbm, b_out),
    ]
    loads = [pltpu.make_async_copy(src, dst, w_sem.at[len(NEAR) + k]) for k, (src, dst) in enumerate(operands)]
    for load in loads:
        load.start()
    loads[0].wait()
    for first in range(0, patches, 128):
        lane_bias = jnp.broadcast_to(b_spatial[first:first + 128].reshape(1, 128), (128, 128))
        bias_col[first:first + 128, :] = lane_bias.T
    loads[1].wait()

    @pl.loop(0, patches // TILE)
    def _(step):
        out_rows = pl.ds(pl.multiple_of(step * TILE, TILE), TILE)
        for first in range(0, patches, TILE):
            w_mix[out_rows, first:first + TILE] = w_spatial[first:first + TILE, out_rows].T

    for load in loads[2:]:
        load.wait()

    def send_result(src, owner, slot, dev, sem):
        pltpu.make_async_remote_copy(
            src_ref=src,
            dst_ref=out_ref.at[owner * own + slot],
            send_sem=sem,
            recv_sem=out_recv.at[owner],
            device_id={axis: dev},
            device_id_type=MESH,
        ).start()

    def send_tile(slot, tile, group):
        for part in reversed(range(per_tile)):
            dev = tile * per_tile + part
            src = o_buf.at[slot, block_rows(dev)]
            if part > 0 or group not in NEAR:
                send_result(src, me, slot, dev, out_send.at[0])
                continue
            handed = (slot == own - 1) & (core > 0)

            @pl.when(jnp.logical_not(handed))
            def _():
                send_result(src, me, slot, dev, out_send.at[0])

            @pl.when(handed)
            def _():
                pltpu.make_async_remote_copy(
                    src_ref=src,
                    dst_ref=relay.at[NEAR.index(group)],
                    send_sem=out_send.at[0],
                    recv_sem=relay_sem.at[0],
                    device_id={axis: mate},
                    device_id_type=MESH,
                ).start()

    def send_home(slot):
        pltpu.make_async_copy(o_buf.at[slot, block_rows(me)], out_ref.at[me * own + slot], out_recv.at[me]).start()
        send_result(o_buf.at[slot, block_rows(mate)], me, slot, mate, out_send.at[0])

    @pl.loop(0, own)
    def _(slot):
        pltpu.make_async_copy(x_buf.at[slot], x_buf.at[slot], in_recv.at[slot]).wait()

        @pl.loop(0, tiles)
        def _(tile):
            here = pl.ds(pl.multiple_of(tile * TILE, TILE), TILE)
            normed = layer_norm(x_buf[slot, here, :], as_row(ln1_gain), as_row(ln1_bias))
            gate = []
            for first in range(0, 2 * half_dim, 256):
                cols = slice(first, first + 256)
                hidden = jnp.dot(normed, w_in[:, cols], preferred_element_type=F32) + b_in[cols].reshape(1, 256)
                act = gelu(hidden)
                if first < half_dim:
                    a_buf[here, cols] = act
                else:
                    gate.append(act)
            gate = jnp.concatenate(gate, axis=1)
            n_buf[here, :] = layer_norm(gate, as_row(ln2_gain), as_row(ln2_bias))

        @pl.when(slot > 0)
        def _():
            send_home(slot - 1)

        @pl.when(inner & (slot == 1))
        def _():
            pltpu.make_async_copy(x_relay, x_relay, bypass_sem.at[0]).wait()
            pltpu.make_async_remote_copy(
                src_ref=x_relay,
                dst_ref=x_buf.at[own - 1, block_rows(opposite)],
                send_sem=bypass_sem.at[1],
                recv_sem=in_recv.at[own - 1],
                device_id={axis: lax.rem(groups + 1 - home, groups) * per_tile + core},
                device_id_type=MESH,
            ).start()

        previous = None
        for group in FAR + NEAR + (0,):
            tile = lax.rem(home + group, groups)
            here = pl.ds(pl.multiple_of(tile * TILE, TILE), TILE)
            spatial = jnp.dot(w_mix[here, :], n_buf[...], preferred_element_type=F32).astype(BF16)
            bias = jnp.tile(bias_col[here, :], (1, half_dim // 128))
            gated = (a_buf[here, :].astype(F32) * (spatial.astype(F32) + bias)).astype(BF16)
            mixed = jnp.dot(gated, w_out[...], preferred_element_type=F32) + as_row(b_out)
            o_buf[slot, here, :] = (x_buf[slot, here, :].astype(F32) + mixed).astype(BF16)
            if previous is not None:
                send_tile(slot, *previous)
            previous = tile, group

    @pl.when(core == 0)
    def _():
        pltpu.make_async_copy(relay, relay, relay_sem.at[0]).wait()
        for k, group in enumerate(NEAR):
            send_result(relay.at[k], mate, own - 1, across(group, 0), relay_sem.at[1])

    send_home(own - 1)

    pltpu.make_async_copy(x_stage, x_stage, in_send.at[0]).wait()
    rest_sent = [x_buf.at[pl.ds(1, own - 1), pl.ds(0, rows * (n_seq - 1))], x_buf.at[0, pl.ds(0, rows * (n_seq - 1 - len(NEAR)))]]
    for part in rest_sent:
        pltpu.make_async_copy(part, part, in_send.at[1]).wait()
    sent = o_buf.at[:, pl.ds(0, rows * (n_seq - 1))]
    pltpu.make_async_copy(sent, sent, out_send.at[0]).wait()

    @pl.when(core == 0)
    def _():
        pltpu.make_async_copy(relay, relay, relay_sem.at[1]).wait()

    @pl.when(inner)
    def _():
        pltpu.make_async_copy(x_relay, x_relay, bypass_sem.at[1]).wait()

    for dev in range(n_seq):
        part = out_ref.at[pl.ds(dev * own, own)]
        pltpu.make_async_copy(part, part, out_recv.at[dev]).wait()


def solution(mesh):
    row_spec = P("data", "seq", None)
    vec_spec = P(None)
    mat_spec = P(None, None)
    in_specs = (row_spec, vec_spec, vec_spec, mat_spec, vec_spec, vec_spec, vec_spec, mat_spec, vec_spec, mat_spec, vec_spec)
    n_seq = mesh.shape["seq"]

    def per_device(patches, ln1_gain, ln1_bias, w_in, b_in, ln2_gain, ln2_bias, w_spatial, b_spatial, w_out, b_out):
        operands = (patches, ln1_gain, ln1_bias, w_in, b_in, ln2_gain, ln2_bias, w_spatial, b_spatial, w_out, b_out)
        images, rows, dim = patches.shape
        own = images // n_seq
        total = rows * n_seq
        half_dim = w_out.shape[0]
        hbm = pl.BlockSpec(memory_space=pltpu.HBM)
        vec = lambda ref: pltpu.VMEM(ref.shape, ref.dtype)
        return pl.pallas_call(
            functools.partial(block_kernel, n_seq, "seq"),
            out_shape=pltpu.VMEM(patches.shape, BF16),
            in_specs=[hbm] * 11,
            out_specs=pl.BlockSpec(memory_space=pltpu.VMEM),
            scratch_shapes=[
                pltpu.VMEM((own, total, dim), BF16),
                pltpu.VMEM((own, total, dim), BF16),
                pltpu.VMEM((total, half_dim), BF16),
                pltpu.VMEM((total, half_dim), BF16),
                *[vec(v) for v in operands[1:]],
                pltpu.VMEM(w_spatial.shape, BF16),
                pltpu.VMEM((total, 128), F32),
                pltpu.VMEM((len(NEAR), rows, dim), BF16),
                pltpu.SemaphoreType.REGULAR,
                pltpu.SemaphoreType.REGULAR,
                pltpu.VMEM((len(NEAR), rows, dim), BF16),
                pltpu.VMEM((rows, dim), BF16),
                pltpu.SemaphoreType.DMA((2,)),
                pltpu.SemaphoreType.DMA((own,)),
                pltpu.SemaphoreType.DMA((1,)),
                pltpu.SemaphoreType.DMA((n_seq,)),
                pltpu.SemaphoreType.DMA((2,)),
                pltpu.SemaphoreType.DMA((2,)),
                pltpu.SemaphoreType.DMA((len(NEAR) + 10,)),
            ],
            compiler_params=pltpu.CompilerParams(
                collective_id=0, has_side_effects=True, vmem_limit_bytes=48 * 1024 * 1024
            ),
            name="gmlp_block",
        )(*[pltpu.with_memory_space_constraint(v, pltpu.HBM) for v in operands])

    return jax.shard_map(per_device, mesh=mesh, in_specs=in_specs, out_specs=row_spec, check_vma=False)
```

```python
import functools

import jax
import jax.numpy as jnp
from jax import lax
from jax.experimental import pallas as pl
from jax.experimental.pallas import tpu as pltpu
from jax.sharding import PartitionSpec as P

LN_EPS = 1e-6
MESH = pl.DeviceIdType.MESH
F32 = jnp.float32
BF16 = jnp.bfloat16
TILE = 256
NEAR = (1, 3)
FAR = (2,)
EARLY = 4


def layer_norm(values, gain_vec, offset):
    values_f = values.astype(F32)
    mean_val = jnp.mean(values_f, axis=-1, keepdims=True)
    centered = values_f - mean_val
    var_val = jnp.mean(centered * centered, axis=-1, keepdims=True)
    return (centered * lax.rsqrt(var_val + LN_EPS) * gain_vec + offset).astype(BF16)


def as_row(ref):
    return ref[...].reshape(1, ref.shape[0])


def gelu(hidden):
    half = 0.5 * hidden
    return (half + half * lax.erf(hidden * (0.5 ** 0.5))).astype(BF16)


def block_kernel(n_seq, axis, x_hbm, ln1_gain_hbm, ln1_bias_hbm, w_in_hbm, b_in_hbm, ln2_gain_hbm, ln2_bias_hbm, w_spatial_hbm,
                 b_spatial_hbm, w_out_hbm, b_out_hbm, out_ref, x_buf, o_buf, n_buf, a_buf, ln1_gain, ln1_bias, w_in, b_in, ln2_gain,
                 ln2_bias, w_spatial, b_spatial, w_out, b_out, w_mix, bias_col, x_stage, near_sem, far_sem,
                 relay, x_relay, in_send, in_recv, out_send, out_recv, relay_sem, bypass_sem, w_sem):
    me = lax.axis_index(axis)
    images, rows, _ = x_hbm.shape
    own = images // n_seq
    patches = rows * n_seq
    half_dim = w_out.shape[0]
    per_tile = TILE // rows
    tiles = patches // TILE
    groups = tiles
    home = me // per_tile

    def block_rows(dev):
        return pl.ds(pl.multiple_of(dev * rows, rows), rows)

    def across(group, part):
        return lax.rem(home + group, groups) * per_tile + part

    def send_block(src, dev, slot, sem):
        pltpu.make_async_remote_copy(
            src_ref=src,
            dst_ref=x_buf.at[slot, block_rows(me)],
            send_sem=sem,
            recv_sem=in_recv.at[slot],
            device_id={axis: dev},
            device_id_type=MESH,
        ).start()

    core = lax.rem(me, per_tile)
    mate = across(0, per_tile - 1 - core)
    side = [across(group, core) for group in NEAR]
    cross = [across(group, per_tile - 1 - core) for group in NEAR]
    far = [across(group, part) for group in FAR for part in range(per_tile)]

    stage = [pltpu.make_async_copy(x_hbm.at[dev * own], x_stage.at[k], w_sem.at[k]) for k, dev in enumerate(side)]
    for load in stage:
        load.start()

    barrier = pltpu.get_barrier_semaphore()
    for dev in side + [mate]:
        pl.semaphore_signal(barrier, inc=1, device_id={axis: dev}, device_id_type=MESH)
    pl.semaphore_wait(barrier, len(side) + 1)

    for dev in side:
        pl.semaphore_signal(near_sem, inc=1, device_id={axis: dev}, device_id_type=MESH)
    for k, dev in enumerate(side):
        stage[k].wait()
        send_block(x_stage.at[k], dev, 0, in_send.at[0])
    for slot in range(1, EARLY):
        for dev in side:
            send_block(x_hbm.at[dev * own + slot], dev, slot, in_send.at[1])
    pl.semaphore_wait(near_sem, len(side))

    pl.semaphore_signal(far_sem, inc=1, device_id={axis: mate}, device_id_type=MESH)
    for slot in range(EARLY):
        for dev in cross:
            send_block(x_hbm.at[dev * own + slot], dev, slot, in_send.at[1])
    pl.semaphore_wait(far_sem, 1)
    for slot in range(EARLY):
        for dev in far + [mate]:
            send_block(x_hbm.at[dev * own + slot], dev, slot, in_send.at[1])

    inner = (core > 0) & (home > 0) & (home < groups - 1)
    opposite = (groups - 1 - home) * per_tile + core

    @pl.when(inner)
    def _():
        pltpu.make_async_remote_copy(
            src_ref=x_hbm.at[far[-1] * own + own - 1],
            dst_ref=x_relay,
            send_sem=in_send.at[1],
            recv_sem=bypass_sem.at[0],
            device_id={axis: opposite},
            device_id_type=MESH,
        ).start()

    @pl.loop(EARLY, own)
    def _(slot):
        for dev in side + cross + far[:-1] + [mate]:
            send_block(x_hbm.at[dev * own + slot], dev, slot, in_send.at[1])

        @pl.when(jnp.logical_not(inner & (slot == own - 1)))
        def _():
            send_block(x_hbm.at[far[-1] * own + slot], far[-1], slot, in_send.at[1])

    @pl.loop(0, own)
    def _(slot):
        pltpu.make_async_copy(x_hbm.at[me * own + slot], x_buf.at[slot, block_rows(me)], in_recv.at[slot]).start()

    operands = [
        (b_spatial_hbm, b_spatial), (w_spatial_hbm, w_spatial), (ln1_gain_hbm, ln1_gain), (ln1_bias_hbm, ln1_bias), (w_in_hbm, w_in),
        (b_in_hbm, b_in), (ln2_gain_hbm, ln2_gain), (ln2_bias_hbm, ln2_bias), (w_out_hbm, w_out), (b_out_hbm, b_out),
    ]
    loads = [pltpu.make_async_copy(src, dst, w_sem.at[len(NEAR) + k]) for k, (src, dst) in enumerate(operands)]
    for load in loads:
        load.start()
    loads[0].wait()
    for first in range(0, patches, 128):
        lane_bias = jnp.broadcast_to(b_spatial[first:first + 128].reshape(1, 128), (128, 128))
        bias_col[first:first + 128, :] = lane_bias.T
    loads[1].wait()

    @pl.loop(0, patches // TILE)
    def _(step):
        out_rows = pl.ds(pl.multiple_of(step * TILE, TILE), TILE)
        for first in range(0, patches, TILE):
            w_mix[out_rows, first:first + TILE] = w_spatial[first:first + TILE, out_rows].T

    for load in loads[2:]:
        load.wait()

    def send_result(src, owner, slot, dev, sem):
        pltpu.make_async_remote_copy(
            src_ref=src,
            dst_ref=out_ref.at[owner * own + slot],
            send_sem=sem,
            recv_sem=out_recv.at[owner],
            device_id={axis: dev},
            device_id_type=MESH,
        ).start()

    def send_tile(slot, tile, group):
        for part in reversed(range(per_tile)):
            dev = tile * per_tile + part
            src = o_buf.at[slot, block_rows(dev)]
            if part > 0 or group not in NEAR:
                send_result(src, me, slot, dev, out_send.at[0])
                continue
            handed = (slot == own - 1) & (core > 0)

            @pl.when(jnp.logical_not(handed))
            def _():
                send_result(src, me, slot, dev, out_send.at[0])

            @pl.when(handed)
            def _():
                pltpu.make_async_remote_copy(
                    src_ref=src,
                    dst_ref=relay.at[NEAR.index(group)],
                    send_sem=out_send.at[0],
                    recv_sem=relay_sem.at[0],
                    device_id={axis: mate},
                    device_id_type=MESH,
                ).start()

    def send_home(slot):
        pltpu.make_async_copy(o_buf.at[slot, block_rows(me)], out_ref.at[me * own + slot], out_recv.at[me]).start()
        send_result(o_buf.at[slot, block_rows(mate)], me, slot, mate, out_send.at[0])

    @pl.loop(0, own)
    def _(slot):
        pltpu.make_async_copy(x_buf.at[slot], x_buf.at[slot], in_recv.at[slot]).wait()

        @pl.loop(0, tiles)
        def _(tile):
            here = pl.ds(pl.multiple_of(tile * TILE, TILE), TILE)
            normed = layer_norm(x_buf[slot, here, :], as_row(ln1_gain), as_row(ln1_bias))
            gate = []
            for first in range(0, 2 * half_dim, 256):
                cols = slice(first, first + 256)
                hidden = jnp.dot(normed, w_in[:, cols], preferred_element_type=F32) + b_in[cols].reshape(1, 256)
                act = gelu(hidden)
                if first < half_dim:
                    a_buf[here, cols] = act
                else:
                    gate.append(act)
            gate = jnp.concatenate(gate, axis=1)
            n_buf[here, :] = layer_norm(gate, as_row(ln2_gain), as_row(ln2_bias))

        @pl.when(slot > 0)
        def _():
            send_home(slot - 1)

        @pl.when(inner & (slot == 1))
        def _():
            pltpu.make_async_copy(x_relay, x_relay, bypass_sem.at[0]).wait()
            pltpu.make_async_remote_copy(
                src_ref=x_relay,
                dst_ref=x_buf.at[own - 1, block_rows(opposite)],
                send_sem=bypass_sem.at[1],
                recv_sem=in_recv.at[own - 1],
                device_id={axis: lax.rem(groups + 1 - home, groups) * per_tile + core},
                device_id_type=MESH,
            ).start()

        previous = None
        for group in FAR + NEAR + (0,):
            tile = lax.rem(home + group, groups)
            here = pl.ds(pl.multiple_of(tile * TILE, TILE), TILE)
            spatial = jnp.dot(w_mix[here, :], n_buf[...], preferred_element_type=F32).astype(BF16)
            bias = jnp.tile(bias_col[here, :], (1, half_dim // 128))
            gated = (a_buf[here, :].astype(F32) * (spatial.astype(F32) + bias)).astype(BF16)
            mixed = jnp.dot(gated, w_out[...], preferred_element_type=F32) + as_row(b_out)
            o_buf[slot, here, :] = (x_buf[slot, here, :].astype(F32) + mixed).astype(BF16)
            if previous is not None:
                send_tile(slot, *previous)
            previous = tile, group

    @pl.when(core == 0)
    def _():
        pltpu.make_async_copy(relay, relay, relay_sem.at[0]).wait()
        for k, group in enumerate(NEAR):
            send_result(relay.at[k], mate, own - 1, across(group, 0), relay_sem.at[1])

    send_home(own - 1)

    pltpu.make_async_copy(x_stage, x_stage, in_send.at[0]).wait()
    rest_sent = [x_buf.at[pl.ds(1, own - 1), pl.ds(0, rows * (n_seq - 1))], x_buf.at[0, pl.ds(0, rows * (n_seq - 1 - len(NEAR)))]]
    for part in rest_sent:
        pltpu.make_async_copy(part, part, in_send.at[1]).wait()
    sent = o_buf.at[:, pl.ds(0, rows * (n_seq - 1))]
    pltpu.make_async_copy(sent, sent, out_send.at[0]).wait()

    @pl.when(core == 0)
    def _():
        pltpu.make_async_copy(relay, relay, relay_sem.at[1]).wait()

    @pl.when(inner)
    def _():
        pltpu.make_async_copy(x_relay, x_relay, bypass_sem.at[1]).wait()

    for dev in range(n_seq):
        part = out_ref.at[pl.ds(dev * own, own)]
        pltpu.make_async_copy(part, part, out_recv.at[dev]).wait()


def put_out_kernel(pieces, src_ref, out_ref, sem):
    size = src_ref.shape[0] // pieces
    copies = [pltpu.make_async_copy(src_ref.at[pl.ds(k * size, size)], out_ref.at[pl.ds(k * size, size)], sem.at[k])
              for k in range(pieces)]
    for copy in copies:
        copy.start()
    for copy in copies:
        copy.wait()


def solution(mesh):
    row_spec = P("data", "seq", None)
    vec_spec = P(None)
    mat_spec = P(None, None)
    in_specs = (row_spec, vec_spec, vec_spec, mat_spec, vec_spec, vec_spec, vec_spec, mat_spec, vec_spec, mat_spec, vec_spec)
    n_seq = mesh.shape["seq"]

    def per_device(patches, ln1_gain, ln1_bias, w_in, b_in, ln2_gain, ln2_bias, w_spatial, b_spatial, w_out, b_out):
        operands = (patches, ln1_gain, ln1_bias, w_in, b_in, ln2_gain, ln2_bias, w_spatial, b_spatial, w_out, b_out)
        images, rows, dim = patches.shape
        own = images // n_seq
        total = rows * n_seq
        half_dim = w_out.shape[0]
        hbm = pl.BlockSpec(memory_space=pltpu.HBM)
        vec = lambda ref: pltpu.VMEM(ref.shape, ref.dtype)
        gathered = pl.pallas_call(
            functools.partial(block_kernel, n_seq, "seq"),
            out_shape=pltpu.VMEM(patches.shape, BF16),
            in_specs=[hbm] * 11,
            out_specs=pl.BlockSpec(memory_space=pltpu.VMEM),
            scratch_shapes=[
                pltpu.VMEM((own, total, dim), BF16),
                pltpu.VMEM((own, total, dim), BF16),
                pltpu.VMEM((total, half_dim), BF16),
                pltpu.VMEM((total, half_dim), BF16),
                *[vec(v) for v in operands[1:]],
                pltpu.VMEM(w_spatial.shape, BF16),
                pltpu.VMEM((total, 128), F32),
                pltpu.VMEM((len(NEAR), rows, dim), BF16),
                pltpu.SemaphoreType.REGULAR,
                pltpu.SemaphoreType.REGULAR,
                pltpu.VMEM((len(NEAR), rows, dim), BF16),
                pltpu.VMEM((rows, dim), BF16),
                pltpu.SemaphoreType.DMA((2,)),
                pltpu.SemaphoreType.DMA((own,)),
                pltpu.SemaphoreType.DMA((1,)),
                pltpu.SemaphoreType.DMA((n_seq,)),
                pltpu.SemaphoreType.DMA((2,)),
                pltpu.SemaphoreType.DMA((2,)),
                pltpu.SemaphoreType.DMA((len(NEAR) + 10,)),
            ],
            compiler_params=pltpu.CompilerParams(
                collective_id=0, has_side_effects=True, vmem_limit_bytes=48 * 1024 * 1024
            ),
            name="gmlp_block",
        )(*[pltpu.with_memory_space_constraint(v, pltpu.HBM) for v in operands])
        return pl.pallas_call(
            functools.partial(put_out_kernel, n_seq),
            out_shape=jax.ShapeDtypeStruct(patches.shape, BF16),
            in_specs=[pl.BlockSpec(memory_space=pltpu.VMEM)],
            out_specs=hbm,
            scratch_shapes=[pltpu.SemaphoreType.DMA((n_seq,))],
            compiler_params=pltpu.CompilerParams(vmem_limit_bytes=8 * 1024 * 1024),
            name="put_out",
        )(pltpu.with_memory_space_constraint(gathered, pltpu.VMEM))

    return jax.shard_map(per_device, mesh=mesh, in_specs=in_specs, out_specs=row_spec, check_vma=False)
```

```python
import functools

import jax
import jax.numpy as jnp
from jax import lax
from jax.experimental import pallas as pl
from jax.experimental.pallas import tpu as pltpu
from jax.sharding import PartitionSpec as P

LN_EPS = 1e-6
MESH = pl.DeviceIdType.MESH
F32 = jnp.float32
BF16 = jnp.bfloat16
TILE = 256
NEAR = (1, 3)
FAR = (2,)
EARLY = 4


def layer_norm(values, gain_vec, offset):
    values_f = values.astype(F32)
    mean_val = jnp.mean(values_f, axis=-1, keepdims=True)
    centered = values_f - mean_val
    var_val = jnp.mean(centered * centered, axis=-1, keepdims=True)
    return (centered * lax.rsqrt(var_val + LN_EPS) * gain_vec + offset).astype(BF16)


def as_row(ref):
    return ref[...].reshape(1, ref.shape[0])


def gelu(hidden):
    half = 0.5 * hidden
    return (half + half * lax.erf(hidden * (0.5 ** 0.5))).astype(BF16)


def block_kernel(n_seq, axis, x_hbm, ln1_gain_hbm, ln1_bias_hbm, w_in_hbm, b_in_hbm, ln2_gain_hbm, ln2_bias_hbm, w_spatial_hbm,
                 b_spatial_hbm, w_out_hbm, b_out_hbm, out_ref, x_buf, o_buf, n_buf, a_buf, ln1_gain, ln1_bias, w_in, b_in, ln2_gain,
                 ln2_bias, w_spatial, b_spatial, w_out, b_out, w_mix, bias_col, x_stage, late_sem, near_sem, far_sem,
                 relay, x_relay, in_send, in_recv, out_send, out_recv, relay_sem, bypass_sem, w_sem):
    me = lax.axis_index(axis)
    images, rows, _ = x_hbm.shape
    own = images // n_seq
    patches = rows * n_seq
    half_dim = w_out.shape[0]
    per_tile = TILE // rows
    tiles = patches // TILE
    groups = tiles
    home = me // per_tile

    def block_rows(dev):
        return pl.ds(pl.multiple_of(dev * rows, rows), rows)

    def across(group, part):
        return lax.rem(home + group, groups) * per_tile + part

    def send_block(src, dev, slot, sem):
        pltpu.make_async_remote_copy(
            src_ref=src,
            dst_ref=x_buf.at[slot, block_rows(me)],
            send_sem=sem,
            recv_sem=in_recv.at[slot],
            device_id={axis: dev},
            device_id_type=MESH,
        ).start()

    core = lax.rem(me, per_tile)
    mate = across(0, per_tile - 1 - core)
    late = home == groups - 1
    beside_late = lax.rem(home, 2) == 0
    upper = lax.rem(home // 2, 2)
    side = [across(1 + 2 * upper, core), across(groups - 1 - 2 * upper, core)]
    cross = [across(group, per_tile - 1 - core) for group in NEAR]
    far = [across(group, part) for group in FAR for part in range(per_tile)]

    stage = [pltpu.make_async_copy(x_hbm.at[dev * own], x_stage.at[k], w_sem.at[k]) for k, dev in enumerate(side)]
    for load in stage:
        load.start()

    barrier = pltpu.get_barrier_semaphore()
    pl.semaphore_signal(barrier, inc=1, device_id={axis: mate}, device_id_type=MESH)

    @pl.when(jnp.logical_not(late))
    def _():
        for dev in side:
            pl.semaphore_signal(barrier, inc=1, device_id={axis: dev}, device_id_type=MESH)

    pl.semaphore_wait(barrier, 2 + lax.rem(home, 2))

    @pl.when(late)
    def _():
        for dev in side:
            pl.semaphore_signal(late_sem, inc=1, device_id={axis: dev}, device_id_type=MESH)

    def send_early(k):
        stage[k].wait()
        send_block(x_stage.at[k], side[k], 0, in_send.at[0])
        for slot in range(1, EARLY):
            send_block(x_hbm.at[side[k] * own + slot], side[k], slot, in_send.at[1])

    send_early(0)

    @pl.when(beside_late)
    def _():
        pl.semaphore_wait(late_sem, 1)

    for dev in side:
        pl.semaphore_signal(near_sem, inc=1, device_id={axis: dev}, device_id_type=MESH)
    send_early(1)
    pl.semaphore_wait(near_sem, len(side))

    pl.semaphore_signal(far_sem, inc=1, device_id={axis: mate}, device_id_type=MESH)
    for slot in range(EARLY):
        for dev in cross:
            send_block(x_hbm.at[dev * own + slot], dev, slot, in_send.at[1])
    pl.semaphore_wait(far_sem, 1)
    for slot in range(EARLY):
        for dev in far + [mate]:
            send_block(x_hbm.at[dev * own + slot], dev, slot, in_send.at[1])

    inner = (core > 0) & (home > 0) & (home < groups - 1)
    opposite = (groups - 1 - home) * per_tile + core

    spared = [(own - 1, 0, rows, 0), (own - 2, 0, rows // 4, rows)]

    @pl.when(inner)
    def _():
        for slot, first, size, place in spared:
            pltpu.make_async_remote_copy(
                src_ref=x_hbm.at[far[-1] * own + slot, pl.ds(first, size)],
                dst_ref=x_relay.at[pl.ds(place, size)],
                send_sem=in_send.at[1],
                recv_sem=bypass_sem.at[0],
                device_id={axis: opposite},
                device_id_type=MESH,
            ).start()

    @pl.loop(EARLY, own)
    def _(slot):
        for dev in side + cross + far[:-1] + [mate]:
            send_block(x_hbm.at[dev * own + slot], dev, slot, in_send.at[1])

        @pl.when(jnp.logical_not(inner & (slot >= own - 2)))
        def _():
            send_block(x_hbm.at[far[-1] * own + slot], far[-1], slot, in_send.at[1])

        @pl.when(inner & (slot == own - 2))
        def _():
            rest = rows - rows // 4
            pltpu.make_async_remote_copy(
                src_ref=x_hbm.at[far[-1] * own + slot, pl.ds(rows // 4, rest)],
                dst_ref=x_buf.at[slot, pl.ds(pl.multiple_of(me * rows + rows // 4, rows // 4), rest)],
                send_sem=in_send.at[1],
                recv_sem=in_recv.at[slot],
                device_id={axis: far[-1]},
                device_id_type=MESH,
            ).start()

    @pl.loop(0, own)
    def _(slot):
        pltpu.make_async_copy(x_hbm.at[me * own + slot], x_buf.at[slot, block_rows(me)], in_recv.at[slot]).start()

    operands = [
        (b_spatial_hbm, b_spatial), (w_spatial_hbm, w_spatial), (ln1_gain_hbm, ln1_gain), (ln1_bias_hbm, ln1_bias), (w_in_hbm, w_in),
        (b_in_hbm, b_in), (ln2_gain_hbm, ln2_gain), (ln2_bias_hbm, ln2_bias), (w_out_hbm, w_out), (b_out_hbm, b_out),
    ]
    loads = [pltpu.make_async_copy(src, dst, w_sem.at[len(NEAR) + k]) for k, (src, dst) in enumerate(operands)]
    for load in loads:
        load.start()
    loads[0].wait()
    for first in range(0, patches, 128):
        lane_bias = jnp.broadcast_to(b_spatial[first:first + 128].reshape(1, 128), (128, 128))
        bias_col[first:first + 128, :] = lane_bias.T
    loads[1].wait()

    @pl.loop(0, patches // TILE)
    def _(step):
        out_rows = pl.ds(pl.multiple_of(step * TILE, TILE), TILE)
        for first in range(0, patches, TILE):
            w_mix[out_rows, first:first + TILE] = w_spatial[first:first + TILE, out_rows].T

    for load in loads[2:]:
        load.wait()

    def send_result(src, owner, slot, dev, sem):
        pltpu.make_async_remote_copy(
            src_ref=src,
            dst_ref=out_ref.at[owner * own + slot],
            send_sem=sem,
            recv_sem=out_recv.at[owner],
            device_id={axis: dev},
            device_id_type=MESH,
        ).start()

    def send_tile(slot, tile, group):
        for part in reversed(range(per_tile)):
            dev = tile * per_tile + part
            src = o_buf.at[slot, block_rows(dev)]
            if part > 0 or group not in NEAR:
                send_result(src, me, slot, dev, out_send.at[0])
                continue
            handed = (slot == own - 1) & (core > 0)

            @pl.when(jnp.logical_not(handed))
            def _():
                send_result(src, me, slot, dev, out_send.at[0])

            @pl.when(handed)
            def _():
                pltpu.make_async_remote_copy(
                    src_ref=src,
                    dst_ref=relay.at[NEAR.index(group)],
                    send_sem=out_send.at[0],
                    recv_sem=relay_sem.at[0],
                    device_id={axis: mate},
                    device_id_type=MESH,
                ).start()

    def send_home(slot):
        pltpu.make_async_copy(o_buf.at[slot, block_rows(me)], out_ref.at[me * own + slot], out_recv.at[me]).start()
        send_result(o_buf.at[slot, block_rows(mate)], me, slot, mate, out_send.at[0])

    @pl.loop(0, own)
    def _(slot):
        pltpu.make_async_copy(x_buf.at[slot], x_buf.at[slot], in_recv.at[slot]).wait()

        @pl.loop(0, tiles)
        def _(tile):
            here = pl.ds(pl.multiple_of(tile * TILE, TILE), TILE)
            normed = layer_norm(x_buf[slot, here, :], as_row(ln1_gain), as_row(ln1_bias))
            gate = []
            for first in range(0, 2 * half_dim, 256):
                cols = slice(first, first + 256)
                hidden = jnp.dot(normed, w_in[:, cols], preferred_element_type=F32) + b_in[cols].reshape(1, 256)
                act = gelu(hidden)
                if first < half_dim:
                    a_buf[here, cols] = act
                else:
                    gate.append(act)
            gate = jnp.concatenate(gate, axis=1)
            n_buf[here, :] = layer_norm(gate, as_row(ln2_gain), as_row(ln2_bias))

        @pl.when(slot > 0)
        def _():
            send_home(slot - 1)

        @pl.when(inner & (slot == 1))
        def _():
            pltpu.make_async_copy(x_relay, x_relay, bypass_sem.at[0]).wait()
            for spared_slot, first, size, place in spared:
                pltpu.make_async_remote_copy(
                    src_ref=x_relay.at[pl.ds(place, size)],
                    dst_ref=x_buf.at[spared_slot, pl.ds(pl.multiple_of(opposite * rows + first, size), size)],
                    send_sem=bypass_sem.at[1],
                    recv_sem=in_recv.at[spared_slot],
                    device_id={axis: lax.rem(groups + 1 - home, groups) * per_tile + core},
                    device_id_type=MESH,
                ).start()

        previous = None
        for group in FAR + NEAR + (0,):
            tile = lax.rem(home + group, groups)
            here = pl.ds(pl.multiple_of(tile * TILE, TILE), TILE)
            spatial = jnp.dot(w_mix[here, :], n_buf[...], preferred_element_type=F32).astype(BF16)
            bias = jnp.tile(bias_col[here, :], (1, half_dim // 128))
            gated = (a_buf[here, :].astype(F32) * (spatial.astype(F32) + bias)).astype(BF16)
            mixed = jnp.dot(gated, w_out[...], preferred_element_type=F32) + as_row(b_out)
            o_buf[slot, here, :] = (x_buf[slot, here, :].astype(F32) + mixed).astype(BF16)
            if previous is not None:
                send_tile(slot, *previous)
            previous = tile, group

    @pl.when(core == 0)
    def _():
        pltpu.make_async_copy(relay, relay, relay_sem.at[0]).wait()
        for k, group in enumerate(NEAR):
            send_result(relay.at[k], mate, own - 1, across(group, 0), relay_sem.at[1])

    send_home(own - 1)

    pltpu.make_async_copy(x_stage, x_stage, in_send.at[0]).wait()
    rest_sent = [x_buf.at[pl.ds(1, own - 1), pl.ds(0, rows * (n_seq - 1))], x_buf.at[0, pl.ds(0, rows * (n_seq - 1 - len(NEAR)))]]
    for part in rest_sent:
        pltpu.make_async_copy(part, part, in_send.at[1]).wait()
    sent = o_buf.at[:, pl.ds(0, rows * (n_seq - 1))]
    pltpu.make_async_copy(sent, sent, out_send.at[0]).wait()

    @pl.when(core == 0)
    def _():
        pltpu.make_async_copy(relay, relay, relay_sem.at[1]).wait()

    @pl.when(inner)
    def _():
        pltpu.make_async_copy(x_relay, x_relay, bypass_sem.at[1]).wait()

    for dev in range(n_seq):
        part = out_ref.at[pl.ds(dev * own, own)]
        pltpu.make_async_copy(part, part, out_recv.at[dev]).wait()


def solution(mesh):
    row_spec = P("data", "seq", None)
    vec_spec = P(None)
    mat_spec = P(None, None)
    in_specs = (row_spec, vec_spec, vec_spec, mat_spec, vec_spec, vec_spec, vec_spec, mat_spec, vec_spec, mat_spec, vec_spec)
    n_seq = mesh.shape["seq"]

    def per_device(patches, ln1_gain, ln1_bias, w_in, b_in, ln2_gain, ln2_bias, w_spatial, b_spatial, w_out, b_out):
        operands = (patches, ln1_gain, ln1_bias, w_in, b_in, ln2_gain, ln2_bias, w_spatial, b_spatial, w_out, b_out)
        images, rows, dim = patches.shape
        own = images // n_seq
        total = rows * n_seq
        half_dim = w_out.shape[0]
        hbm = pl.BlockSpec(memory_space=pltpu.HBM)
        vec = lambda ref: pltpu.VMEM(ref.shape, ref.dtype)
        return pl.pallas_call(
            functools.partial(block_kernel, n_seq, "seq"),
            out_shape=pltpu.VMEM(patches.shape, BF16),
            in_specs=[hbm] * 11,
            out_specs=pl.BlockSpec(memory_space=pltpu.VMEM),
            scratch_shapes=[
                pltpu.VMEM((own, total, dim), BF16),
                pltpu.VMEM((own, total, dim), BF16),
                pltpu.VMEM((total, half_dim), BF16),
                pltpu.VMEM((total, half_dim), BF16),
                *[vec(v) for v in operands[1:]],
                pltpu.VMEM(w_spatial.shape, BF16),
                pltpu.VMEM((total, 128), F32),
                pltpu.VMEM((len(NEAR), rows, dim), BF16),
                pltpu.SemaphoreType.REGULAR,
                pltpu.SemaphoreType.REGULAR,
                pltpu.SemaphoreType.REGULAR,
                pltpu.VMEM((len(NEAR), rows, dim), BF16),
                pltpu.VMEM((rows + rows // 4, dim), BF16),
                pltpu.SemaphoreType.DMA((2,)),
                pltpu.SemaphoreType.DMA((own,)),
                pltpu.SemaphoreType.DMA((1,)),
                pltpu.SemaphoreType.DMA((n_seq,)),
                pltpu.SemaphoreType.DMA((2,)),
                pltpu.SemaphoreType.DMA((2,)),
                pltpu.SemaphoreType.DMA((len(NEAR) + 10,)),
            ],
            compiler_params=pltpu.CompilerParams(
                collective_id=0, has_side_effects=True, vmem_limit_bytes=48 * 1024 * 1024
            ),
            name="gmlp_block",
        )(*[pltpu.with_memory_space_constraint(v, pltpu.HBM) for v in operands])

    return jax.shard_map(per_device, mesh=mesh, in_specs=in_specs, out_specs=row_spec, check_vma=False)
```

```python
import functools

import jax
import jax.numpy as jnp
from jax import lax
from jax.experimental import pallas as pl
from jax.experimental.pallas import tpu as pltpu
from jax.sharding import PartitionSpec as P

LN_EPS = 1e-6
MESH = pl.DeviceIdType.MESH
F32 = jnp.float32
BF16 = jnp.bfloat16
TILE = 256
NEAR = (1, 3)
FAR = (2,)
EARLY = 4


def layer_norm(values, gain_vec, offset):
    values_f = values.astype(F32)
    mean_val = jnp.mean(values_f, axis=-1, keepdims=True)
    centered = values_f - mean_val
    var_val = jnp.mean(centered * centered, axis=-1, keepdims=True)
    return (centered * lax.rsqrt(var_val + LN_EPS) * gain_vec + offset).astype(BF16)


def as_row(ref):
    return ref[...].reshape(1, ref.shape[0])


def gelu(hidden):
    half = 0.5 * hidden
    return (half + half * lax.erf(hidden * (0.5 ** 0.5))).astype(BF16)


def block_kernel(n_seq, axis, x_hbm, ln1_gain_hbm, ln1_bias_hbm, w_in_hbm, b_in_hbm, ln2_gain_hbm, ln2_bias_hbm, w_spatial_hbm,
                 b_spatial_hbm, w_out_hbm, b_out_hbm, out_ref, x_buf, o_buf, n_buf, a_buf, ln1_gain, ln1_bias, w_in, b_in, ln2_gain,
                 ln2_bias, w_spatial, b_spatial, w_out, b_out, w_mix, bias_col, x_stage, late_sem, near_sem, far_sem,
                 relay, x_relay, in_send, in_recv, out_send, out_recv, relay_sem, bypass_sem, w_sem):
    me = lax.axis_index(axis)
    images, rows, _ = x_hbm.shape
    own = images // n_seq
    patches = rows * n_seq
    half_dim = w_out.shape[0]
    per_tile = TILE // rows
    tiles = patches // TILE
    groups = tiles
    home = me // per_tile

    def block_rows(dev):
        return pl.ds(pl.multiple_of(dev * rows, rows), rows)

    def across(group, part):
        return lax.rem(home + group, groups) * per_tile + part

    def send_block(src, dev, slot, sem):
        pltpu.make_async_remote_copy(
            src_ref=src,
            dst_ref=x_buf.at[slot, block_rows(me)],
            send_sem=sem,
            recv_sem=in_recv.at[slot],
            device_id={axis: dev},
            device_id_type=MESH,
        ).start()

    core = lax.rem(me, per_tile)
    mate = across(0, per_tile - 1 - core)
    late = home == groups - 1
    beside_late = lax.rem(home, 2) == 0
    upper = lax.rem(home // 2, 2)
    side = [across(1 + 2 * upper, core), across(groups - 1 - 2 * upper, core)]
    cross = [across(group, per_tile - 1 - core) for group in NEAR]
    far = [across(group, part) for group in FAR for part in range(per_tile)]

    stage = [pltpu.make_async_copy(x_hbm.at[dev * own], x_stage.at[k], w_sem.at[k]) for k, dev in enumerate(side)]
    for load in stage:
        load.start()

    barrier = pltpu.get_barrier_semaphore()
    pl.semaphore_signal(barrier, inc=1, device_id={axis: mate}, device_id_type=MESH)

    @pl.when(jnp.logical_not(late))
    def _():
        for dev in side:
            pl.semaphore_signal(barrier, inc=1, device_id={axis: dev}, device_id_type=MESH)

    pl.semaphore_wait(barrier, 2 + lax.rem(home, 2))

    @pl.when(late)
    def _():
        for dev in side:
            pl.semaphore_signal(late_sem, inc=1, device_id={axis: dev}, device_id_type=MESH)

    def send_early(k):
        stage[k].wait()
        send_block(x_stage.at[k], side[k], 0, in_send.at[0])
        for slot in range(1, EARLY):
            send_block(x_hbm.at[side[k] * own + slot], side[k], slot, in_send.at[1])

    send_early(0)

    @pl.when(beside_late)
    def _():
        pl.semaphore_wait(late_sem, 1)

    for dev in side:
        pl.semaphore_signal(near_sem, inc=1, device_id={axis: dev}, device_id_type=MESH)
    send_early(1)
    operands = [
        (b_spatial_hbm, b_spatial), (w_spatial_hbm, w_spatial), (ln1_gain_hbm, ln1_gain), (ln1_bias_hbm, ln1_bias), (w_in_hbm, w_in),
        (b_in_hbm, b_in), (ln2_gain_hbm, ln2_gain), (ln2_bias_hbm, ln2_bias), (w_out_hbm, w_out), (b_out_hbm, b_out),
    ]
    loads = [pltpu.make_async_copy(src, dst, w_sem.at[len(NEAR) + k]) for k, (src, dst) in enumerate(operands)]
    for load in loads:
        load.start()
    pl.semaphore_wait(near_sem, len(side))

    pl.semaphore_signal(far_sem, inc=1, device_id={axis: mate}, device_id_type=MESH)
    for slot in range(EARLY):
        for dev in cross:
            send_block(x_hbm.at[dev * own + slot], dev, slot, in_send.at[1])
    pl.semaphore_wait(far_sem, 1)
    for slot in range(EARLY):
        for dev in far + [mate]:
            send_block(x_hbm.at[dev * own + slot], dev, slot, in_send.at[1])

    inner = (core > 0) & (home > 0) & (home < groups - 1)
    opposite = (groups - 1 - home) * per_tile + core
    spared = [(own - 1, 0, rows, 0), (own - 2, 0, rows // 4, rows)]

    @pl.when(inner)
    def _():
        for slot, first, size, place in spared:
            pltpu.make_async_remote_copy(
                src_ref=x_hbm.at[far[-1] * own + slot, pl.ds(first, size)],
                dst_ref=x_relay.at[pl.ds(place, size)],
                send_sem=in_send.at[1],
                recv_sem=bypass_sem.at[0],
                device_id={axis: opposite},
                device_id_type=MESH,
            ).start()

    @pl.loop(EARLY, own)
    def _(slot):
        for dev in side + cross + far[:-1] + [mate]:
            send_block(x_hbm.at[dev * own + slot], dev, slot, in_send.at[1])

        @pl.when(jnp.logical_not(inner & (slot >= own - 2)))
        def _():
            send_block(x_hbm.at[far[-1] * own + slot], far[-1], slot, in_send.at[1])

        @pl.when(inner & (slot == own - 2))
        def _():
            rest = rows - rows // 4
            pltpu.make_async_remote_copy(
                src_ref=x_hbm.at[far[-1] * own + slot, pl.ds(rows // 4, rest)],
                dst_ref=x_buf.at[slot, pl.ds(pl.multiple_of(me * rows + rows // 4, rows // 4), rest)],
                send_sem=in_send.at[1],
                recv_sem=in_recv.at[slot],
                device_id={axis: far[-1]},
                device_id_type=MESH,
            ).start()

    @pl.loop(0, own)
    def _(slot):
        pltpu.make_async_copy(x_hbm.at[me * own + slot], x_buf.at[slot, block_rows(me)], in_recv.at[slot]).start()

    loads[0].wait()
    for first in range(0, patches, 128):
        lane_bias = jnp.broadcast_to(b_spatial[first:first + 128].reshape(1, 128), (128, 128))
        bias_col[first:first + 128, :] = lane_bias.T
    loads[1].wait()

    @pl.loop(0, patches // TILE)
    def _(step):
        out_rows = pl.ds(pl.multiple_of(step * TILE, TILE), TILE)
        for first in range(0, patches, TILE):
            w_mix[out_rows, first:first + TILE] = w_spatial[first:first + TILE, out_rows].T

    for load in loads[2:]:
        load.wait()

    def send_result(src, owner, slot, dev, sem):
        pltpu.make_async_remote_copy(
            src_ref=src,
            dst_ref=out_ref.at[owner * own + slot],
            send_sem=sem,
            recv_sem=out_recv.at[owner],
            device_id={axis: dev},
            device_id_type=MESH,
        ).start()

    def send_tile(slot, tile, group):
        for part in reversed(range(per_tile)):
            dev = tile * per_tile + part
            src = o_buf.at[slot, block_rows(dev)]
            if part > 0 or group not in NEAR:
                send_result(src, me, slot, dev, out_send.at[0])
                continue
            handed = (slot == own - 1) & (core > 0)

            @pl.when(jnp.logical_not(handed))
            def _():
                send_result(src, me, slot, dev, out_send.at[0])

            @pl.when(handed)
            def _():
                pltpu.make_async_remote_copy(
                    src_ref=src,
                    dst_ref=relay.at[NEAR.index(group)],
                    send_sem=out_send.at[0],
                    recv_sem=relay_sem.at[0],
                    device_id={axis: mate},
                    device_id_type=MESH,
                ).start()

    def send_home(slot):
        pltpu.make_async_copy(o_buf.at[slot, block_rows(me)], out_ref.at[me * own + slot], out_recv.at[me]).start()
        send_result(o_buf.at[slot, block_rows(mate)], me, slot, mate, out_send.at[0])

    @pl.loop(0, own)
    def _(slot):
        pltpu.make_async_copy(x_buf.at[slot], x_buf.at[slot], in_recv.at[slot]).wait()

        @pl.loop(0, tiles)
        def _(tile):
            here = pl.ds(pl.multiple_of(tile * TILE, TILE), TILE)
            normed = layer_norm(x_buf[slot, here, :], as_row(ln1_gain), as_row(ln1_bias))
            gate = []
            for first in range(0, 2 * half_dim, 256):
                cols = slice(first, first + 256)
                hidden = jnp.dot(normed, w_in[:, cols], preferred_element_type=F32) + b_in[cols].reshape(1, 256)
                act = gelu(hidden)
                if first < half_dim:
                    a_buf[here, cols] = act
                else:
                    gate.append(act)
            gate = jnp.concatenate(gate, axis=1)
            n_buf[here, :] = layer_norm(gate, as_row(ln2_gain), as_row(ln2_bias))

        @pl.when(slot > 0)
        def _():
            send_home(slot - 1)

        @pl.when(inner & (slot == 1))
        def _():
            pltpu.make_async_copy(x_relay, x_relay, bypass_sem.at[0]).wait()
            for spared_slot, first, size, place in spared:
                pltpu.make_async_remote_copy(
                    src_ref=x_relay.at[pl.ds(place, size)],
                    dst_ref=x_buf.at[spared_slot, pl.ds(pl.multiple_of(opposite * rows + first, size), size)],
                    send_sem=bypass_sem.at[1],
                    recv_sem=in_recv.at[spared_slot],
                    device_id={axis: lax.rem(groups + 1 - home, groups) * per_tile + core},
                    device_id_type=MESH,
                ).start()

        previous = None
        for group in FAR + NEAR + (0,):
            tile = lax.rem(home + group, groups)
            here = pl.ds(pl.multiple_of(tile * TILE, TILE), TILE)
            spatial = jnp.dot(w_mix[here, :], n_buf[...], preferred_element_type=F32).astype(BF16)
            bias = jnp.tile(bias_col[here, :], (1, half_dim // 128))
            gated = (a_buf[here, :].astype(F32) * (spatial.astype(F32) + bias)).astype(BF16)
            mixed = jnp.dot(gated, w_out[...], preferred_element_type=F32) + as_row(b_out)
            o_buf[slot, here, :] = (x_buf[slot, here, :].astype(F32) + mixed).astype(BF16)
            if previous is not None:
                send_tile(slot, *previous)
            previous = tile, group

    @pl.when(core == 0)
    def _():
        pltpu.make_async_copy(relay, relay, relay_sem.at[0]).wait()
        for k, group in enumerate(NEAR):
            send_result(relay.at[k], mate, own - 1, across(group, 0), relay_sem.at[1])

    send_home(own - 1)

    pltpu.make_async_copy(x_stage, x_stage, in_send.at[0]).wait()
    rest_sent = [x_buf.at[pl.ds(1, own - 1), pl.ds(0, rows * (n_seq - 1))], x_buf.at[0, pl.ds(0, rows * (n_seq - 1 - len(NEAR)))]]
    for part in rest_sent:
        pltpu.make_async_copy(part, part, in_send.at[1]).wait()
    sent = o_buf.at[:, pl.ds(0, rows * (n_seq - 1))]
    pltpu.make_async_copy(sent, sent, out_send.at[0]).wait()

    @pl.when(core == 0)
    def _():
        pltpu.make_async_copy(relay, relay, relay_sem.at[1]).wait()

    @pl.when(inner)
    def _():
        pltpu.make_async_copy(x_relay, x_relay, bypass_sem.at[1]).wait()

    for dev in range(n_seq):
        part = out_ref.at[pl.ds(dev * own, own)]
        pltpu.make_async_copy(part, part, out_recv.at[dev]).wait()


def solution(mesh):
    row_spec = P("data", "seq", None)
    vec_spec = P(None)
    mat_spec = P(None, None)
    in_specs = (row_spec, vec_spec, vec_spec, mat_spec, vec_spec, vec_spec, vec_spec, mat_spec, vec_spec, mat_spec, vec_spec)
    n_seq = mesh.shape["seq"]

    def per_device(patches, ln1_gain, ln1_bias, w_in, b_in, ln2_gain, ln2_bias, w_spatial, b_spatial, w_out, b_out):
        operands = (patches, ln1_gain, ln1_bias, w_in, b_in, ln2_gain, ln2_bias, w_spatial, b_spatial, w_out, b_out)
        images, rows, dim = patches.shape
        own = images // n_seq
        total = rows * n_seq
        half_dim = w_out.shape[0]
        hbm = pl.BlockSpec(memory_space=pltpu.HBM)
        vec = lambda ref: pltpu.VMEM(ref.shape, ref.dtype)
        return pl.pallas_call(
            functools.partial(block_kernel, n_seq, "seq"),
            out_shape=pltpu.VMEM(patches.shape, BF16),
            in_specs=[hbm] * 11,
            out_specs=pl.BlockSpec(memory_space=pltpu.VMEM),
            scratch_shapes=[
                pltpu.VMEM((own, total, dim), BF16),
                pltpu.VMEM((own, total, dim), BF16),
                pltpu.VMEM((total, half_dim), BF16),
                pltpu.VMEM((total, half_dim), BF16),
                *[vec(v) for v in operands[1:]],
                pltpu.VMEM(w_spatial.shape, BF16),
                pltpu.VMEM((total, 128), F32),
                pltpu.VMEM((len(NEAR), rows, dim), BF16),
                pltpu.SemaphoreType.REGULAR,
                pltpu.SemaphoreType.REGULAR,
                pltpu.SemaphoreType.REGULAR,
                pltpu.VMEM((len(NEAR), rows, dim), BF16),
                pltpu.VMEM((rows + rows // 4, dim), BF16),
                pltpu.SemaphoreType.DMA((2,)),
                pltpu.SemaphoreType.DMA((own,)),
                pltpu.SemaphoreType.DMA((1,)),
                pltpu.SemaphoreType.DMA((n_seq,)),
                pltpu.SemaphoreType.DMA((2,)),
                pltpu.SemaphoreType.DMA((2,)),
                pltpu.SemaphoreType.DMA((len(NEAR) + 10,)),
            ],
            compiler_params=pltpu.CompilerParams(
                collective_id=0, has_side_effects=True, vmem_limit_bytes=48 * 1024 * 1024
            ),
            name="gmlp_block",
        )(*[pltpu.with_memory_space_constraint(v, pltpu.HBM) for v in operands])

    return jax.shard_map(per_device, mesh=mesh, in_specs=in_specs, out_specs=row_spec, check_vma=False)
```

```python
import functools

import jax
import jax.numpy as jnp
from jax import lax
from jax.experimental import pallas as pl
from jax.experimental.pallas import tpu as pltpu
from jax.sharding import PartitionSpec as P

LN_EPS = 1e-6
MESH = pl.DeviceIdType.MESH
F32 = jnp.float32
BF16 = jnp.bfloat16
TILE = 256
NEAR = (1, 3)
FAR = (2,)
EARLY = 4


def layer_norm(values, gain_vec, offset):
    values_f = values.astype(F32)
    mean_val = jnp.mean(values_f, axis=-1, keepdims=True)
    centered = values_f - mean_val
    var_val = jnp.mean(centered * centered, axis=-1, keepdims=True)
    return (centered * lax.rsqrt(var_val + LN_EPS) * gain_vec + offset).astype(BF16)


def as_row(ref):
    return ref[...].reshape(1, ref.shape[0])


def gelu(hidden):
    half = 0.5 * hidden
    return (half + half * lax.erf(hidden * (0.5 ** 0.5))).astype(BF16)


def block_kernel(n_seq, axis, x_hbm, ln1_gain_hbm, ln1_bias_hbm, w_in_hbm, b_in_hbm, ln2_gain_hbm, ln2_bias_hbm, w_spatial_hbm,
                 b_spatial_hbm, w_out_hbm, b_out_hbm, out_ref, x_buf, o_buf, n_buf, a_buf, ln1_gain, ln1_bias, w_in, b_in, ln2_gain,
                 ln2_bias, w_spatial, b_spatial, w_out, b_out, w_mix, bias_col, x_stage, late_sem, near_sem, far_sem,
                 relay, x_relay, in_send, in_recv, out_send, out_recv, relay_sem, bypass_sem, w_sem):
    me = lax.axis_index(axis)
    images, rows, _ = x_hbm.shape
    own = images // n_seq
    patches = rows * n_seq
    half_dim = w_out.shape[0]
    per_tile = TILE // rows
    tiles = patches // TILE
    groups = tiles
    home = me // per_tile

    def block_rows(dev):
        return pl.ds(pl.multiple_of(dev * rows, rows), rows)

    def across(group, part):
        return lax.rem(home + group, groups) * per_tile + part

    def send_block(src, dev, slot, sem):
        pltpu.make_async_remote_copy(
            src_ref=src,
            dst_ref=x_buf.at[slot, block_rows(me)],
            send_sem=sem,
            recv_sem=in_recv.at[slot],
            device_id={axis: dev},
            device_id_type=MESH,
        ).start()

    core = lax.rem(me, per_tile)
    mate = across(0, per_tile - 1 - core)
    late = home == groups - 1
    beside_late = lax.rem(home, 2) == 0
    upper = lax.rem(home // 2, 2)
    side = [across(1 + 2 * upper, core), across(groups - 1 - 2 * upper, core)]
    cross = [across(group, per_tile - 1 - core) for group in NEAR]
    far = [across(group, part) for group in FAR for part in range(per_tile)]

    stage = [pltpu.make_async_copy(x_hbm.at[dev * own], x_stage.at[k], w_sem.at[k]) for k, dev in enumerate(side)]
    for load in stage:
        load.start()

    barrier = pltpu.get_barrier_semaphore()
    pl.semaphore_signal(barrier, inc=1, device_id={axis: mate}, device_id_type=MESH)

    @pl.when(jnp.logical_not(late))
    def _():
        for dev in side:
            pl.semaphore_signal(barrier, inc=1, device_id={axis: dev}, device_id_type=MESH)

    pl.semaphore_wait(barrier, 2 + lax.rem(home, 2))

    @pl.when(late)
    def _():
        for dev in side:
            pl.semaphore_signal(late_sem, inc=1, device_id={axis: dev}, device_id_type=MESH)

    def send_early(k):
        stage[k].wait()
        send_block(x_stage.at[k], side[k], 0, in_send.at[0])
        for slot in range(1, EARLY):
            send_block(x_hbm.at[side[k] * own + slot], side[k], slot, in_send.at[1])

    send_early(0)

    @pl.when(beside_late)
    def _():
        pl.semaphore_wait(late_sem, 1)

    for dev in side:
        pl.semaphore_signal(near_sem, inc=1, device_id={axis: dev}, device_id_type=MESH)
    send_early(1)
    operands = [
        (b_spatial_hbm, b_spatial), (w_spatial_hbm, w_spatial), (ln1_gain_hbm, ln1_gain), (ln1_bias_hbm, ln1_bias), (w_in_hbm, w_in),
        (b_in_hbm, b_in), (ln2_gain_hbm, ln2_gain), (ln2_bias_hbm, ln2_bias), (w_out_hbm, w_out), (b_out_hbm, b_out),
    ]
    loads = [pltpu.make_async_copy(src, dst, w_sem.at[len(NEAR) + k]) for k, (src, dst) in enumerate(operands)]
    for load in loads:
        load.start()
    pl.semaphore_wait(near_sem, len(side))

    pl.semaphore_signal(far_sem, inc=1, device_id={axis: mate}, device_id_type=MESH)
    for slot in range(EARLY):
        for dev in cross:
            send_block(x_hbm.at[dev * own + slot], dev, slot, in_send.at[1])
    pl.semaphore_wait(far_sem, 1)
    for slot in range(EARLY):
        for dev in far + [mate]:
            send_block(x_hbm.at[dev * own + slot], dev, slot, in_send.at[1])

    inner = (core > 0) & (home > 0) & (home < groups - 1)
    opposite = (groups - 1 - home) * per_tile + core
    spared = [(own - 1, 0, rows, 0), (own - 2, 0, rows // 4, rows)]

    @pl.when(inner)
    def _():
        for slot, first, size, place in spared:
            pltpu.make_async_remote_copy(
                src_ref=x_hbm.at[far[-1] * own + slot, pl.ds(first, size)],
                dst_ref=x_relay.at[pl.ds(place, size)],
                send_sem=in_send.at[1],
                recv_sem=bypass_sem.at[0],
                device_id={axis: opposite},
                device_id_type=MESH,
            ).start()

    @pl.loop(EARLY, own)
    def _(slot):
        for dev in side + cross + far[:-1] + [mate]:
            send_block(x_hbm.at[dev * own + slot], dev, slot, in_send.at[1])

        @pl.when(jnp.logical_not(inner & (slot >= own - 2)))
        def _():
            send_block(x_hbm.at[far[-1] * own + slot], far[-1], slot, in_send.at[1])

        @pl.when(inner & (slot == own - 2))
        def _():
            rest = rows - rows // 4
            pltpu.make_async_remote_copy(
                src_ref=x_hbm.at[far[-1] * own + slot, pl.ds(rows // 4, rest)],
                dst_ref=x_buf.at[slot, pl.ds(pl.multiple_of(me * rows + rows // 4, rows // 4), rest)],
                send_sem=in_send.at[1],
                recv_sem=in_recv.at[slot],
                device_id={axis: far[-1]},
                device_id_type=MESH,
            ).start()

    @pl.loop(0, own)
    def _(slot):
        pltpu.make_async_copy(x_hbm.at[me * own + slot], x_buf.at[slot, block_rows(me)], in_recv.at[slot]).start()

    loads[0].wait()
    for first in range(0, patches, 128):
        lane_bias = jnp.broadcast_to(b_spatial[first:first + 128].reshape(1, 128), (128, 128))
        bias_col[first:first + 128, :] = lane_bias.T
    loads[1].wait()

    @pl.loop(0, patches // TILE)
    def _(step):
        out_rows = pl.ds(pl.multiple_of(step * TILE, TILE), TILE)
        for first in range(0, patches, TILE):
            w_mix[out_rows, first:first + TILE] = w_spatial[first:first + TILE, out_rows].T

    for load in loads[2:]:
        load.wait()

    def send_result(src, owner, slot, dev, sem):
        pltpu.make_async_remote_copy(
            src_ref=src,
            dst_ref=out_ref.at[owner * own + slot],
            send_sem=sem,
            recv_sem=out_recv.at[owner],
            device_id={axis: dev},
            device_id_type=MESH,
        ).start()

    def last_part(tile):
        return jnp.where(tile == 0, 0, per_tile - 1)

    def send_tile(slot, tile, group):
        first_dev = tile * per_tile + per_tile - 1 - last_part(tile)
        send_result(o_buf.at[slot, block_rows(first_dev)], me, slot, first_dev, out_send.at[0])
        dev = tile * per_tile + last_part(tile)
        src = o_buf.at[slot, block_rows(dev)]
        if group not in NEAR:
            send_result(src, me, slot, dev, out_send.at[0])
        else:
            handed = (slot == own - 1) & (core > 0)

            @pl.when(jnp.logical_not(handed))
            def _():
                send_result(src, me, slot, dev, out_send.at[0])

            @pl.when(handed)
            def _():
                pltpu.make_async_remote_copy(
                    src_ref=src,
                    dst_ref=relay.at[NEAR.index(group)],
                    send_sem=out_send.at[0],
                    recv_sem=relay_sem.at[0],
                    device_id={axis: mate},
                    device_id_type=MESH,
                ).start()

    def send_home(slot):
        pltpu.make_async_copy(o_buf.at[slot, block_rows(me)], out_ref.at[me * own + slot], out_recv.at[me]).start()
        send_result(o_buf.at[slot, block_rows(mate)], me, slot, mate, out_send.at[0])

    @pl.loop(0, own)
    def _(slot):
        pltpu.make_async_copy(x_buf.at[slot], x_buf.at[slot], in_recv.at[slot]).wait()

        @pl.loop(0, tiles)
        def _(tile):
            here = pl.ds(pl.multiple_of(tile * TILE, TILE), TILE)
            normed = layer_norm(x_buf[slot, here, :], as_row(ln1_gain), as_row(ln1_bias))
            gate = []
            for first in range(0, 2 * half_dim, 256):
                cols = slice(first, first + 256)
                hidden = jnp.dot(normed, w_in[:, cols], preferred_element_type=F32) + b_in[cols].reshape(1, 256)
                act = gelu(hidden)
                if first < half_dim:
                    a_buf[here, cols] = act
                else:
                    gate.append(act)
            gate = jnp.concatenate(gate, axis=1)
            n_buf[here, :] = layer_norm(gate, as_row(ln2_gain), as_row(ln2_bias))

        @pl.when(slot > 0)
        def _():
            send_home(slot - 1)

        @pl.when(inner & (slot == 1))
        def _():
            pltpu.make_async_copy(x_relay, x_relay, bypass_sem.at[0]).wait()
            for spared_slot, first, size, place in spared:
                pltpu.make_async_remote_copy(
                    src_ref=x_relay.at[pl.ds(place, size)],
                    dst_ref=x_buf.at[spared_slot, pl.ds(pl.multiple_of(opposite * rows + first, size), size)],
                    send_sem=bypass_sem.at[1],
                    recv_sem=in_recv.at[spared_slot],
                    device_id={axis: lax.rem(groups + 1 - home, groups) * per_tile + core},
                    device_id_type=MESH,
                ).start()

        previous = None
        for group in FAR + NEAR + (0,):
            tile = lax.rem(home + group, groups)
            here = pl.ds(pl.multiple_of(tile * TILE, TILE), TILE)
            spatial = jnp.dot(w_mix[here, :], n_buf[...], preferred_element_type=F32).astype(BF16)
            bias = jnp.tile(bias_col[here, :], (1, half_dim // 128))
            gated = (a_buf[here, :].astype(F32) * (spatial.astype(F32) + bias)).astype(BF16)
            mixed = jnp.dot(gated, w_out[...], preferred_element_type=F32) + as_row(b_out)
            o_buf[slot, here, :] = (x_buf[slot, here, :].astype(F32) + mixed).astype(BF16)
            if previous is not None:
                send_tile(slot, *previous)
            previous = tile, group

    @pl.when(core == 0)
    def _():
        pltpu.make_async_copy(relay, relay, relay_sem.at[0]).wait()
        for k, group in enumerate(NEAR):
            send_result(relay.at[k], mate, own - 1, across(group, last_part(across(group, 0) // per_tile)), relay_sem.at[1])

    send_home(own - 1)

    pltpu.make_async_copy(x_stage, x_stage, in_send.at[0]).wait()
    rest_sent = [x_buf.at[pl.ds(1, own - 1), pl.ds(0, rows * (n_seq - 1))], x_buf.at[0, pl.ds(0, rows * (n_seq - 1 - len(NEAR)))]]
    for part in rest_sent:
        pltpu.make_async_copy(part, part, in_send.at[1]).wait()
    sent = o_buf.at[:, pl.ds(0, rows * (n_seq - 1))]
    pltpu.make_async_copy(sent, sent, out_send.at[0]).wait()

    @pl.when(core == 0)
    def _():
        pltpu.make_async_copy(relay, relay, relay_sem.at[1]).wait()

    @pl.when(inner)
    def _():
        pltpu.make_async_copy(x_relay, x_relay, bypass_sem.at[1]).wait()

    for dev in range(n_seq):
        part = out_ref.at[pl.ds(dev * own, own)]
        pltpu.make_async_copy(part, part, out_recv.at[dev]).wait()


def solution(mesh):
    row_spec = P("data", "seq", None)
    vec_spec = P(None)
    mat_spec = P(None, None)
    in_specs = (row_spec, vec_spec, vec_spec, mat_spec, vec_spec, vec_spec, vec_spec, mat_spec, vec_spec, mat_spec, vec_spec)
    n_seq = mesh.shape["seq"]

    def per_device(patches, ln1_gain, ln1_bias, w_in, b_in, ln2_gain, ln2_bias, w_spatial, b_spatial, w_out, b_out):
        operands = (patches, ln1_gain, ln1_bias, w_in, b_in, ln2_gain, ln2_bias, w_spatial, b_spatial, w_out, b_out)
        images, rows, dim = patches.shape
        own = images // n_seq
        total = rows * n_seq
        half_dim = w_out.shape[0]
        hbm = pl.BlockSpec(memory_space=pltpu.HBM)
        vec = lambda ref: pltpu.VMEM(ref.shape, ref.dtype)
        return pl.pallas_call(
            functools.partial(block_kernel, n_seq, "seq"),
            out_shape=pltpu.VMEM(patches.shape, BF16),
            in_specs=[hbm] * 11,
            out_specs=pl.BlockSpec(memory_space=pltpu.VMEM),
            scratch_shapes=[
                pltpu.VMEM((own, total, dim), BF16),
                pltpu.VMEM((own, total, dim), BF16),
                pltpu.VMEM((total, half_dim), BF16),
                pltpu.VMEM((total, half_dim), BF16),
                *[vec(v) for v in operands[1:]],
                pltpu.VMEM(w_spatial.shape, BF16),
                pltpu.VMEM((total, 128), F32),
                pltpu.VMEM((len(NEAR), rows, dim), BF16),
                pltpu.SemaphoreType.REGULAR,
                pltpu.SemaphoreType.REGULAR,
                pltpu.SemaphoreType.REGULAR,
                pltpu.VMEM((len(NEAR), rows, dim), BF16),
                pltpu.VMEM((rows + rows // 4, dim), BF16),
                pltpu.SemaphoreType.DMA((2,)),
                pltpu.SemaphoreType.DMA((own,)),
                pltpu.SemaphoreType.DMA((1,)),
                pltpu.SemaphoreType.DMA((n_seq,)),
                pltpu.SemaphoreType.DMA((2,)),
                pltpu.SemaphoreType.DMA((2,)),
                pltpu.SemaphoreType.DMA((len(NEAR) + 10,)),
            ],
            compiler_params=pltpu.CompilerParams(
                collective_id=0, has_side_effects=True, vmem_limit_bytes=48 * 1024 * 1024
            ),
            name="gmlp_block",
        )(*[pltpu.with_memory_space_constraint(v, pltpu.HBM) for v in operands])

    return jax.shard_map(per_device, mesh=mesh, in_specs=in_specs, out_specs=row_spec, check_vma=False)
```

```python
import functools

import jax
import jax.numpy as jnp
from jax import lax
from jax.experimental import pallas as pl
from jax.experimental.pallas import tpu as pltpu
from jax.sharding import PartitionSpec as P

LN_EPS = 1e-6
MESH = pl.DeviceIdType.MESH
F32 = jnp.float32
BF16 = jnp.bfloat16
TILE = 256
NEAR = (1, 3)
FAR = (2,)
EARLY = 4


def layer_norm(values, gain_vec, offset):
    values_f = values.astype(F32)
    mean_val = jnp.mean(values_f, axis=-1, keepdims=True)
    centered = values_f - mean_val
    var_val = jnp.mean(centered * centered, axis=-1, keepdims=True)
    return (centered * lax.rsqrt(var_val + LN_EPS) * gain_vec + offset).astype(BF16)


def as_row(ref):
    return ref[...].reshape(1, ref.shape[0])


def gelu(hidden):
    half = 0.5 * hidden
    return (half + half * lax.erf(hidden * (0.5 ** 0.5))).astype(BF16)


def block_kernel(n_seq, axis, x_hbm, ln1_gain_hbm, ln1_bias_hbm, w_in_hbm, b_in_hbm, ln2_gain_hbm, ln2_bias_hbm, w_spatial_hbm,
                 b_spatial_hbm, w_out_hbm, b_out_hbm, out_ref, x_buf, o_buf, n_buf, a_buf, ln1_gain, ln1_bias, w_in, b_in, ln2_gain,
                 ln2_bias, w_spatial, b_spatial, w_out, b_out, w_mix, bias_col, x_stage, late_sem, near_sem, far_sem,
                 relay, x_relay, in_send, in_recv, out_send, out_recv, relay_sem, bypass_sem, w_sem):
    me = lax.axis_index(axis)
    images, rows, _ = x_hbm.shape
    own = images // n_seq
    patches = rows * n_seq
    half_dim = w_out.shape[0]
    per_tile = TILE // rows
    tiles = patches // TILE
    groups = tiles
    home = me // per_tile

    def block_rows(dev):
        return pl.ds(pl.multiple_of(dev * rows, rows), rows)

    def across(group, part):
        return lax.rem(home + group, groups) * per_tile + part

    def send_block(src, dev, slot, sem):
        pltpu.make_async_remote_copy(
            src_ref=src,
            dst_ref=x_buf.at[slot, block_rows(me)],
            send_sem=sem,
            recv_sem=in_recv.at[slot],
            device_id={axis: dev},
            device_id_type=MESH,
        ).start()

    core = lax.rem(me, per_tile)
    mate = across(0, per_tile - 1 - core)
    late = home == groups - 1
    beside_late = lax.rem(home, 2) == 0
    upper = lax.rem((home + 1) // 2, 2)
    side = [across(1 + 2 * upper, core), across(groups - 1 - 2 * upper, core)]
    cross = [across(group, per_tile - 1 - core) for group in NEAR]
    far = [across(group, part) for group in FAR for part in range(per_tile)]

    stage = [pltpu.make_async_copy(x_hbm.at[dev * own], x_stage.at[k], w_sem.at[k]) for k, dev in enumerate(side)]
    for load in stage:
        load.start()

    barrier = pltpu.get_barrier_semaphore()
    pl.semaphore_signal(barrier, inc=1, device_id={axis: mate}, device_id_type=MESH)

    @pl.when(jnp.logical_not(late))
    def _():
        for dev in side:
            pl.semaphore_signal(barrier, inc=1, device_id={axis: dev}, device_id_type=MESH)

    pl.semaphore_wait(barrier, 2 + lax.rem(home, 2))

    @pl.when(late)
    def _():
        for dev in side:
            pl.semaphore_signal(late_sem, inc=1, device_id={axis: dev}, device_id_type=MESH)

    def send_early(k):
        stage[k].wait()
        send_block(x_stage.at[k], side[k], 0, in_send.at[0])
        for slot in range(1, EARLY):
            send_block(x_hbm.at[side[k] * own + slot], side[k], slot, in_send.at[1])

    send_early(0)

    @pl.when(beside_late)
    def _():
        pl.semaphore_wait(late_sem, 1)

    for dev in side:
        pl.semaphore_signal(near_sem, inc=1, device_id={axis: dev}, device_id_type=MESH)
    send_early(1)
    operands = [
        (b_spatial_hbm, b_spatial), (w_spatial_hbm, w_spatial), (ln1_gain_hbm, ln1_gain), (ln1_bias_hbm, ln1_bias), (w_in_hbm, w_in),
        (b_in_hbm, b_in), (ln2_gain_hbm, ln2_gain), (ln2_bias_hbm, ln2_bias), (w_out_hbm, w_out), (b_out_hbm, b_out),
    ]
    loads = [pltpu.make_async_copy(src, dst, w_sem.at[len(NEAR) + k]) for k, (src, dst) in enumerate(operands)]
    for load in loads:
        load.start()
    pl.semaphore_wait(near_sem, len(side))

    pl.semaphore_signal(far_sem, inc=1, device_id={axis: mate}, device_id_type=MESH)
    for slot in range(EARLY):
        for dev in cross:
            send_block(x_hbm.at[dev * own + slot], dev, slot, in_send.at[1])
    pl.semaphore_wait(far_sem, 1)
    for slot in range(EARLY):
        for dev in far + [mate]:
            send_block(x_hbm.at[dev * own + slot], dev, slot, in_send.at[1])

    inner = (core > 0) & (home > 0) & (home < groups - 1)
    opposite = (groups - 1 - home) * per_tile + core
    spared = [(own - 1, 0, rows, 0), (own - 2, 0, rows // 4, rows)]

    @pl.when(inner)
    def _():
        for slot, first, size, place in spared:
            pltpu.make_async_remote_copy(
                src_ref=x_hbm.at[far[-1] * own + slot, pl.ds(first, size)],
                dst_ref=x_relay.at[pl.ds(place, size)],
                send_sem=in_send.at[1],
                recv_sem=bypass_sem.at[0],
                device_id={axis: opposite},
                device_id_type=MESH,
            ).start()

    @pl.loop(EARLY, own)
    def _(slot):
        for dev in side + cross + far[:-1] + [mate]:
            send_block(x_hbm.at[dev * own + slot], dev, slot, in_send.at[1])

        @pl.when(jnp.logical_not(inner & (slot >= own - 2)))
        def _():
            send_block(x_hbm.at[far[-1] * own + slot], far[-1], slot, in_send.at[1])

        @pl.when(inner & (slot == own - 2))
        def _():
            rest = rows - rows // 4
            pltpu.make_async_remote_copy(
                src_ref=x_hbm.at[far[-1] * own + slot, pl.ds(rows // 4, rest)],
                dst_ref=x_buf.at[slot, pl.ds(pl.multiple_of(me * rows + rows // 4, rows // 4), rest)],
                send_sem=in_send.at[1],
                recv_sem=in_recv.at[slot],
                device_id={axis: far[-1]},
                device_id_type=MESH,
            ).start()

    @pl.loop(0, own)
    def _(slot):
        pltpu.make_async_copy(x_hbm.at[me * own + slot], x_buf.at[slot, block_rows(me)], in_recv.at[slot]).start()

    loads[0].wait()
    for first in range(0, patches, 128):
        lane_bias = jnp.broadcast_to(b_spatial[first:first + 128].reshape(1, 128), (128, 128))
        bias_col[first:first + 128, :] = lane_bias.T
    loads[1].wait()

    @pl.loop(0, patches // TILE)
    def _(step):
        out_rows = pl.ds(pl.multiple_of(step * TILE, TILE), TILE)
        for first in range(0, patches, TILE):
            w_mix[out_rows, first:first + TILE] = w_spatial[first:first + TILE, out_rows].T

    for load in loads[2:]:
        load.wait()

    def send_result(src, owner, slot, dev, sem):
        pltpu.make_async_remote_copy(
            src_ref=src,
            dst_ref=out_ref.at[owner * own + slot],
            send_sem=sem,
            recv_sem=out_recv.at[owner],
            device_id={axis: dev},
            device_id_type=MESH,
        ).start()

    def last_part(tile):
        return jnp.where(tile == 0, 0, per_tile - 1)

    def send_tile(slot, tile, group):
        first_dev = tile * per_tile + per_tile - 1 - last_part(tile)
        send_result(o_buf.at[slot, block_rows(first_dev)], me, slot, first_dev, out_send.at[0])
        dev = tile * per_tile + last_part(tile)
        src = o_buf.at[slot, block_rows(dev)]
        if group not in NEAR:
            send_result(src, me, slot, dev, out_send.at[0])
        else:
            handed = (slot == own - 1) & (core > 0)

            @pl.when(jnp.logical_not(handed))
            def _():
                send_result(src, me, slot, dev, out_send.at[0])

            @pl.when(handed)
            def _():
                pltpu.make_async_remote_copy(
                    src_ref=src,
                    dst_ref=relay.at[NEAR.index(group)],
                    send_sem=out_send.at[0],
                    recv_sem=relay_sem.at[0],
                    device_id={axis: mate},
                    device_id_type=MESH,
                ).start()

    def send_home(slot):
        pltpu.make_async_copy(o_buf.at[slot, block_rows(me)], out_ref.at[me * own + slot], out_recv.at[me]).start()
        send_result(o_buf.at[slot, block_rows(mate)], me, slot, mate, out_send.at[0])

    @pl.loop(0, own)
    def _(slot):
        pltpu.make_async_copy(x_buf.at[slot], x_buf.at[slot], in_recv.at[slot]).wait()

        @pl.loop(0, tiles)
        def _(tile):
            here = pl.ds(pl.multiple_of(tile * TILE, TILE), TILE)
            normed = layer_norm(x_buf[slot, here, :], as_row(ln1_gain), as_row(ln1_bias))
            gate = []
            for first in range(0, 2 * half_dim, 256):
                cols = slice(first, first + 256)
                hidden = jnp.dot(normed, w_in[:, cols], preferred_element_type=F32) + b_in[cols].reshape(1, 256)
                act = gelu(hidden)
                if first < half_dim:
                    a_buf[here, cols] = act
                else:
                    gate.append(act)
            gate = jnp.concatenate(gate, axis=1)
            n_buf[here, :] = layer_norm(gate, as_row(ln2_gain), as_row(ln2_bias))

        @pl.when(slot > 0)
        def _():
            send_home(slot - 1)

        @pl.when(inner & (slot == 1))
        def _():
            pltpu.make_async_copy(x_relay, x_relay, bypass_sem.at[0]).wait()
            for spared_slot, first, size, place in spared:
                pltpu.make_async_remote_copy(
                    src_ref=x_relay.at[pl.ds(place, size)],
                    dst_ref=x_buf.at[spared_slot, pl.ds(pl.multiple_of(opposite * rows + first, size), size)],
                    send_sem=bypass_sem.at[1],
                    recv_sem=in_recv.at[spared_slot],
                    device_id={axis: lax.rem(groups + 1 - home, groups) * per_tile + core},
                    device_id_type=MESH,
                ).start()

        previous = None
        for group in FAR + NEAR + (0,):
            tile = lax.rem(home + group, groups)
            here = pl.ds(pl.multiple_of(tile * TILE, TILE), TILE)
            spatial = jnp.dot(w_mix[here, :], n_buf[...], preferred_element_type=F32).astype(BF16)
            bias = jnp.tile(bias_col[here, :], (1, half_dim // 128))
            gated = (a_buf[here, :].astype(F32) * (spatial.astype(F32) + bias)).astype(BF16)
            mixed = jnp.dot(gated, w_out[...], preferred_element_type=F32) + as_row(b_out)
            o_buf[slot, here, :] = (x_buf[slot, here, :].astype(F32) + mixed).astype(BF16)
            if previous is not None:
                send_tile(slot, *previous)
            previous = tile, group

    @pl.when(core == 0)
    def _():
        pltpu.make_async_copy(relay, relay, relay_sem.at[0]).wait()
        for k, group in enumerate(NEAR):
            send_result(relay.at[k], mate, own - 1, across(group, last_part(across(group, 0) // per_tile)), relay_sem.at[1])

    send_home(own - 1)

    pltpu.make_async_copy(x_stage, x_stage, in_send.at[0]).wait()
    rest_sent = [x_buf.at[pl.ds(1, own - 1), pl.ds(0, rows * (n_seq - 1))], x_buf.at[0, pl.ds(0, rows * (n_seq - 1 - len(NEAR)))]]
    for part in rest_sent:
        pltpu.make_async_copy(part, part, in_send.at[1]).wait()
    sent = o_buf.at[:, pl.ds(0, rows * (n_seq - 1))]
    pltpu.make_async_copy(sent, sent, out_send.at[0]).wait()

    @pl.when(core == 0)
    def _():
        pltpu.make_async_copy(relay, relay, relay_sem.at[1]).wait()

    @pl.when(inner)
    def _():
        pltpu.make_async_copy(x_relay, x_relay, bypass_sem.at[1]).wait()

    for dev in range(n_seq):
        part = out_ref.at[pl.ds(dev * own, own)]
        pltpu.make_async_copy(part, part, out_recv.at[dev]).wait()


def solution(mesh):
    row_spec = P("data", "seq", None)
    vec_spec = P(None)
    mat_spec = P(None, None)
    in_specs = (row_spec, vec_spec, vec_spec, mat_spec, vec_spec, vec_spec, vec_spec, mat_spec, vec_spec, mat_spec, vec_spec)
    n_seq = mesh.shape["seq"]

    def per_device(patches, ln1_gain, ln1_bias, w_in, b_in, ln2_gain, ln2_bias, w_spatial, b_spatial, w_out, b_out):
        operands = (patches, ln1_gain, ln1_bias, w_in, b_in, ln2_gain, ln2_bias, w_spatial, b_spatial, w_out, b_out)
        images, rows, dim = patches.shape
        own = images // n_seq
        total = rows * n_seq
        half_dim = w_out.shape[0]
        hbm = pl.BlockSpec(memory_space=pltpu.HBM)
        vec = lambda ref: pltpu.VMEM(ref.shape, ref.dtype)
        return pl.pallas_call(
            functools.partial(block_kernel, n_seq, "seq"),
            out_shape=pltpu.VMEM(patches.shape, BF16),
            in_specs=[hbm] * 11,
            out_specs=pl.BlockSpec(memory_space=pltpu.VMEM),
            scratch_shapes=[
                pltpu.VMEM((own, total, dim), BF16),
                pltpu.VMEM((own, total, dim), BF16),
                pltpu.VMEM((total, half_dim), BF16),
                pltpu.VMEM((total, half_dim), BF16),
                *[vec(v) for v in operands[1:]],
                pltpu.VMEM(w_spatial.shape, BF16),
                pltpu.VMEM((total, 128), F32),
                pltpu.VMEM((len(NEAR), rows, dim), BF16),
                pltpu.SemaphoreType.REGULAR,
                pltpu.SemaphoreType.REGULAR,
                pltpu.SemaphoreType.REGULAR,
                pltpu.VMEM((len(NEAR), rows, dim), BF16),
                pltpu.VMEM((rows + rows // 4, dim), BF16),
                pltpu.SemaphoreType.DMA((2,)),
                pltpu.SemaphoreType.DMA((own,)),
                pltpu.SemaphoreType.DMA((1,)),
                pltpu.SemaphoreType.DMA((n_seq,)),
                pltpu.SemaphoreType.DMA((2,)),
                pltpu.SemaphoreType.DMA((2,)),
                pltpu.SemaphoreType.DMA((len(NEAR) + 10,)),
            ],
            compiler_params=pltpu.CompilerParams(
                collective_id=0, has_side_effects=True, vmem_limit_bytes=48 * 1024 * 1024
            ),
            name="gmlp_block",
        )(*[pltpu.with_memory_space_constraint(v, pltpu.HBM) for v in operands])

    return jax.shard_map(per_device, mesh=mesh, in_specs=in_specs, out_specs=row_spec, check_vma=False)
```

```python
import functools

import jax
import jax.numpy as jnp
from jax import lax
from jax.experimental import pallas as pl
from jax.experimental.pallas import tpu as pltpu
from jax.sharding import PartitionSpec as P

LN_EPS = 1e-6
MESH = pl.DeviceIdType.MESH
F32 = jnp.float32
BF16 = jnp.bfloat16
TILE = 256
NEAR = (1, 3)
FAR = (2,)
EARLY = 4


def layer_norm(values, gain_vec, offset):
    values_f = values.astype(F32)
    mean_val = jnp.mean(values_f, axis=-1, keepdims=True)
    centered = values_f - mean_val
    var_val = jnp.mean(centered * centered, axis=-1, keepdims=True)
    return (centered * lax.rsqrt(var_val + LN_EPS) * gain_vec + offset).astype(BF16)


def as_row(ref):
    return ref[...].reshape(1, ref.shape[0])


def gelu(hidden):
    half = 0.5 * hidden
    return (half + half * lax.erf(hidden * (0.5 ** 0.5))).astype(BF16)


def block_kernel(n_seq, axis, x_hbm, ln1_gain_hbm, ln1_bias_hbm, w_in_hbm, b_in_hbm, ln2_gain_hbm, ln2_bias_hbm, w_spatial_hbm,
                 b_spatial_hbm, w_out_hbm, b_out_hbm, out_ref, x_buf, o_buf, n_buf, a_buf, ln1_gain, ln1_bias, w_in, b_in, ln2_gain,
                 ln2_bias, w_spatial, b_spatial, w_out, b_out, w_mix, bias_col, x_stage, late_sem, near_sem, far_sem,
                 relay, x_relay, in_send, in_recv, out_send, out_recv, relay_sem, bypass_sem, w_sem):
    me = lax.axis_index(axis)
    images, rows, _ = x_hbm.shape
    own = images // n_seq
    patches = rows * n_seq
    half_dim = w_out.shape[0]
    per_tile = TILE // rows
    tiles = patches // TILE
    groups = tiles
    home = me // per_tile

    def block_rows(dev):
        return pl.ds(pl.multiple_of(dev * rows, rows), rows)

    def across(group, part):
        return lax.rem(home + group, groups) * per_tile + part

    def send_block(src, dev, slot, sem):
        pltpu.make_async_remote_copy(
            src_ref=src,
            dst_ref=x_buf.at[slot, block_rows(me)],
            send_sem=sem,
            recv_sem=in_recv.at[slot],
            device_id={axis: dev},
            device_id_type=MESH,
        ).start()

    core = lax.rem(me, per_tile)
    mate = across(0, per_tile - 1 - core)
    late = home == groups - 1
    beside_late = lax.rem(home, 2) == 0
    upper = lax.rem((home + 1) // 2, 2)
    side = [across(1 + 2 * upper, core), across(groups - 1 - 2 * upper, core)]
    cross = [across(group, per_tile - 1 - core) for group in NEAR]
    far = [across(group, part) for group in FAR for part in range(per_tile)]

    pieces = [(0, rows // 4), (rows // 4, rows - rows // 4)]
    stage = []
    for k, dev in enumerate(side):
        stage.append([pltpu.make_async_copy(x_hbm.at[dev * own, pl.ds(first, size)], x_stage.at[k, pl.ds(first, size)],
                                            w_sem.at[k * len(pieces) + p]) for p, (first, size) in enumerate(pieces)])
    for p in range(len(pieces)):
        for loads in stage:
            loads[p].start()

    barrier = pltpu.get_barrier_semaphore()
    pl.semaphore_signal(barrier, inc=1, device_id={axis: mate}, device_id_type=MESH)

    @pl.when(jnp.logical_not(late))
    def _():
        for dev in side:
            pl.semaphore_signal(barrier, inc=1, device_id={axis: dev}, device_id_type=MESH)

    pl.semaphore_wait(barrier, 2 + lax.rem(home, 2))

    @pl.when(late)
    def _():
        for dev in side:
            pl.semaphore_signal(late_sem, inc=1, device_id={axis: dev}, device_id_type=MESH)

    def send_early(k):
        for load, (first, size) in zip(stage[k], pieces):
            load.wait()
            pltpu.make_async_remote_copy(
                src_ref=x_stage.at[k, pl.ds(first, size)],
                dst_ref=x_buf.at[0, pl.ds(pl.multiple_of(me * rows + first, rows // 4), size)],
                send_sem=in_send.at[0],
                recv_sem=in_recv.at[0],
                device_id={axis: side[k]},
                device_id_type=MESH,
            ).start()
        for slot in range(1, EARLY):
            send_block(x_hbm.at[side[k] * own + slot], side[k], slot, in_send.at[1])

    send_early(0)

    @pl.when(beside_late)
    def _():
        pl.semaphore_wait(late_sem, 1)

    for dev in side:
        pl.semaphore_signal(near_sem, inc=1, device_id={axis: dev}, device_id_type=MESH)
    send_early(1)
    operands = [
        (b_spatial_hbm, b_spatial), (w_spatial_hbm, w_spatial), (ln1_gain_hbm, ln1_gain), (ln1_bias_hbm, ln1_bias), (w_in_hbm, w_in),
        (b_in_hbm, b_in), (ln2_gain_hbm, ln2_gain), (ln2_bias_hbm, ln2_bias), (w_out_hbm, w_out), (b_out_hbm, b_out),
    ]
    loads = [pltpu.make_async_copy(src, dst, w_sem.at[2 * len(NEAR) + k]) for k, (src, dst) in enumerate(operands)]
    for load in loads:
        load.start()
    pl.semaphore_wait(near_sem, len(side))

    pl.semaphore_signal(far_sem, inc=1, device_id={axis: mate}, device_id_type=MESH)
    for slot in range(EARLY):
        for dev in cross:
            send_block(x_hbm.at[dev * own + slot], dev, slot, in_send.at[1])
    pl.semaphore_wait(far_sem, 1)
    for slot in range(EARLY):
        for dev in far + [mate]:
            send_block(x_hbm.at[dev * own + slot], dev, slot, in_send.at[1])

    inner = (core > 0) & (home > 0) & (home < groups - 1)
    opposite = (groups - 1 - home) * per_tile + core
    spared = [(own - 1, 0, rows, 0), (own - 2, 0, rows // 4, rows)]

    @pl.when(inner)
    def _():
        for slot, first, size, place in spared:
            pltpu.make_async_remote_copy(
                src_ref=x_hbm.at[far[-1] * own + slot, pl.ds(first, size)],
                dst_ref=x_relay.at[pl.ds(place, size)],
                send_sem=in_send.at[1],
                recv_sem=bypass_sem.at[0],
                device_id={axis: opposite},
                device_id_type=MESH,
            ).start()

    @pl.loop(EARLY, own)
    def _(slot):
        for dev in side + cross + far[:-1] + [mate]:
            send_block(x_hbm.at[dev * own + slot], dev, slot, in_send.at[1])

        @pl.when(jnp.logical_not(inner & (slot >= own - 2)))
        def _():
            send_block(x_hbm.at[far[-1] * own + slot], far[-1], slot, in_send.at[1])

        @pl.when(inner & (slot == own - 2))
        def _():
            rest = rows - rows // 4
            pltpu.make_async_remote_copy(
                src_ref=x_hbm.at[far[-1] * own + slot, pl.ds(rows // 4, rest)],
                dst_ref=x_buf.at[slot, pl.ds(pl.multiple_of(me * rows + rows // 4, rows // 4), rest)],
                send_sem=in_send.at[1],
                recv_sem=in_recv.at[slot],
                device_id={axis: far[-1]},
                device_id_type=MESH,
            ).start()

    @pl.loop(0, own)
    def _(slot):
        pltpu.make_async_copy(x_hbm.at[me * own + slot], x_buf.at[slot, block_rows(me)], in_recv.at[slot]).start()

    loads[0].wait()
    for first in range(0, patches, 128):
        lane_bias = jnp.broadcast_to(b_spatial[first:first + 128].reshape(1, 128), (128, 128))
        bias_col[first:first + 128, :] = lane_bias.T
    loads[1].wait()

    @pl.loop(0, patches // TILE)
    def _(step):
        out_rows = pl.ds(pl.multiple_of(step * TILE, TILE), TILE)
        for first in range(0, patches, TILE):
            w_mix[out_rows, first:first + TILE] = w_spatial[first:first + TILE, out_rows].T

    for load in loads[2:]:
        load.wait()

    def send_result(src, owner, slot, dev, sem):
        pltpu.make_async_remote_copy(
            src_ref=src,
            dst_ref=out_ref.at[owner * own + slot],
            send_sem=sem,
            recv_sem=out_recv.at[owner],
            device_id={axis: dev},
            device_id_type=MESH,
        ).start()

    def last_part(tile):
        return jnp.where(tile == 0, 0, per_tile - 1)

    def send_tile(slot, tile, group):
        first_dev = tile * per_tile + per_tile - 1 - last_part(tile)
        send_result(o_buf.at[slot, block_rows(first_dev)], me, slot, first_dev, out_send.at[0])
        dev = tile * per_tile + last_part(tile)
        src = o_buf.at[slot, block_rows(dev)]
        if group not in NEAR:
            send_result(src, me, slot, dev, out_send.at[0])
        else:
            handed = (slot == own - 1) & (core > 0)

            @pl.when(jnp.logical_not(handed))
            def _():
                send_result(src, me, slot, dev, out_send.at[0])

            @pl.when(handed)
            def _():
                pltpu.make_async_remote_copy(
                    src_ref=src,
                    dst_ref=relay.at[NEAR.index(group)],
                    send_sem=out_send.at[0],
                    recv_sem=relay_sem.at[0],
                    device_id={axis: mate},
                    device_id_type=MESH,
                ).start()

    def send_home(slot):
        pltpu.make_async_copy(o_buf.at[slot, block_rows(me)], out_ref.at[me * own + slot], out_recv.at[me]).start()
        send_result(o_buf.at[slot, block_rows(mate)], me, slot, mate, out_send.at[0])

    @pl.loop(0, own)
    def _(slot):
        pltpu.make_async_copy(x_buf.at[slot], x_buf.at[slot], in_recv.at[slot]).wait()

        @pl.loop(0, tiles)
        def _(tile):
            here = pl.ds(pl.multiple_of(tile * TILE, TILE), TILE)
            normed = layer_norm(x_buf[slot, here, :], as_row(ln1_gain), as_row(ln1_bias))
            gate = []
            for first in range(0, 2 * half_dim, 256):
                cols = slice(first, first + 256)
                hidden = jnp.dot(normed, w_in[:, cols], preferred_element_type=F32) + b_in[cols].reshape(1, 256)
                act = gelu(hidden)
                if first < half_dim:
                    a_buf[here, cols] = act
                else:
                    gate.append(act)
            gate = jnp.concatenate(gate, axis=1)
            n_buf[here, :] = layer_norm(gate, as_row(ln2_gain), as_row(ln2_bias))

        @pl.when(slot > 0)
        def _():
            send_home(slot - 1)

        @pl.when(inner & (slot == 1))
        def _():
            pltpu.make_async_copy(x_relay, x_relay, bypass_sem.at[0]).wait()
            for spared_slot, first, size, place in spared:
                pltpu.make_async_remote_copy(
                    src_ref=x_relay.at[pl.ds(place, size)],
                    dst_ref=x_buf.at[spared_slot, pl.ds(pl.multiple_of(opposite * rows + first, size), size)],
                    send_sem=bypass_sem.at[1],
                    recv_sem=in_recv.at[spared_slot],
                    device_id={axis: lax.rem(groups + 1 - home, groups) * per_tile + core},
                    device_id_type=MESH,
                ).start()

        previous = None
        for group in FAR + NEAR + (0,):
            tile = lax.rem(home + group, groups)
            here = pl.ds(pl.multiple_of(tile * TILE, TILE), TILE)
            spatial = jnp.dot(w_mix[here, :], n_buf[...], preferred_element_type=F32).astype(BF16)
            bias = jnp.tile(bias_col[here, :], (1, half_dim // 128))
            gated = (a_buf[here, :].astype(F32) * (spatial.astype(F32) + bias)).astype(BF16)
            mixed = jnp.dot(gated, w_out[...], preferred_element_type=F32) + as_row(b_out)
            o_buf[slot, here, :] = (x_buf[slot, here, :].astype(F32) + mixed).astype(BF16)
            if previous is not None:
                send_tile(slot, *previous)
            previous = tile, group

    @pl.when(core == 0)
    def _():
        pltpu.make_async_copy(relay, relay, relay_sem.at[0]).wait()
        for k, group in enumerate(NEAR):
            send_result(relay.at[k], mate, own - 1, across(group, last_part(across(group, 0) // per_tile)), relay_sem.at[1])

    send_home(own - 1)

    pltpu.make_async_copy(x_stage, x_stage, in_send.at[0]).wait()
    rest_sent = [x_buf.at[pl.ds(1, own - 1), pl.ds(0, rows * (n_seq - 1))], x_buf.at[0, pl.ds(0, rows * (n_seq - 1 - len(NEAR)))]]
    for part in rest_sent:
        pltpu.make_async_copy(part, part, in_send.at[1]).wait()
    sent = o_buf.at[:, pl.ds(0, rows * (n_seq - 1))]
    pltpu.make_async_copy(sent, sent, out_send.at[0]).wait()

    @pl.when(core == 0)
    def _():
        pltpu.make_async_copy(relay, relay, relay_sem.at[1]).wait()

    @pl.when(inner)
    def _():
        pltpu.make_async_copy(x_relay, x_relay, bypass_sem.at[1]).wait()

    for dev in range(n_seq):
        part = out_ref.at[pl.ds(dev * own, own)]
        pltpu.make_async_copy(part, part, out_recv.at[dev]).wait()


def solution(mesh):
    row_spec = P("data", "seq", None)
    vec_spec = P(None)
    mat_spec = P(None, None)
    in_specs = (row_spec, vec_spec, vec_spec, mat_spec, vec_spec, vec_spec, vec_spec, mat_spec, vec_spec, mat_spec, vec_spec)
    n_seq = mesh.shape["seq"]

    def per_device(patches, ln1_gain, ln1_bias, w_in, b_in, ln2_gain, ln2_bias, w_spatial, b_spatial, w_out, b_out):
        operands = (patches, ln1_gain, ln1_bias, w_in, b_in, ln2_gain, ln2_bias, w_spatial, b_spatial, w_out, b_out)
        images, rows, dim = patches.shape
        own = images // n_seq
        total = rows * n_seq
        half_dim = w_out.shape[0]
        hbm = pl.BlockSpec(memory_space=pltpu.HBM)
        vec = lambda ref: pltpu.VMEM(ref.shape, ref.dtype)
        return pl.pallas_call(
            functools.partial(block_kernel, n_seq, "seq"),
            out_shape=pltpu.VMEM(patches.shape, BF16),
            in_specs=[hbm] * 11,
            out_specs=pl.BlockSpec(memory_space=pltpu.VMEM),
            scratch_shapes=[
                pltpu.VMEM((own, total, dim), BF16),
                pltpu.VMEM((own, total, dim), BF16),
                pltpu.VMEM((total, half_dim), BF16),
                pltpu.VMEM((total, half_dim), BF16),
                *[vec(v) for v in operands[1:]],
                pltpu.VMEM(w_spatial.shape, BF16),
                pltpu.VMEM((total, 128), F32),
                pltpu.VMEM((len(NEAR), rows, dim), BF16),
                pltpu.SemaphoreType.REGULAR,
                pltpu.SemaphoreType.REGULAR,
                pltpu.SemaphoreType.REGULAR,
                pltpu.VMEM((len(NEAR), rows, dim), BF16),
                pltpu.VMEM((rows + rows // 4, dim), BF16),
                pltpu.SemaphoreType.DMA((2,)),
                pltpu.SemaphoreType.DMA((own,)),
                pltpu.SemaphoreType.DMA((1,)),
                pltpu.SemaphoreType.DMA((n_seq,)),
                pltpu.SemaphoreType.DMA((2,)),
                pltpu.SemaphoreType.DMA((2,)),
                pltpu.SemaphoreType.DMA((2 * len(NEAR) + 10,)),
            ],
            compiler_params=pltpu.CompilerParams(
                collective_id=0, has_side_effects=True, vmem_limit_bytes=48 * 1024 * 1024
            ),
            name="gmlp_block",
        )(*[pltpu.with_memory_space_constraint(v, pltpu.HBM) for v in operands])

    return jax.shard_map(per_device, mesh=mesh, in_specs=in_specs, out_specs=row_spec, check_vma=False)
```

```python
import functools

import jax
import jax.numpy as jnp
from jax import lax
from jax.experimental import pallas as pl
from jax.experimental.pallas import tpu as pltpu
from jax.sharding import PartitionSpec as P

LN_EPS = 1e-6
MESH = pl.DeviceIdType.MESH
F32 = jnp.float32
BF16 = jnp.bfloat16
TILE = 256
NEAR = (1, 3)
FAR = (2,)
EARLY = 4


def layer_norm(values, gain_vec, offset):
    values_f = values.astype(F32)
    mean_val = jnp.mean(values_f, axis=-1, keepdims=True)
    centered = values_f - mean_val
    var_val = jnp.mean(centered * centered, axis=-1, keepdims=True)
    return (centered * lax.rsqrt(var_val + LN_EPS) * gain_vec + offset).astype(BF16)


def as_row(ref):
    return ref[...].reshape(1, ref.shape[0])


def gelu(hidden):
    half = 0.5 * hidden
    return (half + half * lax.erf(hidden * (0.5 ** 0.5))).astype(BF16)


def block_kernel(n_seq, axis, x_hbm, ln1_gain_hbm, ln1_bias_hbm, w_in_hbm, b_in_hbm, ln2_gain_hbm, ln2_bias_hbm, w_spatial_hbm,
                 b_spatial_hbm, w_out_hbm, b_out_hbm, out_ref, x_buf, o_buf, n_buf, a_buf, ln1_gain, ln1_bias, w_in, b_in, ln2_gain,
                 ln2_bias, w_spatial, b_spatial, w_out, b_out, w_mix, bias_col, x_stage, late_sem, near_sem, far_sem,
                 relay, x_relay, in_send, in_recv, out_send, out_recv, relay_sem, bypass_sem, w_sem):
    me = lax.axis_index(axis)
    images, rows, _ = x_hbm.shape
    own = images // n_seq
    patches = rows * n_seq
    half_dim = w_out.shape[0]
    per_tile = TILE // rows
    tiles = patches // TILE
    groups = tiles
    home = me // per_tile

    def block_rows(dev):
        return pl.ds(pl.multiple_of(dev * rows, rows), rows)

    def across(group, part):
        return lax.rem(home + group, groups) * per_tile + part

    def send_block(src, dev, slot, sem):
        pltpu.make_async_remote_copy(
            src_ref=src,
            dst_ref=x_buf.at[slot, block_rows(me)],
            send_sem=sem,
            recv_sem=in_recv.at[slot],
            device_id={axis: dev},
            device_id_type=MESH,
        ).start()

    core = lax.rem(me, per_tile)
    mate = across(0, per_tile - 1 - core)
    late = home == groups - 1
    beside_late = lax.rem(home, 2) == 0
    upper = lax.rem((home + 1) // 2, 2)
    side = [across(1 + 2 * upper, core), across(groups - 1 - 2 * upper, core)]
    cross = [across(group, per_tile - 1 - core) for group in NEAR]
    far = [across(group, part) for group in FAR for part in range(per_tile)]

    pieces = [(0, rows // 8), (rows // 8, rows - rows // 8)]
    stage = []
    for k, dev in enumerate(side):
        stage.append([pltpu.make_async_copy(x_hbm.at[dev * own, pl.ds(first, size)], x_stage.at[k, pl.ds(first, size)],
                                            w_sem.at[k * len(pieces) + p]) for p, (first, size) in enumerate(pieces)])
    for p in range(len(pieces)):
        for loads in stage:
            loads[p].start()

    barrier = pltpu.get_barrier_semaphore()
    pl.semaphore_signal(barrier, inc=1, device_id={axis: mate}, device_id_type=MESH)

    @pl.when(jnp.logical_not(late))
    def _():
        for dev in side:
            pl.semaphore_signal(barrier, inc=1, device_id={axis: dev}, device_id_type=MESH)

    pl.semaphore_wait(barrier, 2 + lax.rem(home, 2))

    @pl.when(late)
    def _():
        for dev in side:
            pl.semaphore_signal(late_sem, inc=1, device_id={axis: dev}, device_id_type=MESH)

    def send_early(k):
        for load, (first, size) in zip(stage[k], pieces):
            load.wait()
            pltpu.make_async_remote_copy(
                src_ref=x_stage.at[k, pl.ds(first, size)],
                dst_ref=x_buf.at[0, pl.ds(pl.multiple_of(me * rows + first, rows // 8), size)],
                send_sem=in_send.at[0],
                recv_sem=in_recv.at[0],
                device_id={axis: side[k]},
                device_id_type=MESH,
            ).start()
        for slot in range(1, EARLY):
            send_block(x_hbm.at[side[k] * own + slot], side[k], slot, in_send.at[1])

    send_early(0)

    @pl.when(beside_late)
    def _():
        pl.semaphore_wait(late_sem, 1)

    for dev in side:
        pl.semaphore_signal(near_sem, inc=1, device_id={axis: dev}, device_id_type=MESH)
    send_early(1)
    operands = [
        (b_spatial_hbm, b_spatial), (w_spatial_hbm, w_spatial), (ln1_gain_hbm, ln1_gain), (ln1_bias_hbm, ln1_bias), (w_in_hbm, w_in),
        (b_in_hbm, b_in), (ln2_gain_hbm, ln2_gain), (ln2_bias_hbm, ln2_bias), (w_out_hbm, w_out), (b_out_hbm, b_out),
    ]
    loads = [pltpu.make_async_copy(src, dst, w_sem.at[2 * len(NEAR) + k]) for k, (src, dst) in enumerate(operands)]
    for load in loads:
        load.start()
    pl.semaphore_wait(near_sem, len(side))

    pl.semaphore_signal(far_sem, inc=1, device_id={axis: mate}, device_id_type=MESH)
    for slot in range(EARLY):
        for dev in cross:
            send_block(x_hbm.at[dev * own + slot], dev, slot, in_send.at[1])
    pl.semaphore_wait(far_sem, 1)
    for slot in range(EARLY):
        for dev in far + [mate]:
            send_block(x_hbm.at[dev * own + slot], dev, slot, in_send.at[1])

    inner = (core > 0) & (home > 0) & (home < groups - 1)
    opposite = (groups - 1 - home) * per_tile + core
    spared = [(own - 1, 0, rows, 0), (own - 2, 0, rows // 4, rows)]

    @pl.when(inner)
    def _():
        for slot, first, size, place in spared:
            pltpu.make_async_remote_copy(
                src_ref=x_hbm.at[far[-1] * own + slot, pl.ds(first, size)],
                dst_ref=x_relay.at[pl.ds(place, size)],
                send_sem=in_send.at[1],
                recv_sem=bypass_sem.at[0],
                device_id={axis: opposite},
                device_id_type=MESH,
            ).start()

    @pl.loop(EARLY, own)
    def _(slot):
        for dev in side + cross + far[:-1] + [mate]:
            send_block(x_hbm.at[dev * own + slot], dev, slot, in_send.at[1])

        @pl.when(jnp.logical_not(inner & (slot >= own - 2)))
        def _():
            send_block(x_hbm.at[far[-1] * own + slot], far[-1], slot, in_send.at[1])

        @pl.when(inner & (slot == own - 2))
        def _():
            rest = rows - rows // 4
            pltpu.make_async_remote_copy(
                src_ref=x_hbm.at[far[-1] * own + slot, pl.ds(rows // 4, rest)],
                dst_ref=x_buf.at[slot, pl.ds(pl.multiple_of(me * rows + rows // 4, rows // 4), rest)],
                send_sem=in_send.at[1],
                recv_sem=in_recv.at[slot],
                device_id={axis: far[-1]},
                device_id_type=MESH,
            ).start()

    @pl.loop(0, own)
    def _(slot):
        pltpu.make_async_copy(x_hbm.at[me * own + slot], x_buf.at[slot, block_rows(me)], in_recv.at[slot]).start()

    loads[0].wait()
    for first in range(0, patches, 128):
        lane_bias = jnp.broadcast_to(b_spatial[first:first + 128].reshape(1, 128), (128, 128))
        bias_col[first:first + 128, :] = lane_bias.T
    loads[1].wait()

    @pl.loop(0, patches // TILE)
    def _(step):
        out_rows = pl.ds(pl.multiple_of(step * TILE, TILE), TILE)
        for first in range(0, patches, TILE):
            w_mix[out_rows, first:first + TILE] = w_spatial[first:first + TILE, out_rows].T

    for load in loads[2:]:
        load.wait()

    def send_result(src, owner, slot, dev, sem):
        pltpu.make_async_remote_copy(
            src_ref=src,
            dst_ref=out_ref.at[owner * own + slot],
            send_sem=sem,
            recv_sem=out_recv.at[owner],
            device_id={axis: dev},
            device_id_type=MESH,
        ).start()

    def last_part(tile):
        return jnp.where(tile == 0, 0, per_tile - 1)

    def send_tile(slot, tile, group):
        first_dev = tile * per_tile + per_tile - 1 - last_part(tile)
        send_result(o_buf.at[slot, block_rows(first_dev)], me, slot, first_dev, out_send.at[0])
        dev = tile * per_tile + last_part(tile)
        src = o_buf.at[slot, block_rows(dev)]
        if group not in NEAR:
            send_result(src, me, slot, dev, out_send.at[0])
        else:
            handed = (slot == own - 1) & (core > 0)

            @pl.when(jnp.logical_not(handed))
            def _():
                send_result(src, me, slot, dev, out_send.at[0])

            @pl.when(handed)
            def _():
                pltpu.make_async_remote_copy(
                    src_ref=src,
                    dst_ref=relay.at[NEAR.index(group)],
                    send_sem=out_send.at[0],
                    recv_sem=relay_sem.at[0],
                    device_id={axis: mate},
                    device_id_type=MESH,
                ).start()

    def send_home(slot):
        pltpu.make_async_copy(o_buf.at[slot, block_rows(me)], out_ref.at[me * own + slot], out_recv.at[me]).start()
        send_result(o_buf.at[slot, block_rows(mate)], me, slot, mate, out_send.at[0])

    @pl.loop(0, own)
    def _(slot):
        pltpu.make_async_copy(x_buf.at[slot], x_buf.at[slot], in_recv.at[slot]).wait()

        @pl.loop(0, tiles)
        def _(tile):
            here = pl.ds(pl.multiple_of(tile * TILE, TILE), TILE)
            normed = layer_norm(x_buf[slot, here, :], as_row(ln1_gain), as_row(ln1_bias))
            gate = []
            for first in range(0, 2 * half_dim, 256):
                cols = slice(first, first + 256)
                hidden = jnp.dot(normed, w_in[:, cols], preferred_element_type=F32) + b_in[cols].reshape(1, 256)
                act = gelu(hidden)
                if first < half_dim:
                    a_buf[here, cols] = act
                else:
                    gate.append(act)
            gate = jnp.concatenate(gate, axis=1)
            n_buf[here, :] = layer_norm(gate, as_row(ln2_gain), as_row(ln2_bias))

        @pl.when(slot > 0)
        def _():
            send_home(slot - 1)

        @pl.when(inner & (slot == 1))
        def _():
            pltpu.make_async_copy(x_relay, x_relay, bypass_sem.at[0]).wait()
            for spared_slot, first, size, place in spared:
                pltpu.make_async_remote_copy(
                    src_ref=x_relay.at[pl.ds(place, size)],
                    dst_ref=x_buf.at[spared_slot, pl.ds(pl.multiple_of(opposite * rows + first, size), size)],
                    send_sem=bypass_sem.at[1],
                    recv_sem=in_recv.at[spared_slot],
                    device_id={axis: lax.rem(groups + 1 - home, groups) * per_tile + core},
                    device_id_type=MESH,
                ).start()

        previous = None
        for group in FAR + NEAR + (0,):
            tile = lax.rem(home + group, groups)
            here = pl.ds(pl.multiple_of(tile * TILE, TILE), TILE)
            spatial = jnp.dot(w_mix[here, :], n_buf[...], preferred_element_type=F32).astype(BF16)
            bias = jnp.tile(bias_col[here, :], (1, half_dim // 128))
            gated = (a_buf[here, :].astype(F32) * (spatial.astype(F32) + bias)).astype(BF16)
            mixed = jnp.dot(gated, w_out[...], preferred_element_type=F32) + as_row(b_out)
            o_buf[slot, here, :] = (x_buf[slot, here, :].astype(F32) + mixed).astype(BF16)
            if previous is not None:
                send_tile(slot, *previous)
            previous = tile, group

    @pl.when(core == 0)
    def _():
        pltpu.make_async_copy(relay, relay, relay_sem.at[0]).wait()
        for k, group in enumerate(NEAR):
            send_result(relay.at[k], mate, own - 1, across(group, last_part(across(group, 0) // per_tile)), relay_sem.at[1])

    send_home(own - 1)

    pltpu.make_async_copy(x_stage, x_stage, in_send.at[0]).wait()
    rest_sent = [x_buf.at[pl.ds(1, own - 1), pl.ds(0, rows * (n_seq - 1))], x_buf.at[0, pl.ds(0, rows * (n_seq - 1 - len(NEAR)))]]
    for part in rest_sent:
        pltpu.make_async_copy(part, part, in_send.at[1]).wait()
    sent = o_buf.at[:, pl.ds(0, rows * (n_seq - 1))]
    pltpu.make_async_copy(sent, sent, out_send.at[0]).wait()

    @pl.when(core == 0)
    def _():
        pltpu.make_async_copy(relay, relay, relay_sem.at[1]).wait()

    @pl.when(inner)
    def _():
        pltpu.make_async_copy(x_relay, x_relay, bypass_sem.at[1]).wait()

    for dev in range(n_seq):
        part = out_ref.at[pl.ds(dev * own, own)]
        pltpu.make_async_copy(part, part, out_recv.at[dev]).wait()


def solution(mesh):
    row_spec = P("data", "seq", None)
    vec_spec = P(None)
    mat_spec = P(None, None)
    in_specs = (row_spec, vec_spec, vec_spec, mat_spec, vec_spec, vec_spec, vec_spec, mat_spec, vec_spec, mat_spec, vec_spec)
    n_seq = mesh.shape["seq"]

    def per_device(patches, ln1_gain, ln1_bias, w_in, b_in, ln2_gain, ln2_bias, w_spatial, b_spatial, w_out, b_out):
        operands = (patches, ln1_gain, ln1_bias, w_in, b_in, ln2_gain, ln2_bias, w_spatial, b_spatial, w_out, b_out)
        images, rows, dim = patches.shape
        own = images // n_seq
        total = rows * n_seq
        half_dim = w_out.shape[0]
        hbm = pl.BlockSpec(memory_space=pltpu.HBM)
        vec = lambda ref: pltpu.VMEM(ref.shape, ref.dtype)
        return pl.pallas_call(
            functools.partial(block_kernel, n_seq, "seq"),
            out_shape=pltpu.VMEM(patches.shape, BF16),
            in_specs=[hbm] * 11,
            out_specs=pl.BlockSpec(memory_space=pltpu.VMEM),
            scratch_shapes=[
                pltpu.VMEM((own, total, dim), BF16),
                pltpu.VMEM((own, total, dim), BF16),
                pltpu.VMEM((total, half_dim), BF16),
                pltpu.VMEM((total, half_dim), BF16),
                *[vec(v) for v in operands[1:]],
                pltpu.VMEM(w_spatial.shape, BF16),
                pltpu.VMEM((total, 128), F32),
                pltpu.VMEM((len(NEAR), rows, dim), BF16),
                pltpu.SemaphoreType.REGULAR,
                pltpu.SemaphoreType.REGULAR,
                pltpu.SemaphoreType.REGULAR,
                pltpu.VMEM((len(NEAR), rows, dim), BF16),
                pltpu.VMEM((rows + rows // 4, dim), BF16),
                pltpu.SemaphoreType.DMA((2,)),
                pltpu.SemaphoreType.DMA((own,)),
                pltpu.SemaphoreType.DMA((1,)),
                pltpu.SemaphoreType.DMA((n_seq,)),
                pltpu.SemaphoreType.DMA((2,)),
                pltpu.SemaphoreType.DMA((2,)),
                pltpu.SemaphoreType.DMA((2 * len(NEAR) + 10,)),
            ],
            compiler_params=pltpu.CompilerParams(
                collective_id=0, has_side_effects=True, vmem_limit_bytes=48 * 1024 * 1024
            ),
            name="gmlp_block",
        )(*[pltpu.with_memory_space_constraint(v, pltpu.HBM) for v in operands])

    return jax.shard_map(per_device, mesh=mesh, in_specs=in_specs, out_specs=row_spec, check_vma=False)
```
